32 devices in a mesh: width: 4 (over x, core), tok: 8 (over z, y).
Axes of the slice: x: 2, y: 2, z: 4, core: 2. Of those that a mesh axis runs over, the one named last changes fastest.
Arguments:
- tokens_in: bfloat16 [8192, 768], P('tok'), may hold values from -6 to 6
- seq_lengths: int32 [8, 24], P('tok'), may hold values from 1 to 512, 992 in all within a row
- query_weight: bfloat16 [768, 768], P(('width', 'tok')), may hold values from -0.21875 to 0.21875
- key_weight: bfloat16 [768, 768], P(('width', 'tok')), may hold values from -0.21875 to 0.21875
- value_weight: bfloat16 [768, 768], P(('width', 'tok')), may hold values from -0.21875 to 0.21875
- output_weight: bfloat16 [768, 768], P(('width', 'tok')), may hold values from -0.625 to 0.625
- expand_weight: bfloat16 [3072, 768], P(('width', 'tok')), may hold values from -0.21875 to 0.21875
- shrink_weight: bfloat16 [3072, 768], P(('width', 'tok')), may hold values from -0.109375 to 0.109375
- query_bias: bfloat16 [768], P(('width', 'tok')), may hold values from -1.796875 to 1.796875
- value_bias: bfloat16 [768], P(('width', 'tok')), may hold values from -1.796875 to 1.796875
- output_bias: bfloat16 [768], P(('width', 'tok')), may hold values from -1.796875 to 1.796875
- expand_bias: bfloat16 [3072], P(('width', 'tok')), may hold values from -1.796875 to 1.796875
- shrink_bias: bfloat16 [768], P(('width', 'tok')), may hold values from -1.796875 to 1.796875
- first_gain: bfloat16 [768], P(('width', 'tok')), may hold values from 0.5 to 1.5
- first_shift: bfloat16 [768], P(('width', 'tok')), may hold values from -1.796875 to 1.796875
- second_gain: bfloat16 [768], P(('width', 'tok')), may hold values from 0.5 to 1.5
- second_shift: bfloat16 [768], P(('width', 'tok')), may hold values from -1.796875 to 1.796875
- out_grad: bfloat16 [4, 8192, 768], P('width', 'tok'), may hold values from -6 to 6
Outputs:
- layer_out: bfloat16 [4, 8192, 768], P('width', 'tok')
- input_grad: float32 [4, 8192, 768], P('width', 'tok')
- query_weight_grad: float32 [768, 768], P(('width', 'tok'))
- key_weight_grad: float32 [768, 768], P(('width', 'tok'))
- value_weight_grad: float32 [768, 768], P(('width', 'tok'))
- output_weight_grad: float32 [768, 768], P(('width', 'tok'))
- expand_weight_grad: float32 [3072, 768], P(('width', 'tok'))
- shrink_weight_grad: float32 [3072, 768], P(('width', 'tok'))
- query_bias_grad: float32 [768], P(('width', 'tok'))
- value_bias_grad: float32 [768], P(('width', 'tok'))
- output_bias_grad: float32 [768], P(('width', 'tok'))
- expand_bias_grad: float32 [3072], P(('width', 'tok'))
- shrink_bias_grad: float32 [768], P(('width', 'tok'))
- first_gain_grad: float32 [768], P(('width', 'tok'))
- first_shift_grad: float32 [768], P(('width', 'tok'))
- second_gain_grad: float32 [768], P(('width', 'tok'))
- second_shift_grad: float32 [768], P(('width', 'tok'))
The draws below stay inside these ranges and needn't reach their ends.
Inputs may be any that keep to these rules, and one draw needn't show every extreme that they name: `seq_lengths`: each tok shard's 24 lengths sum to 992, and the longest of each shard is exactly 512; a shard's sequences lie end to end from its first slot, and its last 32 slots are padding.
All inputs are finite; a program needn't handle non-finite values.
Results may differ from the reference program's by a relative error of at most 0.017.
Values may be sent and summed in bfloat16 or wider, within the bound.
A program may use at most 320 MiB of HBM per device.

```python
import math
import jax
import jax.numpy as jnp
import numpy as np
from jax import lax

D = 768
HEADS = 12
HEAD_DIM = 64
FF = 3072
TOK_DEV = 1024
NSEQ = 24
PAD = 32
LMAX = 512
GROUPS = 4
TOK_SHARDS = 8
TOKENS = 8192


def shard_levels(stream_key, dims, cuts, smallest, largest):
    def one(axis_at, shards_of):
        steps = jax.random.uniform(jax.random.fold_in(jax.random.fold_in(stream_key, 6), axis_at), (shards_of,), jnp.float32, smallest / len(cuts), largest / len(cuts))
        return jnp.repeat(jnp.exp(steps), dims[axis_at] // shards_of).reshape((-1,) + (1,) * (len(dims) - axis_at - 1))

    factor_of = one(*cuts[0])
    for cut in cuts[1:]:
        factor_of = factor_of * one(*cut)
    return factor_of


def split_up(count, total, most, slope):
    weights = [(1 << 20) // math.isqrt(rank ** slope) + 1 for rank in range(2, count + 1)]
    rest, given = total - most - (count - 1), [1] * (count - 1)
    while rest > 0:
        movable = [i for i in range(count - 1) if given[i] < most]
        whole, remaining = sum([weights[i] for i in movable]), rest
        for i in movable:
            more = min(most - given[i], max(1, remaining * weights[i] // whole), rest)
            given[i] = given[i] + more
            rest = rest - more
    return np.array([most] + given)


def ragged(own_key, count, total, reach, skew):
    if count == 2:
        one = jax.random.randint(own_key, (), max(1, total - reach), min(reach, total - 1) + 1)
        return jnp.stack([one, total - one])
    sizes = jnp.asarray(split_up(count, total, reach, skew), jnp.int32)
    twos = (count - 1) // 2
    source_of, receiver = sizes[1:1 + 2 * twos:2], sizes[2:2 + 2 * twos:2]
    room = jnp.minimum(source_of - 1, reach - receiver)
    shifted = jax.random.randint(jax.random.fold_in(own_key, 1), (twos,), 0, 1 << 20) % (room + 1)
    sizes = sizes.at[1:1 + 2 * twos:2].set(source_of - shifted).at[2:2 + 2 * twos:2].set(receiver + shifted)
    return sizes[jax.random.permutation(jax.random.fold_in(own_key, 2), count)]


def bell_draw(key, extent, deviation, bound, split=(), kind=jnp.bfloat16):
    level = shard_levels(key, extent, split, -0.22, 0.18) if split else 1.0
    values = jax.random.normal(key, extent, jnp.float32) * deviation * level
    return jnp.minimum(jnp.maximum(values, -bound), bound).astype(kind)


def setup_inputs(seed: int = 0) -> dict:
    arg_keys = jax.random.split(jax.random.key(seed), 19)
    return {
        "tokens_in": bell_draw(arg_keys[0], (TOKENS, D), 1.0, 6.0, ((0, 8),)),
        "seq_lengths": jax.vmap(lambda own: ragged(own, NSEQ, TOK_DEV - PAD, LMAX, 2))(jax.random.split(arg_keys[1], TOK_SHARDS)).reshape((TOK_SHARDS, NSEQ)).astype(jnp.int32),
        "query_weight": bell_draw(arg_keys[2], (D, D), D ** -0.5, 0.21875, ((0, 32),)),
        "key_weight": bell_draw(arg_keys[3], (D, D), D ** -0.5, 0.21875, ((0, 32),)),
        "value_weight": bell_draw(arg_keys[4], (D, D), D ** -0.5, 0.21875, ((0, 32),)),
        "output_weight": bell_draw(arg_keys[5], (D, D), (D // 8) ** -0.5, 0.625, ((0, 32),)),
        "expand_weight": bell_draw(arg_keys[6], (FF, D), D ** -0.5, 0.21875, ((0, 32),)),
        "shrink_weight": bell_draw(arg_keys[7], (FF, D), FF ** -0.5, 0.109375, ((0, 32),)),
        "query_bias": bell_draw(arg_keys[8], (D,), 0.3, 1.796875, ((0, 32),)),
        "value_bias": bell_draw(arg_keys[9], (D,), 0.3, 1.796875, ((0, 32),)),
        "output_bias": bell_draw(arg_keys[10], (D,), 0.3, 1.796875, ((0, 32),)),
        "expand_bias": bell_draw(arg_keys[11], (FF,), 0.3, 1.796875, ((0, 32),)),
        "shrink_bias": bell_draw(arg_keys[12], (D,), 0.3, 1.796875, ((0, 32),)),
        "first_gain": jnp.clip(1.0 + 0.1 * jax.random.normal(arg_keys[13], (D,), jnp.float32), 0.5, 1.5).astype(jnp.bfloat16),
        "first_shift": bell_draw(arg_keys[14], (D,), 0.3, 1.796875, ((0, 32),)),
        "second_gain": jnp.clip(1.0 + 0.1 * jax.random.normal(arg_keys[15], (D,), jnp.float32), 0.5, 1.5).astype(jnp.bfloat16),
        "second_shift": bell_draw(arg_keys[16], (D,), 0.3, 1.796875, ((0, 32),)),
        "out_grad": bell_draw(arg_keys[17], (GROUPS, TOKENS, D), 1.0, 6.0, ((0, 4), (1, 8))),
    }


@jax.custom_vjp
def low(v):
    return lax.optimization_barrier(v.astype(jnp.bfloat16)).astype(jnp.float32)

@jax.custom_vjp
def low_back(v):
    return v

def low_keep(v):
    return (low(v), None)

def low_pass(kept, grad):
    return (grad,)

def back_keep(v):
    return (v, None)

def back_low(kept, grad):
    return (low(grad),)
low.defvjp(low_keep, low_pass)
low_back.defvjp(back_keep, back_low)
norm_eps = 1e-12

def matmul(left, right):
    return jnp.dot(left, right, precision=lax.Precision.HIGHEST)

def matmul_rows(left, right):
    return lax.dot_general(left, right, (((1,), (1,)), ((), ())), precision=lax.Precision.HIGHEST)

def layer_norm(value, gain, shift):
    average = lax.optimization_barrier(jnp.mean(value, axis=-1, keepdims=True))
    centred = value - average
    variance = lax.optimization_barrier(jnp.mean(centred * centred, axis=-1, keepdims=True))
    return centred * lax.rsqrt(variance + norm_eps) * gain + shift

def forward(params, inputs, segment, subnet):
    query_weight, key_weight, value_weight, output_weight, expand_weight, shrink_weight, query_bias, value_bias, output_bias, expand_bias, shrink_bias, first_gain, first_shift, second_gain, second_shift = params
    head_count = (subnet + 1) * HEADS // GROUPS
    feat_used = head_count * HEAD_DIM
    units_used = (subnet + 1) * FF // GROUPS
    length = inputs.shape[0]
    score_scale = 1.0 / math.sqrt(HEAD_DIM)
    query_rows = low(low_back(matmul_rows(inputs, query_weight[:feat_used]) + query_bias[:feat_used]))
    key_rows = low(low_back(matmul_rows(inputs, key_weight[:feat_used])))
    value_rows = low(low_back(matmul_rows(inputs, value_weight[:feat_used]) + value_bias[:feat_used]))
    query_heads = query_rows.reshape(length, head_count, HEAD_DIM)
    key_heads = key_rows.reshape(length, head_count, HEAD_DIM)
    value_heads = value_rows.reshape(length, head_count, HEAD_DIM)
    scores = jnp.einsum('qhd,khd->hqk', query_heads, key_heads, precision=lax.Precision.HIGHEST) * score_scale
    scores = low_back(scores)
    allowed = segment[:, None] == segment[None, :]
    scores = jnp.where(allowed[None], scores, -1e+30)
    probs = jax.nn.softmax(scores, axis=-1)
    context = jnp.einsum('hqk,khd->qhd', low(probs), value_heads, precision=lax.Precision.HIGHEST)
    context = low(low_back(context.reshape(length, feat_used)))
    attended = low_back(matmul(context, output_weight[:feat_used]) + output_bias)
    normed = layer_norm(inputs + attended, first_gain, first_shift)
    upward = low_back(matmul_rows(low(normed), expand_weight[:units_used]) + expand_bias[:units_used])
    activated = low(jax.nn.gelu(upward, approximate=False))
    branch = low_back(matmul(activated, shrink_weight[:units_used]) + shrink_bias)
    return layer_norm(normed + branch, second_gain, second_shift)

def reference(tokens_in, seq_lengths, query_weight, key_weight, value_weight, output_weight, expand_weight, shrink_weight, query_bias, value_bias, output_bias, expand_bias, shrink_bias, first_gain, first_shift, second_gain, second_shift, out_grad):
    params = tuple((array.astype(jnp.float32) for array in (query_weight, key_weight, value_weight, output_weight, expand_weight, shrink_weight, query_bias, value_bias, output_bias, expand_bias, shrink_bias, first_gain, first_shift, second_gain, second_shift)))
    positions = jnp.arange(TOK_DEV, dtype=jnp.int32)
    seq_ends = jnp.cumsum(seq_lengths, axis=1).astype(jnp.int32)
    segments = lax.optimization_barrier(jnp.sum((positions[None, :, None] >= seq_ends[:, None, :]).astype(jnp.int32), axis=2))
    inputs = tokens_in.astype(jnp.float32).reshape(TOK_SHARDS, TOK_DEV, D)
    totals = tuple((jnp.zeros(array.shape, jnp.float32) for array in params))
    layer_outs = []
    input_grads = []
    for subnet in range(GROUPS):
        cotangent = out_grad[subnet].astype(jnp.float32).reshape(TOK_SHARDS, TOK_DEV, D)

        def block_step(carried, pieces, subnet=subnet):
            block_inputs, block_segment, block_cot = pieces

            def local_forward(weights_now, rows_now):
                return forward(weights_now, rows_now, block_segment, subnet)
            result, pullback = jax.vjp(local_forward, params, block_inputs)
            weight_grads, row_grads = pullback(block_cot)
            carried = tuple((left + right for left, right in zip(carried, weight_grads)))
            return (carried, (result.astype(jnp.bfloat16), row_grads))
        totals, (result, row_grads) = lax.scan(block_step, totals, (inputs, segments, cotangent))
        layer_outs.append(result.reshape(TOKENS, D))
        input_grads.append(row_grads.reshape(TOKENS, D))
    query_wgrad, key_wgrad, value_wgrad, output_wgrad, expand_wgrad, shrink_wgrad, query_bgrad, value_bgrad, output_bgrad, expand_bgrad, shrink_bgrad, first_ggrad, first_sgrad, second_ggrad, second_sgrad = totals
    return (jnp.stack(layer_outs), jnp.stack(input_grads), query_wgrad, key_wgrad, value_wgrad, output_wgrad, expand_wgrad, shrink_wgrad, query_bgrad, value_bgrad, output_bgrad, expand_bgrad, shrink_bgrad, first_ggrad, first_sgrad, second_ggrad, second_sgrad)
```

```python
import functools
import math

import jax
import jax.numpy as jnp
from jax import lax
from jax.experimental import pallas as pl
from jax.experimental.pallas import tpu as pltpu
from jax.sharding import PartitionSpec as P

HEADS = 12
HEAD_DIM = 64
norm_eps = 1e-12
BF = jnp.bfloat16
F32 = jnp.float32
BR = 128
BC = 256
RT = 256
MASKED = -1e30


def nt(left, right):
    return lax.dot_general(left, right, (((1,), (1,)), ((), ())), preferred_element_type=F32)


def tn(left, right):
    return lax.dot_general(left, right, (((0,), (0,)), ((), ())), preferred_element_type=F32)


def nn(left, right):
    return jnp.dot(left, right, preferred_element_type=F32)


def rows_at(index, size):
    return pl.ds(pl.multiple_of(index * size, size), size)


def head_of(shape, axis):
    return lax.broadcasted_iota(jnp.int32, shape, axis) // HEAD_DIM


def attn_fwd(scal, bounds, x_ref, wq_ref, wk_ref, wv_ref, bias_ref, segc_ref, segr_ref,
             ctx_ref, lse_ref, q_s, kt_s, v_s, s_s, m_s):
    heads = q_s.shape[1] // HEAD_DIM
    tokens = x_ref.shape[0]

    @pl.when(pl.program_id(0) <= scal[0])
    def _():
        wq, wk, wv = wq_ref[0], wk_ref[0], wv_ref[0]

        @pl.loop(0, tokens // RT)
        def _(i):
            r = rows_at(i, RT)
            xb = x_ref[r, :]
            q = (nt(xb, wq) + bias_ref[0, 0:1, :]).astype(BF).astype(F32)
            q_s[r, :] = (q * 0.125).astype(BF)
            v = (nt(xb, wv) + bias_ref[0, 1:2, :]).astype(BF)
            kt = nt(wk, xb).astype(BF)
            for h in range(heads):
                v_s[h, r, :] = jnp.where(head_of(v.shape, 1) == h, v, jnp.zeros_like(v))
                kt_s[h, :, r] = jnp.where(head_of(kt.shape, 0) == h, kt, jnp.zeros_like(kt))

        @pl.loop(0, tokens // BR)
        def _(i):
            r = rows_at(i, BR)
            qb = q_s[r, :]
            seg = segc_ref[r, :]
            seg = jnp.concatenate([seg] * (BC // 128), axis=1)
            lo, hi = bounds[0, i], bounds[1, i]
            m_s[...] = jnp.full_like(m_s, MASKED)

            @pl.loop(lo, hi)
            def _(j):
                c = rows_at(j, BC)
                keep = seg == segr_ref[0:1, c]
                for h in range(heads):
                    s = jnp.where(keep, nn(qb, kt_s[h, :, c]), MASKED)
                    s_s[h, :, c] = s
                    m_s[h] = jnp.maximum(m_s[h], s)

            tops = [jnp.max(m_s[h], axis=1, keepdims=True) for h in range(heads)]
            zero = jnp.zeros((BR, 1), F32)

            def second(j, carry):
                out, sums = carry
                c = rows_at(j, BC)
                new = []
                for h in range(heads):
                    e = jnp.exp(s_s[h, :, c] - tops[h])
                    out = out + nn(e.astype(BF), v_s[h, c, :])
                    new.append(sums[h] + jnp.sum(e, axis=1, keepdims=True))
                return out, tuple(new)

            out, sums = lax.fori_loop(
                lo, hi, second, (jnp.zeros((BR, q_s.shape[1]), F32), (zero,) * heads))
            lane = head_of(out.shape, 1)
            div = jnp.broadcast_to(sums[0], out.shape)
            col = lax.broadcasted_iota(jnp.int32, (BR, 128), 1)
            lse = jnp.broadcast_to(tops[0] + jnp.log(sums[0]), (BR, 128))
            for h in range(1, heads):
                div = jnp.where(lane == h, sums[h], div)
                lse = jnp.where(col == h, tops[h] + jnp.log(sums[h]), lse)
            ctx_ref[0, r, :] = (out / div).astype(BF)
            lse_ref[0, r, :] = lse


def attn_bwd(scal, bounds, x_ref, wq_ref, wk_ref, wv_ref, bias_ref, bcol_ref, segc_ref, segr_ref,
             ctx_ref, lse_ref, do_ref, dot_ref, s1g_ref,
             ig_ref, dwq_ref, dwk_ref, dwv_ref, db_ref,
             q_s, qt_s, k_s, kt_s, vt_s, dq_s, dkt_s, dvt_s, kt_f, vt_f):
    heads = q_s.shape[1] // HEAD_DIM
    tokens = x_ref.shape[0]

    @pl.when(pl.program_id(0) == 0)
    def _():
        ig_ref[...] = s1g_ref[...]

    @pl.when(pl.program_id(0) <= scal[0])
    def _():
        wq, wk, wv = wq_ref[0], wk_ref[0], wv_ref[0]
        qcol = bcol_ref[0, :, 0:1].astype(F32)
        vcol = bcol_ref[0, :, 1:2].astype(F32)

        @pl.loop(0, tokens // RT)
        def _(i):
            r = rows_at(i, RT)
            xb = x_ref[r, :]
            q = (nt(xb, wq) + bias_ref[0, 0:1, :]).astype(BF).astype(F32)
            q_s[r, :] = (q * 0.125).astype(BF)
            qt = (nt(wq, xb) + qcol).astype(BF).astype(F32)
            qt_s[:, r] = (qt * 0.125).astype(BF)
            k = nt(xb, wk).astype(BF)
            kt = nt(wk, xb).astype(BF)
            vt = (nt(wv, xb) + vcol).astype(BF)
            for h in range(heads):
                k_s[h, r, :] = jnp.where(head_of(k.shape, 1) == h, k, jnp.zeros_like(k))
                kt_s[h, :, r] = jnp.where(head_of(kt.shape, 0) == h, kt, jnp.zeros_like(kt))
                vt_s[h, :, r] = jnp.where(head_of(vt.shape, 0) == h, vt, jnp.zeros_like(vt))

        kt_f[...] = jnp.zeros_like(kt_f)
        vt_f[...] = jnp.zeros_like(vt_f)

        @pl.loop(0, tokens // BR)
        def _(i):
            r = rows_at(i, BR)
            qb = q_s[r, :]
            dob = do_ref[0, r, :]
            seg = segc_ref[r, :]
            seg = jnp.concatenate([seg] * (BC // 128), axis=1)
            prod = dob.astype(F32) * ctx_ref[0, r, :].astype(F32)
            lane = head_of(prod.shape, 1)
            inner = [jnp.sum(jnp.where(lane == h, prod, 0.0), axis=1, keepdims=True) for h in range(heads)]
            lses = [lse_ref[0, r, h : h + 1] for h in range(heads)]
            qts = [qt_s[h * HEAD_DIM : (h + 1) * HEAD_DIM, r] for h in range(heads)]
            dots = [dot_ref[0, h * HEAD_DIM : (h + 1) * HEAD_DIM, r] for h in range(heads)]

            def block(j, dq):
                c = rows_at(j, BC)
                keep = seg == segr_ref[0:1, c]
                for h in range(heads):
                    hs = slice(h * HEAD_DIM, (h + 1) * HEAD_DIM)
                    s = jnp.where(keep, nn(qb, kt_s[h, :, c]), MASKED)
                    p = jnp.exp(s - lses[h])
                    dp = nn(dob, vt_s[h, :, c])
                    ds = (p * (dp - inner[h])).astype(BF)
                    dq = dq + nn(ds, k_s[h, c, :])
                    kt_f[hs, c] += nn(qts[h], ds)
                    vt_f[hs, c] += nn(dots[h], p.astype(BF))
                return dq

            dq = lax.fori_loop(bounds[0, i], bounds[1, i], block, jnp.zeros(qb.shape, F32))
            dq_s[r, :] = (dq * 0.125).astype(BF)

        dkt_s[...] = kt_f[...].astype(BF)
        dvt_s[...] = vt_f[...].astype(BF)

        @pl.loop(0, tokens // RT)
        def _(i):
            r = rows_at(i, RT)
            ig_ref[r, :] += nn(dq_s[r, :], wq) + tn(dkt_s[:, r], wk) + tn(dvt_s[:, r], wv)

        x = x_ref[...]
        dwq_ref[0] = tn(dq_s[...], x).astype(BF)
        dwk_ref[0] = nn(dkt_s[...], x).astype(BF)
        dwv_ref[0] = nn(dvt_s[...], x).astype(BF)
        ones = jnp.ones((8, tokens), BF)
        db_ref[0, 0:8, :] = nn(ones, dq_s[...])
        db_ref[0, 8:16, :] = nt(ones, dvt_s[...])


def normal_parts(value):
    phi = jnp.exp(-0.5 * value * value) * (1.0 / math.sqrt(2.0 * math.pi))
    cum = 0.5 + 0.5 * lax.erf(value * math.sqrt(0.5))
    return cum, phi


def middle(scal, x_ref, ctx_ref, wo_ref, e_ref, s_ref, vec_ref, eb_ref, c_ref,
           lo_ref, s1g_ref, do_ref, dot_ref, dwo_ref, vg_ref, ebg_ref, de_hbm, ds_hbm,
           nl_s, n1_s, r1_s, br_s, act_s, gp_s, ug_s, bg_s, stage, sems):
    tokens, width = x_ref.shape
    used = scal[0] + 1
    tiles = tokens // RT
    ob, sb = vec_ref[2:3, :], vec_ref[3:4, :]
    g1, b1 = vec_ref[4:5, :], vec_ref[5:6, :]
    g2, b2 = vec_ref[6:7, :], vec_ref[7:8, :]

    def mean(v):
        return jnp.sum(v, axis=1, keepdims=True) * (1.0 / width)

    @pl.loop(0, tiles)
    def _(i):
        r = rows_at(i, RT)
        total = lax.fori_loop(
            0, used, lambda q, t: t + nn(ctx_ref[q, r, :], wo_ref[q]), jnp.zeros((RT, width), F32))
        v = x_ref[r, :].astype(F32) + (total + ob)
        v = v - mean(v)
        rstd = lax.rsqrt(mean(v * v) + norm_eps)
        n = v * rstd
        n1_s[r, :] = n
        r1_s[r, :] = jnp.broadcast_to(rstd, (RT, 128))
        normed = n * g1 + b1
        nl_s[r, :] = normed.astype(BF)
        br_s[r, :] = normed + sb

    @pl.loop(0, used)
    def _(q):
        @pl.loop(0, tiles)
        def _(i):
            r = rows_at(i, RT)
            u = nt(nl_s[r, :], e_ref[q]) + eb_ref[q, 0:1, :]
            cum, phi = normal_parts(u)
            act = (u * cum).astype(BF)
            act_s[q, r, :] = act
            gp_s[q, r, :] = (cum + u * phi).astype(BF)
            br_s[r, :] += nn(act, s_ref[q])

    zero = jnp.zeros((1, width), F32)

    def second_norm(i, sums):
        r = rows_at(i, RT)
        v = br_s[r, :]
        v = v - mean(v)
        rstd = lax.rsqrt(mean(v * v) + norm_eps)
        n = v * rstd
        lo_ref[r, :] = (n * g2 + b2).astype(BF)
        c = c_ref[r, :].astype(F32)
        m = c * g2
        g = rstd * (m - mean(m) - n * mean(m * n))
        s1g_ref[r, :] = g
        bg = g.astype(BF)
        bg_s[r, :] = bg
        return (sums[0] + jnp.sum(c * n, axis=0, keepdims=True),
                sums[1] + jnp.sum(c, axis=0, keepdims=True),
                sums[2] + jnp.sum(bg.astype(F32), axis=0, keepdims=True))

    g2g, b2g, sbg = lax.fori_loop(0, tiles, second_norm, (zero, zero, zero))
    vg_ref[6:7, :] = g2g
    vg_ref[7:8, :] = b2g
    vg_ref[3:4, :] = sbg

    def moved(kind, q, out_hbm):
        return pltpu.make_async_copy(stage.at[kind], out_hbm.at[q], sems.at[kind])

    @pl.loop(0, used)
    def _(q):
        def tile(i, total):
            r = rows_at(i, RT)
            d = nt(bg_s[r, :], s_ref[q]) * gp_s[q, r, :].astype(F32)
            ug = d.astype(BF)
            ug_s[r, :] = ug
            s1g_ref[r, :] += nn(ug, e_ref[q])
            return total + jnp.sum(ug.astype(F32), axis=0, keepdims=True)

        ebg_ref[q, 0:1, :] = lax.fori_loop(0, tiles, tile, zero)

        @pl.when(q > 0)
        def _():
            moved(0, q - 1, de_hbm).wait()
            moved(1, q - 1, ds_hbm).wait()

        for n in range(width // RT):
            cols = slice(n * RT, (n + 1) * RT)
            stage[0, cols, :] = tn(ug_s[:, cols], nl_s[...]).astype(BF)
            stage[1, cols, :] = tn(act_s[q, :, cols], bg_s[...]).astype(BF)
        moved(0, q, de_hbm).start()
        moved(1, q, ds_hbm).start()

    def first_norm(i, sums):
        r = rows_at(i, RT)
        g = s1g_ref[r, :]
        n = n1_s[r, :]
        m = g * g1
        out = r1_s[r, 0:1] * (m - mean(m) - n * mean(m * n))
        s1g_ref[r, :] = out
        ag = out.astype(BF)
        ug_s[r, :] = ag

        @pl.loop(0, used)
        def _(q):
            do_ref[q, r, :] = nt(ag, wo_ref[q]).astype(BF)
            dot_ref[q, :, r] = nt(wo_ref[q], ag).astype(BF)

        return (sums[0] + jnp.sum(g * n, axis=0, keepdims=True),
                sums[1] + jnp.sum(g, axis=0, keepdims=True),
                sums[2] + jnp.sum(ag.astype(F32), axis=0, keepdims=True))

    g1g, b1g, obg = lax.fori_loop(0, tiles, first_norm, (zero, zero, zero))
    vg_ref[4:5, :] = g1g
    vg_ref[5:6, :] = b1g
    vg_ref[2:3, :] = obg

    @pl.loop(0, used)
    def _(q):
        dwo_ref[q] = tn(ctx_ref[q], ug_s[...]).astype(BF)

    moved(0, used - 1, de_hbm).wait()
    moved(1, used - 1, ds_hbm).wait()


def run_middle(scal, x, ctx, wo, e, s, vec, eb, cot):
    groups, feat, width = wo.shape
    tokens = x.shape[0]
    vm = pl.BlockSpec(memory_space=pltpu.VMEM)
    sds = jax.ShapeDtypeStruct
    return pl.pallas_call(
        middle,
        name="middle",
        out_shape=(
            sds((tokens, width), BF), sds((tokens, width), F32),
            sds((groups, tokens, feat), BF), sds((groups, feat, tokens), BF),
            sds((groups, feat, width), BF), sds((8, width), F32), sds((groups, 8, width), F32),
            sds(e.shape, BF), sds(s.shape, BF)),
        in_specs=[pl.BlockSpec(memory_space=pltpu.SMEM)] + [vm] * 8,
        out_specs=(vm,) * 7 + (pl.BlockSpec(memory_space=pl.ANY),) * 2,
        scratch_shapes=[
            pltpu.VMEM((tokens, width), BF), pltpu.VMEM((tokens, width), F32),
            pltpu.VMEM((tokens, 128), F32), pltpu.VMEM((tokens, width), F32),
            pltpu.VMEM((groups, tokens, width), BF), pltpu.VMEM((groups, tokens, width), BF),
            pltpu.VMEM((tokens, width), BF), pltpu.VMEM((tokens, width), BF),
            pltpu.VMEM((2, width, width), BF), pltpu.SemaphoreType.DMA((2,))],
        compiler_params=pltpu.CompilerParams(vmem_limit_bytes=62 << 20),
    )(scal, x, ctx, wo, e, s, vec, eb, cot)


def attn_specs(tokens, width, feat):
    def at_quarter(*block):
        return pl.BlockSpec((1,) + block, lambda q, s, b: (jnp.minimum(q, s[0]), 0, 0))

    def whole(*block):
        return pl.BlockSpec(block, lambda q, s, b: (0, 0))

    return at_quarter, whole


def run_fwd(scal, bounds, x, wq, wk, wv, bias, segc, segr):
    groups, feat, width = wq.shape
    tokens = x.shape[0]
    heads = feat // HEAD_DIM
    at_quarter, whole = attn_specs(tokens, width, feat)
    sds = jax.ShapeDtypeStruct
    return pl.pallas_call(
        attn_fwd,
        name="attn_fwd",
        out_shape=(sds((groups, tokens, feat), BF), sds((groups, tokens, 128), F32)),
        grid_spec=pltpu.PrefetchScalarGridSpec(
            num_scalar_prefetch=2, grid=(groups,),
            in_specs=[whole(tokens, width)] + [at_quarter(feat, width)] * 3
            + [at_quarter(8, feat), whole(tokens, 128), whole(8, tokens)],
            out_specs=(at_quarter(tokens, feat), at_quarter(tokens, 128)),
            scratch_shapes=[
                pltpu.VMEM((tokens, feat), BF), pltpu.VMEM((heads, feat, tokens), BF),
                pltpu.VMEM((heads, tokens, feat), BF), pltpu.VMEM((heads, BR, tokens), F32),
                pltpu.VMEM((heads, BR, BC), F32)]),
        compiler_params=pltpu.CompilerParams(vmem_limit_bytes=60 << 20),
    )(scal, bounds, x, wq, wk, wv, bias, segc, segr)


def run_bwd(scal, bounds, x, wq, wk, wv, bias, bcol, segc, segr, ctx, lse, do, dot, s1g):
    groups, feat, width = wq.shape
    tokens = x.shape[0]
    heads = feat // HEAD_DIM
    at_quarter, whole = attn_specs(tokens, width, feat)
    sds = jax.ShapeDtypeStruct
    return pl.pallas_call(
        attn_bwd,
        name="attn_bwd",
        out_shape=(sds((tokens, width), F32),) + (sds((groups, feat, width), BF),) * 3
        + (sds((groups, 16, feat), F32),),
        grid_spec=pltpu.PrefetchScalarGridSpec(
            num_scalar_prefetch=2, grid=(groups,),
            in_specs=[whole(tokens, width)] + [at_quarter(feat, width)] * 3
            + [at_quarter(8, feat), at_quarter(feat, 128), whole(tokens, 128), whole(8, tokens),
               at_quarter(tokens, feat), at_quarter(tokens, 128), at_quarter(tokens, feat),
               at_quarter(feat, tokens), whole(tokens, width)],
            out_specs=(whole(tokens, width),) + (at_quarter(feat, width),) * 3 + (at_quarter(16, feat),),
            scratch_shapes=[
                pltpu.VMEM((tokens, feat), BF), pltpu.VMEM((feat, tokens), BF),
                pltpu.VMEM((heads, tokens, feat), BF), pltpu.VMEM((heads, feat, tokens), BF),
                pltpu.VMEM((heads, feat, tokens), BF), pltpu.VMEM((tokens, feat), BF),
                pltpu.VMEM((feat, tokens), BF), pltpu.VMEM((feat, tokens), BF),
                pltpu.VMEM((feat, tokens), F32), pltpu.VMEM((feat, tokens), F32)]),
        compiler_params=pltpu.CompilerParams(vmem_limit_bytes=60 << 20),
    )(scal, bounds, x, wq, wk, wv, bias, bcol, segc, segr, ctx, lse, do, dot, s1g)


def columns(array):
    return jnp.broadcast_to(array[:, :, None], array.shape + (128,)).astype(BF)


def gather_all(pack):
    return lax.all_gather(pack, ("width", "tok"), axis=0, tiled=False)


def scatter_all(terms):
    flat = terms.reshape((-1,) + terms.shape[2:])
    return lax.psum_scatter(flat, ("width", "tok"), scatter_dimension=0, tiled=True)[0]


def local(tokens_in, seq_lengths, *rest):
    weights, biases, out_grad = rest[:6], rest[6:15], rest[15]
    groups = lax.axis_size("width")
    shards = lax.axis_size("tok")
    level = lax.axis_index("width")
    tokens, width = tokens_in.shape
    owned = weights[0].shape[0]
    owned_ff = weights[4].shape[0]
    feat = owned * shards
    units = owned_ff * shards

    small = jnp.concatenate(biases)
    small = jnp.pad(small, (0, width - small.shape[0]))[None, :]
    small = jnp.pad(small, ((0, 7), (0, 0)))
    got = gather_all(jnp.concatenate(weights + (small,), axis=0))
    got = got.reshape((groups, shards) + got.shape[1:])

    def rows(lower, count):
        return got[:, :, lower : lower + count].reshape(groups, count * shards, width)

    wq, wk, wv, wo = (rows(n * owned, owned) for n in range(4))
    we, ws = rows(4 * owned, owned_ff), rows(4 * owned + owned_ff, owned_ff)
    row = got[:, :, 4 * owned + 2 * owned_ff]
    sizes = [b.shape[0] for b in biases]
    starts = [sum(sizes[:n]) for n in range(9)]
    vecs = [row[:, :, a : a + n].reshape(groups, n * shards) for a, n in zip(starts, sizes)]
    eb = jnp.pad(vecs[3][:, None, :].astype(F32), ((0, 0), (0, 7), (0, 0)))
    order = [vecs[0], vecs[1], vecs[2], vecs[4]] + vecs[5:]
    vec = jnp.stack([v.reshape(-1) for v in order]).astype(F32)
    bias = jnp.pad(jnp.stack([vecs[0], vecs[1]], axis=1).astype(F32), ((0, 0), (0, 6), (0, 0)))
    bcol = jnp.pad(jnp.stack([vecs[0], vecs[1]], axis=2), ((0, 0), (0, 0), (0, 126)))

    ends = jnp.cumsum(seq_lengths[0])
    positions = jnp.arange(tokens, dtype=jnp.int32)
    segment = jnp.sum((positions[:, None] >= ends[None, :]).astype(jnp.int32), axis=1)
    lows = jnp.sum((segment[None, :] < segment[::BR, None]).astype(jnp.int32), axis=1)
    highs = jnp.sum((segment[None, :] <= segment[BR - 1 :: BR, None]).astype(jnp.int32), axis=1)
    bounds = jnp.stack([lows // BC, (highs + BC - 1) // BC])
    segc = jnp.broadcast_to(segment[:, None], (tokens, 128))
    segr = jnp.broadcast_to(segment[None, :], (8, tokens))
    scal = level[None].astype(jnp.int32)

    ctx, lse = run_fwd(scal, bounds, tokens_in, wq, wk, wv, bias, segc, segr)
    result, s1g, do, dot, dwo, vg, ebg, de, ds = run_middle(
        scal, tokens_in, ctx, wo, we, ws, vec, eb, out_grad[0])
    input_grad, dwq, dwk, dwv, db = run_bwd(
        scal, bounds, tokens_in, wq, wk, wv, bias, bcol, segc, segr, ctx, lse, do, dot, s1g)

    mine = jnp.arange(groups) <= level

    def pieces(term):
        return term.reshape((groups, shards, -1) + term.shape[2:])

    def split(line):
        return line.reshape(groups, shards, -1)

    def only(term):
        return jnp.where(mine.reshape((groups,) + (1,) * (term.ndim - 1)), term, jnp.zeros_like(term))

    lines = [
        only(split(db[:, 0])), only(split(db[:, 8])), split(vg[2]), only(split(ebg[:, 0])),
        split(vg[3]), split(vg[4]), split(vg[5]), split(vg[6]), split(vg[7])]
    line = jnp.concatenate(lines, axis=2).astype(BF)
    line = jnp.pad(line, ((0, 0), (0, 0), (0, width - line.shape[2])))
    line = jnp.pad(line[:, :, None, :], ((0, 0), (0, 0), (0, 7), (0, 0)))
    terms = only(jnp.concatenate([pieces(t) for t in (dwq, dwk, dwv, dwo, de, ds)], axis=2))
    final = scatter_all(jnp.concatenate([terms, line], axis=2)).astype(F32)
    outs = [final[n * owned : (n + 1) * owned] for n in range(4)]
    outs += [final[4 * owned : 4 * owned + owned_ff], final[4 * owned + owned_ff : 4 * owned + 2 * owned_ff]]
    last = final[4 * owned + 2 * owned_ff]
    outs += [last[a : a + n] for a, n in zip(starts, sizes)]
    return (result[None], input_grad[None]) + tuple(outs)


def solution(mesh):
    both = ("width", "tok")
    placed = (P("tok", None), P("tok", None)) + (P(both, None),) * 6 + (P(both),) * 9
    return jax.shard_map(
        local,
        mesh=mesh,
        in_specs=placed + (P("width", "tok", None),),
        out_specs=(P("width", "tok", None), P("width", "tok", None))
        + (P(both, None),) * 6 + (P(both),) * 9,
        check_vma=False,
    )
```

```python
import functools
import math

import jax
import jax.numpy as jnp
from jax import lax
from jax.experimental import pallas as pl
from jax.experimental.pallas import tpu as pltpu
from jax.sharding import PartitionSpec as P

HEADS = 12
HEAD_DIM = 64
norm_eps = 1e-12
BF = jnp.bfloat16
F32 = jnp.float32
BR = 128
BC = 256
RT = 256
MASKED = -1e30


def nt(left, right):
    return lax.dot_general(left, right, (((1,), (1,)), ((), ())), preferred_element_type=F32)


def tn(left, right):
    return lax.dot_general(left, right, (((0,), (0,)), ((), ())), preferred_element_type=F32)


def nn(left, right):
    return jnp.dot(left, right, preferred_element_type=F32)


def rows_at(index, size):
    return pl.ds(pl.multiple_of(index * size, size), size)


def head_of(shape, axis):
    return lax.broadcasted_iota(jnp.int32, shape, axis) // HEAD_DIM


def attn_fwd(scal, bounds, x_ref, wq_ref, wk_ref, wv_ref, bias_ref, segc_ref, segr_ref,
             ctx_ref, lse_ref, q_s, kt_s, v_s, s_s, m_s):
    heads = q_s.shape[1] // HEAD_DIM
    tokens = x_ref.shape[0]

    @pl.when(pl.program_id(0) <= scal[0])
    def _():
        wq, wk, wv = wq_ref[0], wk_ref[0], wv_ref[0]

        @pl.loop(0, tokens // RT)
        def _(i):
            r = rows_at(i, RT)
            xb = x_ref[r, :]
            q = (nt(xb, wq) + bias_ref[0, 0:1, :]).astype(BF).astype(F32)
            q_s[r, :] = (q * 0.125).astype(BF)
            v = (nt(xb, wv) + bias_ref[0, 1:2, :]).astype(BF)
            kt = nt(wk, xb).astype(BF)
            for h in range(heads):
                v_s[h, r, :] = jnp.where(head_of(v.shape, 1) == h, v, jnp.zeros_like(v))
                kt_s[h, :, r] = jnp.where(head_of(kt.shape, 0) == h, kt, jnp.zeros_like(kt))

        @pl.loop(0, tokens // BR)
        def _(i):
            r = rows_at(i, BR)
            qb = q_s[r, :]
            seg = segc_ref[r, :]
            seg = jnp.concatenate([seg] * (BC // 128), axis=1)
            lo, hi = bounds[0, i], bounds[1, i]
            m_s[...] = jnp.full_like(m_s, MASKED)

            @pl.loop(lo, hi)
            def _(j):
                c = rows_at(j, BC)
                keep = seg == segr_ref[0:1, c]
                for h in range(heads):
                    s = jnp.where(keep, nn(qb, kt_s[h, :, c]), MASKED)
                    s_s[h, :, c] = s
                    m_s[h] = jnp.maximum(m_s[h], s)

            tops = [jnp.max(m_s[h], axis=1, keepdims=True) for h in range(heads)]
            zero = jnp.zeros((BR, 1), F32)

            def second(j, carry):
                out, sums = carry
                c = rows_at(j, BC)
                new = []
                for h in range(heads):
                    e = jnp.exp(s_s[h, :, c] - tops[h])
                    out = out + nn(e.astype(BF), v_s[h, c, :])
                    new.append(sums[h] + jnp.sum(e, axis=1, keepdims=True))
                return out, tuple(new)

            out, sums = lax.fori_loop(
                lo, hi, second, (jnp.zeros((BR, q_s.shape[1]), F32), (zero,) * heads))
            lane = head_of(out.shape, 1)
            div = jnp.broadcast_to(sums[0], out.shape)
            col = lax.broadcasted_iota(jnp.int32, (BR, 128), 1)
            lse = jnp.broadcast_to(tops[0] + jnp.log(sums[0]), (BR, 128))
            for h in range(1, heads):
                div = jnp.where(lane == h, sums[h], div)
                lse = jnp.where(col == h, tops[h] + jnp.log(sums[h]), lse)
            ctx_ref[0, r, :] = (out / div).astype(BF)
            lse_ref[0, r, :] = lse


def attn_bwd(scal, bounds, x_ref, wq_ref, wk_ref, wv_ref, bias_ref, bcol_ref, segc_ref, segr_ref,
             ctx_ref, lse_ref, do_ref, dot_ref, s1g_ref,
             ig_ref, dwq_ref, dwk_ref, dwv_ref, db_ref,
             q_s, qt_s, k_s, kt_s, vt_s, dq_s, dkt_s, dvt_s, kt_f, vt_f):
    heads = q_s.shape[1] // HEAD_DIM
    tokens = x_ref.shape[0]

    @pl.when(pl.program_id(0) == 0)
    def _():
        ig_ref[...] = s1g_ref[...]

    @pl.when(pl.program_id(0) <= scal[0])
    def _():
        wq, wk, wv = wq_ref[0], wk_ref[0], wv_ref[0]
        qcol = bcol_ref[0, :, 0:1].astype(F32)
        vcol = bcol_ref[0, :, 1:2].astype(F32)

        @pl.loop(0, tokens // RT)
        def _(i):
            r = rows_at(i, RT)
            xb = x_ref[r, :]
            q = (nt(xb, wq) + bias_ref[0, 0:1, :]).astype(BF).astype(F32)
            q_s[r, :] = (q * 0.125).astype(BF)
            qt = (nt(wq, xb) + qcol).astype(BF).astype(F32)
            qt_s[:, r] = (qt * 0.125).astype(BF)
            k = nt(xb, wk).astype(BF)
            kt = nt(wk, xb).astype(BF)
            vt = (nt(wv, xb) + vcol).astype(BF)
            for h in range(heads):
                k_s[h, r, :] = jnp.where(head_of(k.shape, 1) == h, k, jnp.zeros_like(k))
                kt_s[h, :, r] = jnp.where(head_of(kt.shape, 0) == h, kt, jnp.zeros_like(kt))
                vt_s[h, :, r] = jnp.where(head_of(vt.shape, 0) == h, vt, jnp.zeros_like(vt))

        kt_f[...] = jnp.zeros_like(kt_f)
        vt_f[...] = jnp.zeros_like(vt_f)

        @pl.loop(0, tokens // BR)
        def _(i):
            r = rows_at(i, BR)
            qb = q_s[r, :]
            dob = do_ref[0, r, :]
            seg = segc_ref[r, :]
            seg = jnp.concatenate([seg] * (BC // 128), axis=1)
            prod = dob.astype(F32) * ctx_ref[0, r, :].astype(F32)
            lane = head_of(prod.shape, 1)
            inner = [jnp.sum(jnp.where(lane == h, prod, 0.0), axis=1, keepdims=True) for h in range(heads)]
            lses = [lse_ref[0, r, h : h + 1] for h in range(heads)]
            qts = [qt_s[h * HEAD_DIM : (h + 1) * HEAD_DIM, r] for h in range(heads)]
            dots = [dot_ref[0, h * HEAD_DIM : (h + 1) * HEAD_DIM, r] for h in range(heads)]

            def block(j, dq):
                c = rows_at(j, BC)
                keep = seg == segr_ref[0:1, c]
                for h in range(heads):
                    hs = slice(h * HEAD_DIM, (h + 1) * HEAD_DIM)
                    s = jnp.where(keep, nn(qb, kt_s[h, :, c]), MASKED)
                    p = jnp.exp(s - lses[h])
                    dp = nn(dob, vt_s[h, :, c])
                    ds = (p * (dp - inner[h])).astype(BF)
                    dq = dq + nn(ds, k_s[h, c, :])
                    kt_f[hs, c] += nn(qts[h], ds)
                    vt_f[hs, c] += nn(dots[h], p.astype(BF))
                return dq

            dq = lax.fori_loop(bounds[0, i], bounds[1, i], block, jnp.zeros(qb.shape, F32))
            dq_s[r, :] = (dq * 0.125).astype(BF)

        dkt_s[...] = kt_f[...].astype(BF)
        dvt_s[...] = vt_f[...].astype(BF)

        @pl.loop(0, tokens // RT)
        def _(i):
            r = rows_at(i, RT)
            ig_ref[r, :] += nn(dq_s[r, :], wq) + tn(dkt_s[:, r], wk) + tn(dvt_s[:, r], wv)

        x = x_ref[...]
        dwq_ref[0] = tn(dq_s[...], x).astype(BF)
        dwk_ref[0] = nn(dkt_s[...], x).astype(BF)
        dwv_ref[0] = nn(dvt_s[...], x).astype(BF)
        ones = jnp.ones((8, tokens), BF)
        db_ref[0, 0:8, :] = nn(ones, dq_s[...])
        db_ref[0, 8:16, :] = nt(ones, dvt_s[...])


def normal_parts(value):
    phi = jnp.exp(-0.5 * value * value) * (1.0 / math.sqrt(2.0 * math.pi))
    cum = 0.5 + 0.5 * lax.erf(value * math.sqrt(0.5))
    return cum, phi


def middle(scal, x_ref, ctx_ref, wo_ref, e_ref, s_ref, vec_ref, eb_ref, c_ref,
           lo_ref, s1g_ref, do_ref, dot_ref, dwo_ref, vg_ref, ebg_ref, de_hbm, ds_hbm,
           nl_s, n1_s, r1_s, br_s, act_s, gp_s, ug_s, bg_s, stage, sems):
    tokens, width = x_ref.shape
    used = scal[0] + 1
    tiles = tokens // RT
    ob, sb = vec_ref[2:3, :], vec_ref[3:4, :]
    g1, b1 = vec_ref[4:5, :], vec_ref[5:6, :]
    g2, b2 = vec_ref[6:7, :], vec_ref[7:8, :]

    def mean(v):
        return jnp.sum(v, axis=1, keepdims=True) * (1.0 / width)

    @pl.loop(0, tiles)
    def _(i):
        r = rows_at(i, RT)
        total = lax.fori_loop(
            0, used, lambda q, t: t + nn(ctx_ref[q, r, :], wo_ref[q]), jnp.zeros((RT, width), F32))
        v = x_ref[r, :].astype(F32) + (total + ob)
        v = v - mean(v)
        rstd = lax.rsqrt(mean(v * v) + norm_eps)
        n = v * rstd
        n1_s[r, :] = n
        r1_s[r, :] = jnp.broadcast_to(rstd, (RT, 128))
        normed = n * g1 + b1
        nl_s[r, :] = normed.astype(BF)
        br_s[r, :] = normed + sb

    @pl.loop(0, used)
    def _(q):
        @pl.loop(0, tiles)
        def _(i):
            r = rows_at(i, RT)
            u = nt(nl_s[r, :], e_ref[q]) + eb_ref[q, 0:1, :]
            cum, phi = normal_parts(u)
            act = (u * cum).astype(BF)
            act_s[q, r, :] = act
            gp_s[q, r, :] = (cum + u * phi).astype(BF)
            br_s[r, :] += nn(act, s_ref[q])

    zero = jnp.zeros((1, width), F32)

    def second_norm(i, sums):
        r = rows_at(i, RT)
        v = br_s[r, :]
        v = v - mean(v)
        rstd = lax.rsqrt(mean(v * v) + norm_eps)
        n = v * rstd
        lo_ref[r, :] = (n * g2 + b2).astype(BF)
        c = c_ref[r, :].astype(F32)
        m = c * g2
        g = rstd * (m - mean(m) - n * mean(m * n))
        s1g_ref[r, :] = g
        bg = g.astype(BF)
        bg_s[r, :] = bg
        return (sums[0] + jnp.sum(c * n, axis=0, keepdims=True),
                sums[1] + jnp.sum(c, axis=0, keepdims=True),
                sums[2] + jnp.sum(bg.astype(F32), axis=0, keepdims=True))

    g2g, b2g, sbg = lax.fori_loop(0, tiles, second_norm, (zero, zero, zero))
    vg_ref[6:7, :] = g2g
    vg_ref[7:8, :] = b2g
    vg_ref[3:4, :] = sbg

    def moved(kind, q, out_hbm):
        return pltpu.make_async_copy(stage.at[kind], out_hbm.at[q], sems.at[kind])

    @pl.loop(0, used)
    def _(q):
        def tile(i, total):
            r = rows_at(i, RT)
            d = nt(bg_s[r, :], s_ref[q]) * gp_s[q, r, :].astype(F32)
            ug = d.astype(BF)
            ug_s[r, :] = ug
            s1g_ref[r, :] += nn(ug, e_ref[q])
            return total + jnp.sum(ug.astype(F32), axis=0, keepdims=True)

        ebg_ref[q, 0:1, :] = lax.fori_loop(0, tiles, tile, zero)

        @pl.when(q > 0)
        def _():
            moved(0, q - 1, de_hbm).wait()
            moved(1, q - 1, ds_hbm).wait()

        for n in range(width // RT):
            cols = slice(n * RT, (n + 1) * RT)
            stage[0, cols, :] = tn(ug_s[:, cols], nl_s[...]).astype(BF)
            stage[1, cols, :] = tn(act_s[q, :, cols], bg_s[...]).astype(BF)
        moved(0, q, de_hbm).start()
        moved(1, q, ds_hbm).start()

    def first_norm(i, sums):
        r = rows_at(i, RT)
        g = s1g_ref[r, :]
        n = n1_s[r, :]
        m = g * g1
        out = r1_s[r, 0:1] * (m - mean(m) - n * mean(m * n))
        s1g_ref[r, :] = out
        ag = out.astype(BF)
        ug_s[r, :] = ag

        @pl.loop(0, used)
        def _(q):
            do_ref[q, r, :] = nt(ag, wo_ref[q]).astype(BF)
            dot_ref[q, :, r] = nt(wo_ref[q], ag).astype(BF)

        return (sums[0] + jnp.sum(g * n, axis=0, keepdims=True),
                sums[1] + jnp.sum(g, axis=0, keepdims=True),
                sums[2] + jnp.sum(ag.astype(F32), axis=0, keepdims=True))

    g1g, b1g, obg = lax.fori_loop(0, tiles, first_norm, (zero, zero, zero))
    vg_ref[4:5, :] = g1g
    vg_ref[5:6, :] = b1g
    vg_ref[2:3, :] = obg

    @pl.loop(0, used)
    def _(q):
        dwo_ref[q] = tn(ctx_ref[q], ug_s[...]).astype(BF)

    moved(0, used - 1, de_hbm).wait()
    moved(1, used - 1, ds_hbm).wait()


def run_middle(scal, x, ctx, wo, e, s, vec, eb, cot):
    groups, feat, width = wo.shape
    tokens = x.shape[0]
    vm = pl.BlockSpec(memory_space=pltpu.VMEM)
    sds = jax.ShapeDtypeStruct
    return pl.pallas_call(
        middle,
        name="middle",
        cost_estimate=pl.CostEstimate(flops=int(50e9), bytes_accessed=int(30e6), transcendentals=0),
        out_shape=(
            sds((tokens, width), BF), sds((tokens, width), F32),
            sds((groups, tokens, feat), BF), sds((groups, feat, tokens), BF),
            sds((groups, feat, width), BF), sds((8, width), F32), sds((groups, 8, width), F32),
            sds(e.shape, BF), sds(s.shape, BF)),
        in_specs=[pl.BlockSpec(memory_space=pltpu.SMEM)] + [vm] * 8,
        out_specs=(vm,) * 7 + (pl.BlockSpec(memory_space=pl.ANY),) * 2,
        scratch_shapes=[
            pltpu.VMEM((tokens, width), BF), pltpu.VMEM((tokens, width), F32),
            pltpu.VMEM((tokens, 128), F32), pltpu.VMEM((tokens, width), F32),
            pltpu.VMEM((groups, tokens, width), BF), pltpu.VMEM((groups, tokens, width), BF),
            pltpu.VMEM((tokens, width), BF), pltpu.VMEM((tokens, width), BF),
            pltpu.VMEM((2, width, width), BF), pltpu.SemaphoreType.DMA((2,))],
        compiler_params=pltpu.CompilerParams(vmem_limit_bytes=62 << 20),
    )(scal, x, ctx, wo, e, s, vec, eb, cot)


def attn_specs(tokens, width, feat):
    def at_quarter(*block):
        return pl.BlockSpec((1,) + block, lambda q, s, b: (jnp.minimum(q, s[0]), 0, 0))

    def whole(*block):
        return pl.BlockSpec(block, lambda q, s, b: (0, 0))

    return at_quarter, whole


def run_fwd(scal, bounds, x, wq, wk, wv, bias, segc, segr):
    groups, feat, width = wq.shape
    tokens = x.shape[0]
    heads = feat // HEAD_DIM
    at_quarter, whole = attn_specs(tokens, width, feat)
    sds = jax.ShapeDtypeStruct
    return pl.pallas_call(
        attn_fwd,
        name="attn_fwd",
        cost_estimate=pl.CostEstimate(flops=int(40e9), bytes_accessed=int(30e6), transcendentals=0),
        out_shape=(sds((groups, tokens, feat), BF), sds((groups, tokens, 128), F32)),
        grid_spec=pltpu.PrefetchScalarGridSpec(
            num_scalar_prefetch=2, grid=(groups,),
            in_specs=[whole(tokens, width)] + [at_quarter(feat, width)] * 3
            + [at_quarter(8, feat), whole(tokens, 128), whole(8, tokens)],
            out_specs=(at_quarter(tokens, feat), at_quarter(tokens, 128)),
            scratch_shapes=[
                pltpu.VMEM((tokens, feat), BF), pltpu.VMEM((heads, feat, tokens), BF),
                pltpu.VMEM((heads, tokens, feat), BF), pltpu.VMEM((heads, BR, tokens), F32),
                pltpu.VMEM((heads, BR, BC), F32)]),
        compiler_params=pltpu.CompilerParams(vmem_limit_bytes=60 << 20),
    )(scal, bounds, x, wq, wk, wv, bias, segc, segr)


def run_bwd(scal, bounds, x, wq, wk, wv, bias, bcol, segc, segr, ctx, lse, do, dot, s1g):
    groups, feat, width = wq.shape
    tokens = x.shape[0]
    heads = feat // HEAD_DIM
    at_quarter, whole = attn_specs(tokens, width, feat)
    sds = jax.ShapeDtypeStruct
    return pl.pallas_call(
        attn_bwd,
        name="attn_bwd",
        cost_estimate=pl.CostEstimate(flops=int(90e9), bytes_accessed=int(30e6), transcendentals=0),
        out_shape=(sds((tokens, width), F32),) + (sds((groups, feat, width), BF),) * 3
        + (sds((groups, 16, feat), F32),),
        grid_spec=pltpu.PrefetchScalarGridSpec(
            num_scalar_prefetch=2, grid=(groups,),
            in_specs=[whole(tokens, width)] + [at_quarter(feat, width)] * 3
            + [at_quarter(8, feat), at_quarter(feat, 128), whole(tokens, 128), whole(8, tokens),
               at_quarter(tokens, feat), at_quarter(tokens, 128), at_quarter(tokens, feat),
               at_quarter(feat, tokens), whole(tokens, width)],
            out_specs=(whole(tokens, width),) + (at_quarter(feat, width),) * 3 + (at_quarter(16, feat),),
            scratch_shapes=[
                pltpu.VMEM((tokens, feat), BF), pltpu.VMEM((feat, tokens), BF),
                pltpu.VMEM((heads, tokens, feat), BF), pltpu.VMEM((heads, feat, tokens), BF),
                pltpu.VMEM((heads, feat, tokens), BF), pltpu.VMEM((tokens, feat), BF),
                pltpu.VMEM((feat, tokens), BF), pltpu.VMEM((feat, tokens), BF),
                pltpu.VMEM((feat, tokens), F32), pltpu.VMEM((feat, tokens), F32)]),
        compiler_params=pltpu.CompilerParams(vmem_limit_bytes=60 << 20),
    )(scal, bounds, x, wq, wk, wv, bias, bcol, segc, segr, ctx, lse, do, dot, s1g)


def columns(array):
    return jnp.broadcast_to(array[:, :, None], array.shape + (128,)).astype(BF)


def gather_all(pack):
    return lax.all_gather(pack, ("width", "tok"), axis=0, tiled=False)


def scatter_all(terms):
    flat = terms.reshape((-1,) + terms.shape[2:])
    return lax.psum_scatter(flat, ("width", "tok"), scatter_dimension=0, tiled=True)[0]


def local(tokens_in, seq_lengths, *rest):
    weights, biases, out_grad = rest[:6], rest[6:15], rest[15]
    groups = lax.axis_size("width")
    shards = lax.axis_size("tok")
    level = lax.axis_index("width")
    tokens, width = tokens_in.shape
    owned = weights[0].shape[0]
    owned_ff = weights[4].shape[0]
    feat = owned * shards
    units = owned_ff * shards

    small = jnp.concatenate(biases)
    small = jnp.pad(small, (0, width - small.shape[0]))[None, :]
    small = jnp.pad(small, ((0, 7), (0, 0)))
    got = gather_all(jnp.concatenate(weights[:3] + (small,), axis=0))
    got = got.reshape((groups, shards) + got.shape[1:])
    late = gather_all(jnp.concatenate(weights[3:], axis=0))
    late = late.reshape((groups, shards) + late.shape[1:])

    def rows(source, lower, count):
        return source[:, :, lower : lower + count].reshape(groups, count * shards, width)

    wq, wk, wv = (rows(got, n * owned, owned) for n in range(3))
    wo = rows(late, 0, owned)
    we, ws = rows(late, owned, owned_ff), rows(late, owned + owned_ff, owned_ff)
    row = got[:, :, 3 * owned]
    sizes = [b.shape[0] for b in biases]
    starts = [sum(sizes[:n]) for n in range(9)]
    vecs = [row[:, :, a : a + n].reshape(groups, n * shards) for a, n in zip(starts, sizes)]
    eb = jnp.pad(vecs[3][:, None, :].astype(F32), ((0, 0), (0, 7), (0, 0)))
    order = [vecs[0], vecs[1], vecs[2], vecs[4]] + vecs[5:]
    vec = jnp.stack([v.reshape(-1) for v in order]).astype(F32)
    bias = jnp.pad(jnp.stack([vecs[0], vecs[1]], axis=1).astype(F32), ((0, 0), (0, 6), (0, 0)))
    bcol = jnp.pad(jnp.stack([vecs[0], vecs[1]], axis=2), ((0, 0), (0, 0), (0, 126)))

    ends = jnp.cumsum(seq_lengths[0])
    positions = jnp.arange(tokens, dtype=jnp.int32)
    segment = jnp.sum((positions[:, None] >= ends[None, :]).astype(jnp.int32), axis=1)
    lows = jnp.sum((segment[None, :] < segment[::BR, None]).astype(jnp.int32), axis=1)
    highs = jnp.sum((segment[None, :] <= segment[BR - 1 :: BR, None]).astype(jnp.int32), axis=1)
    bounds = jnp.stack([lows // BC, (highs + BC - 1) // BC])
    segc = jnp.broadcast_to(segment[:, None], (tokens, 128))
    segr = jnp.broadcast_to(segment[None, :], (8, tokens))
    scal = level[None].astype(jnp.int32)

    ctx, lse = run_fwd(scal, bounds, tokens_in, wq, wk, wv, bias, segc, segr)
    result, s1g, do, dot, dwo, vg, ebg, de, ds = run_middle(
        scal, tokens_in, ctx, wo, we, ws, vec, eb, out_grad[0])
    mine = jnp.arange(groups) <= level

    def pieces(term):
        return term.reshape((groups, shards, -1) + term.shape[2:])

    def split(line):
        return line.reshape(groups, shards, -1)

    def only(term):
        return jnp.where(mine.reshape((groups,) + (1,) * (term.ndim - 1)), term, jnp.zeros_like(term))

    def packed(*terms):
        return only(jnp.concatenate([pieces(t) for t in terms], axis=2))

    first, s1g = lax.optimization_barrier((packed(dwo, de, ds), s1g))
    early = scatter_all(first)
    input_grad, dwq, dwk, dwv, db = run_bwd(
        scal, bounds, tokens_in, wq, wk, wv, bias, bcol, segc, segr, ctx, lse, do, dot, s1g)

    lines = [
        only(split(db[:, 0])), only(split(db[:, 8])), split(vg[2]), only(split(ebg[:, 0])),
        split(vg[3]), split(vg[4]), split(vg[5]), split(vg[6]), split(vg[7])]
    line = jnp.concatenate(lines, axis=2).astype(BF)
    line = jnp.pad(line, ((0, 0), (0, 0), (0, width - line.shape[2])))
    line = jnp.pad(line[:, :, None, :], ((0, 0), (0, 0), (0, 7), (0, 0)))
    second = jnp.concatenate([packed(dwq, dwk, dwv), line], axis=2)
    second, early = lax.optimization_barrier((second, early))
    early = early.astype(F32)
    final = scatter_all(second).astype(F32)
    outs = [final[n * owned : (n + 1) * owned] for n in range(3)]
    outs += [early[:owned], early[owned : owned + owned_ff], early[owned + owned_ff :]]
    last = final[3 * owned]
    outs += [last[a : a + n] for a, n in zip(starts, sizes)]
    return (result[None], input_grad[None]) + tuple(outs)


def solution(mesh):
    both = ("width", "tok")
    placed = (P("tok", None), P("tok", None)) + (P(both, None),) * 6 + (P(both),) * 9
    return jax.shard_map(
        local,
        mesh=mesh,
        in_specs=placed + (P("width", "tok", None),),
        out_specs=(P("width", "tok", None), P("width", "tok", None))
        + (P(both, None),) * 6 + (P(both),) * 9,
        check_vma=False,
    )
```

```python
import functools
import math

import jax
import jax.numpy as jnp
from jax import lax
from jax.experimental import pallas as pl
from jax.experimental.pallas import tpu as pltpu
from jax.sharding import PartitionSpec as P

HEADS = 12
HEAD_DIM = 64
norm_eps = 1e-12
BF = jnp.bfloat16
F32 = jnp.float32
BR = 128
BC = 256
RT = 256
MASKED = -1e30


def nt(left, right):
    return lax.dot_general(left, right, (((1,), (1,)), ((), ())), preferred_element_type=F32)


def tn(left, right):
    return lax.dot_general(left, right, (((0,), (0,)), ((), ())), preferred_element_type=F32)


def nn(left, right):
    return jnp.dot(left, right, preferred_element_type=F32)


def rows_at(index, size):
    return pl.ds(pl.multiple_of(index * size, size), size)


def head_of(shape, axis):
    return lax.broadcasted_iota(jnp.int32, shape, axis) // HEAD_DIM


def attn_fwd(scal, bounds, x_ref, wq_ref, wk_ref, wv_ref, bias_ref, segc_ref, segr_ref,
             ctx_ref, lse_ref, q_s, kt_s, v_s, s_s, m_s):
    heads = q_s.shape[1] // HEAD_DIM
    tokens = x_ref.shape[0]

    @pl.when(pl.program_id(0) <= scal[0])
    def _():
        wq, wk, wv = wq_ref[0], wk_ref[0], wv_ref[0]

        @pl.loop(0, tokens // RT)
        def _(i):
            r = rows_at(i, RT)
            xb = x_ref[r, :]
            q = (nt(xb, wq) + bias_ref[0, 0:1, :]).astype(BF).astype(F32)
            q_s[r, :] = (q * 0.125).astype(BF)
            v = (nt(xb, wv) + bias_ref[0, 1:2, :]).astype(BF)
            kt = nt(wk, xb).astype(BF)
            for h in range(heads):
                v_s[h, r, :] = jnp.where(head_of(v.shape, 1) == h, v, jnp.zeros_like(v))
                kt_s[h, :, r] = jnp.where(head_of(kt.shape, 0) == h, kt, jnp.zeros_like(kt))

        @pl.loop(0, tokens // BR)
        def _(i):
            r = rows_at(i, BR)
            qb = q_s[r, :]
            seg = segc_ref[r, :]
            seg = jnp.concatenate([seg] * (BC // 128), axis=1)
            lo, hi = bounds[0, i], bounds[1, i]
            m_s[...] = jnp.full_like(m_s, MASKED)

            @pl.loop(lo, hi)
            def _(j):
                c = rows_at(j, BC)
                keep = seg == segr_ref[0:1, c]
                for h in range(heads):
                    s = jnp.where(keep, nn(qb, kt_s[h, :, c]), MASKED)
                    s_s[h, :, c] = s
                    m_s[h] = jnp.maximum(m_s[h], s)

            tops = [jnp.max(m_s[h], axis=1, keepdims=True) for h in range(heads)]
            zero = jnp.zeros((BR, 1), F32)

            def second(j, carry):
                out, sums = carry
                c = rows_at(j, BC)
                new = []
                for h in range(heads):
                    e = jnp.exp(s_s[h, :, c] - tops[h])
                    out = out + nn(e.astype(BF), v_s[h, c, :])
                    new.append(sums[h] + jnp.sum(e, axis=1, keepdims=True))
                return out, tuple(new)

            out, sums = lax.fori_loop(
                lo, hi, second, (jnp.zeros((BR, q_s.shape[1]), F32), (zero,) * heads))
            lane = head_of(out.shape, 1)
            div = jnp.broadcast_to(sums[0], out.shape)
            col = lax.broadcasted_iota(jnp.int32, (BR, 128), 1)
            lse = jnp.broadcast_to(tops[0] + jnp.log(sums[0]), (BR, 128))
            for h in range(1, heads):
                div = jnp.where(lane == h, sums[h], div)
                lse = jnp.where(col == h, tops[h] + jnp.log(sums[h]), lse)
            ctx_ref[0, r, :] = (out / div).astype(BF)
            lse_ref[0, r, :] = lse


def attn_bwd(scal, bounds, x_ref, wq_ref, wk_ref, wv_ref, bias_ref, bcol_ref, segc_ref, segr_ref,
             ctx_ref, lse_ref, do_ref, dot_ref, s1g_ref,
             ig_ref, dwq_ref, dwk_ref, dwv_ref, db_ref,
             q_s, qt_s, k_s, kt_s, vt_s, dq_s, dkt_s, dvt_s, kt_f, vt_f):
    heads = q_s.shape[1] // HEAD_DIM
    tokens = x_ref.shape[0]

    @pl.when(pl.program_id(0) == 0)
    def _():
        ig_ref[...] = s1g_ref[...]

    @pl.when(pl.program_id(0) <= scal[0])
    def _():
        wq, wk, wv = wq_ref[0], wk_ref[0], wv_ref[0]
        qcol = bcol_ref[0, :, 0:1].astype(F32)
        vcol = bcol_ref[0, :, 1:2].astype(F32)

        @pl.loop(0, tokens // RT)
        def _(i):
            r = rows_at(i, RT)
            xb = x_ref[r, :]
            q = (nt(xb, wq) + bias_ref[0, 0:1, :]).astype(BF).astype(F32)
            q_s[r, :] = (q * 0.125).astype(BF)
            qt = (nt(wq, xb) + qcol).astype(BF).astype(F32)
            qt_s[:, r] = (qt * 0.125).astype(BF)
            k = nt(xb, wk).astype(BF)
            kt = nt(wk, xb).astype(BF)
            vt = (nt(wv, xb) + vcol).astype(BF)
            for h in range(heads):
                k_s[h, r, :] = jnp.where(head_of(k.shape, 1) == h, k, jnp.zeros_like(k))
                kt_s[h, :, r] = jnp.where(head_of(kt.shape, 0) == h, kt, jnp.zeros_like(kt))
                vt_s[h, :, r] = jnp.where(head_of(vt.shape, 0) == h, vt, jnp.zeros_like(vt))

        kt_f[...] = jnp.zeros_like(kt_f)
        vt_f[...] = jnp.zeros_like(vt_f)

        @pl.loop(0, tokens // BR)
        def _(i):
            r = rows_at(i, BR)
            qb = q_s[r, :]
            dob = do_ref[0, r, :]
            seg = segc_ref[r, :]
            seg = jnp.concatenate([seg] * (BC // 128), axis=1)
            prod = dob.astype(F32) * ctx_ref[0, r, :].astype(F32)
            lane = head_of(prod.shape, 1)
            inner = [jnp.sum(jnp.where(lane == h, prod, 0.0), axis=1, keepdims=True) for h in range(heads)]
            lses = [lse_ref[0, r, h : h + 1] for h in range(heads)]
            qts = [qt_s[h * HEAD_DIM : (h + 1) * HEAD_DIM, r] for h in range(heads)]
            dots = [dot_ref[0, h * HEAD_DIM : (h + 1) * HEAD_DIM, r] for h in range(heads)]

            def block(j, dq):
                c = rows_at(j, BC)
                keep = seg == segr_ref[0:1, c]
                for h in range(heads):
                    hs = slice(h * HEAD_DIM, (h + 1) * HEAD_DIM)
                    s = jnp.where(keep, nn(qb, kt_s[h, :, c]), MASKED)
                    p = jnp.exp(s - lses[h])
                    dp = nn(dob, vt_s[h, :, c])
                    ds = (p * (dp - inner[h])).astype(BF)
                    dq = dq + nn(ds, k_s[h, c, :])
                    kt_f[hs, c] += nn(qts[h], ds)
                    vt_f[hs, c] += nn(dots[h], p.astype(BF))
                return dq

            dq = lax.fori_loop(bounds[0, i], bounds[1, i], block, jnp.zeros(qb.shape, F32))
            dq_s[r, :] = (dq * 0.125).astype(BF)

        dkt_s[...] = kt_f[...].astype(BF)
        dvt_s[...] = vt_f[...].astype(BF)

        @pl.loop(0, tokens // RT)
        def _(i):
            r = rows_at(i, RT)
            ig_ref[r, :] += nn(dq_s[r, :], wq) + tn(dkt_s[:, r], wk) + tn(dvt_s[:, r], wv)

        x = x_ref[...]
        dwq_ref[0] = tn(dq_s[...], x).astype(BF)
        dwk_ref[0] = nn(dkt_s[...], x).astype(BF)
        dwv_ref[0] = nn(dvt_s[...], x).astype(BF)
        ones = jnp.ones((8, tokens), BF)
        db_ref[0, 0:8, :] = nn(ones, dq_s[...])
        db_ref[0, 8:16, :] = nt(ones, dvt_s[...])


def normal_parts(value):
    phi = jnp.exp(-0.5 * value * value) * (1.0 / math.sqrt(2.0 * math.pi))
    cum = 0.5 + 0.5 * lax.erf(value * math.sqrt(0.5))
    return cum, phi


def middle(scal, x_ref, ctx_ref, wo_ref, e_ref, s_ref, vec_ref, eb_ref, c_ref,
           lo_ref, s1g_ref, do_ref, dot_ref, dwo_ref, vg_ref, ebg_ref, de_hbm, ds_hbm,
           nl_s, n1_s, r1_s, br_s, act_s, gp_s, ug_s, bg_s, stage, sems):
    tokens, width = x_ref.shape
    used = scal[0] + 1
    tiles = tokens // RT
    ob, sb = vec_ref[2:3, :], vec_ref[3:4, :]
    g1, b1 = vec_ref[4:5, :], vec_ref[5:6, :]
    g2, b2 = vec_ref[6:7, :], vec_ref[7:8, :]

    def mean(v):
        return jnp.sum(v, axis=1, keepdims=True) * (1.0 / width)

    @pl.loop(0, tiles)
    def _(i):
        r = rows_at(i, RT)
        total = lax.fori_loop(
            0, used, lambda q, t: t + nn(ctx_ref[q, r, :], wo_ref[q]), jnp.zeros((RT, width), F32))
        v = x_ref[r, :].astype(F32) + (total + ob)
        v = v - mean(v)
        rstd = lax.rsqrt(mean(v * v) + norm_eps)
        n = v * rstd
        n1_s[r, :] = n
        r1_s[r, :] = jnp.broadcast_to(rstd, (RT, 128))
        normed = n * g1 + b1
        nl_s[r, :] = normed.astype(BF)
        br_s[r, :] = normed + sb

    @pl.loop(0, used)
    def _(q):
        @pl.loop(0, tiles)
        def _(i):
            r = rows_at(i, RT)
            u = nt(nl_s[r, :], e_ref[q]) + eb_ref[q, 0:1, :]
            cum, phi = normal_parts(u)
            act = (u * cum).astype(BF)
            act_s[q, r, :] = act
            gp_s[q, r, :] = (cum + u * phi).astype(BF)
            br_s[r, :] += nn(act, s_ref[q])

    zero = jnp.zeros((1, width), F32)

    def second_norm(i, sums):
        r = rows_at(i, RT)
        v = br_s[r, :]
        v = v - mean(v)
        rstd = lax.rsqrt(mean(v * v) + norm_eps)
        n = v * rstd
        lo_ref[r, :] = (n * g2 + b2).astype(BF)
        c = c_ref[r, :].astype(F32)
        m = c * g2
        g = rstd * (m - mean(m) - n * mean(m * n))
        s1g_ref[r, :] = g
        bg = g.astype(BF)
        bg_s[r, :] = bg
        return (sums[0] + jnp.sum(c * n, axis=0, keepdims=True),
                sums[1] + jnp.sum(c, axis=0, keepdims=True),
                sums[2] + jnp.sum(bg.astype(F32), axis=0, keepdims=True))

    g2g, b2g, sbg = lax.fori_loop(0, tiles, second_norm, (zero, zero, zero))
    vg_ref[6:7, :] = g2g
    vg_ref[7:8, :] = b2g
    vg_ref[3:4, :] = sbg

    def moved(kind, q, out_hbm):
        return pltpu.make_async_copy(stage.at[kind], out_hbm.at[q], sems.at[kind])

    @pl.loop(0, used)
    def _(q):
        def tile(i, total):
            r = rows_at(i, RT)
            d = nt(bg_s[r, :], s_ref[q]) * gp_s[q, r, :].astype(F32)
            ug = d.astype(BF)
            ug_s[r, :] = ug
            s1g_ref[r, :] += nn(ug, e_ref[q])
            return total + jnp.sum(ug.astype(F32), axis=0, keepdims=True)

        ebg_ref[q, 0:1, :] = lax.fori_loop(0, tiles, tile, zero)

        @pl.when(q > 0)
        def _():
            moved(0, q - 1, de_hbm).wait()
            moved(1, q - 1, ds_hbm).wait()

        for n in range(width // RT):
            cols = slice(n * RT, (n + 1) * RT)
            stage[0, cols, :] = tn(ug_s[:, cols], nl_s[...]).astype(BF)
            stage[1, cols, :] = tn(act_s[q, :, cols], bg_s[...]).astype(BF)
        moved(0, q, de_hbm).start()
        moved(1, q, ds_hbm).start()

    def first_norm(i, sums):
        r = rows_at(i, RT)
        g = s1g_ref[r, :]
        n = n1_s[r, :]
        m = g * g1
        out = r1_s[r, 0:1] * (m - mean(m) - n * mean(m * n))
        s1g_ref[r, :] = out
        ag = out.astype(BF)
        ug_s[r, :] = ag

        @pl.loop(0, used)
        def _(q):
            do_ref[q, r, :] = nt(ag, wo_ref[q]).astype(BF)
            dot_ref[q, :, r] = nt(wo_ref[q], ag).astype(BF)

        return (sums[0] + jnp.sum(g * n, axis=0, keepdims=True),
                sums[1] + jnp.sum(g, axis=0, keepdims=True),
                sums[2] + jnp.sum(ag.astype(F32), axis=0, keepdims=True))

    g1g, b1g, obg = lax.fori_loop(0, tiles, first_norm, (zero, zero, zero))
    vg_ref[4:5, :] = g1g
    vg_ref[5:6, :] = b1g
    vg_ref[2:3, :] = obg

    @pl.loop(0, used)
    def _(q):
        dwo_ref[q] = tn(ctx_ref[q], ug_s[...]).astype(BF)

    moved(0, used - 1, de_hbm).wait()
    moved(1, used - 1, ds_hbm).wait()


def run_middle(scal, x, ctx, wo, e, s, vec, eb, cot):
    groups, feat, width = wo.shape
    tokens = x.shape[0]
    vm = pl.BlockSpec(memory_space=pltpu.VMEM)
    sds = jax.ShapeDtypeStruct
    return pl.pallas_call(
        middle,
        name="middle",
        cost_estimate=pl.CostEstimate(flops=int(50e9), bytes_accessed=int(30e6), transcendentals=0),
        out_shape=(
            sds((tokens, width), BF), sds((tokens, width), F32),
            sds((groups, tokens, feat), BF), sds((groups, feat, tokens), BF),
            sds((groups, feat, width), BF), sds((8, width), F32), sds((groups, 8, width), F32),
            sds(e.shape, BF), sds(s.shape, BF)),
        in_specs=[pl.BlockSpec(memory_space=pltpu.SMEM)] + [vm] * 8,
        out_specs=(vm,) * 7 + (pl.BlockSpec(memory_space=pl.ANY),) * 2,
        scratch_shapes=[
            pltpu.VMEM((tokens, width), BF), pltpu.VMEM((tokens, width), F32),
            pltpu.VMEM((tokens, 128), F32), pltpu.VMEM((tokens, width), F32),
            pltpu.VMEM((groups, tokens, width), BF), pltpu.VMEM((groups, tokens, width), BF),
            pltpu.VMEM((tokens, width), BF), pltpu.VMEM((tokens, width), BF),
            pltpu.VMEM((2, width, width), BF), pltpu.SemaphoreType.DMA((2,))],
        compiler_params=pltpu.CompilerParams(vmem_limit_bytes=62 << 20),
    )(scal, x, ctx, wo, e, s, vec, eb, cot)


def attn_specs(tokens, width, feat):
    def at_quarter(*block):
        return pl.BlockSpec((1,) + block, lambda q, s, b: (jnp.minimum(q, s[0]), 0, 0))

    def whole(*block):
        return pl.BlockSpec(block, lambda q, s, b: (0, 0))

    return at_quarter, whole


def run_fwd(scal, bounds, x, wq, wk, wv, bias, segc, segr):
    groups, feat, width = wq.shape
    tokens = x.shape[0]
    heads = feat // HEAD_DIM
    at_quarter, whole = attn_specs(tokens, width, feat)
    sds = jax.ShapeDtypeStruct
    return pl.pallas_call(
        attn_fwd,
        name="attn_fwd",
        cost_estimate=pl.CostEstimate(flops=int(40e9), bytes_accessed=int(30e6), transcendentals=0),
        out_shape=(sds((groups, tokens, feat), BF), sds((groups, tokens, 128), F32)),
        grid_spec=pltpu.PrefetchScalarGridSpec(
            num_scalar_prefetch=2, grid=(groups,),
            in_specs=[whole(tokens, width)] + [at_quarter(feat, width)] * 3
            + [at_quarter(8, feat), whole(tokens, 128), whole(8, tokens)],
            out_specs=(at_quarter(tokens, feat), at_quarter(tokens, 128)),
            scratch_shapes=[
                pltpu.VMEM((tokens, feat), BF), pltpu.VMEM((heads, feat, tokens), BF),
                pltpu.VMEM((heads, tokens, feat), BF), pltpu.VMEM((heads, BR, tokens), F32),
                pltpu.VMEM((heads, BR, BC), F32)]),
        compiler_params=pltpu.CompilerParams(vmem_limit_bytes=60 << 20),
    )(scal, bounds, x, wq, wk, wv, bias, segc, segr)


def run_bwd(scal, bounds, x, wq, wk, wv, bias, bcol, segc, segr, ctx, lse, do, dot, s1g):
    groups, feat, width = wq.shape
    tokens = x.shape[0]
    heads = feat // HEAD_DIM
    at_quarter, whole = attn_specs(tokens, width, feat)
    sds = jax.ShapeDtypeStruct
    return pl.pallas_call(
        attn_bwd,
        name="attn_bwd",
        cost_estimate=pl.CostEstimate(flops=int(90e9), bytes_accessed=int(30e6), transcendentals=0),
        out_shape=(sds((tokens, width), F32),) + (sds((groups, feat, width), BF),) * 3
        + (sds((groups, 16, feat), F32),),
        grid_spec=pltpu.PrefetchScalarGridSpec(
            num_scalar_prefetch=2, grid=(groups,),
            in_specs=[whole(tokens, width)] + [at_quarter(feat, width)] * 3
            + [at_quarter(8, feat), at_quarter(feat, 128), whole(tokens, 128), whole(8, tokens),
               at_quarter(tokens, feat), at_quarter(tokens, 128), at_quarter(tokens, feat),
               at_quarter(feat, tokens), whole(tokens, width)],
            out_specs=(whole(tokens, width),) + (at_quarter(feat, width),) * 3 + (at_quarter(16, feat),),
            scratch_shapes=[
                pltpu.VMEM((tokens, feat), BF), pltpu.VMEM((feat, tokens), BF),
                pltpu.VMEM((heads, tokens, feat), BF), pltpu.VMEM((heads, feat, tokens), BF),
                pltpu.VMEM((heads, feat, tokens), BF), pltpu.VMEM((tokens, feat), BF),
                pltpu.VMEM((feat, tokens), BF), pltpu.VMEM((feat, tokens), BF),
                pltpu.VMEM((feat, tokens), F32), pltpu.VMEM((feat, tokens), F32)]),
        compiler_params=pltpu.CompilerParams(vmem_limit_bytes=60 << 20),
    )(scal, bounds, x, wq, wk, wv, bias, bcol, segc, segr, ctx, lse, do, dot, s1g)


PART = 16


def peer_copy(src, dst, send, recv, **where):
    return pltpu.make_async_remote_copy(
        src_ref=src, dst_ref=dst, send_sem=send, recv_sem=recv,
        device_id=where, device_id_type=pl.DeviceIdType.MESH)


def greet(w, t):
    barrier = pltpu.get_barrier_semaphore()
    mesh_id = pl.DeviceIdType.MESH
    pl.semaphore_signal(barrier, inc=1, device_id={"width": w ^ 1, "tok": t}, device_id_type=mesh_id)
    pl.semaphore_signal(barrier, inc=1, device_id={"width": w ^ 2, "tok": t}, device_id_type=mesh_id)
    pl.semaphore_signal(barrier, inc=1, device_id={"width": w, "tok": t ^ 1}, device_id_type=mesh_id)
    for k in range(1, 4):
        other = lax.rem(t + 2 * k, 8)
        pl.semaphore_signal(barrier, inc=1, device_id={"width": w, "tok": other}, device_id_type=mesh_id)
    pl.semaphore_wait(barrier, 6)


def reduce_kernel(g_ref, out_ref, ra, sx, rx, acc, ry, sy, rz,
                  sa_sem, ra_sem, sx_sem, rx_sem, sy_sem, ry_sem, sz_sem, rz_sem):
    w = lax.axis_index("width")
    t = lax.axis_index("tok")
    y = lax.rem(t, 2)
    z = lax.div(t, 2)
    parts = g_ref.shape[3] // PART
    greet(w, t)

    def rows(p):
        return pl.ds(pl.multiple_of(p * PART, PART), PART)

    def near(p, slot, quarter):
        return peer_copy(g_ref.at[quarter, :, :, rows(p), :], ra.at[slot, :, :, rows(p), :],
                         sa_sem.at[slot, p], ra_sem.at[slot, p], width=w ^ 1, tok=t)

    def across(p):
        return peer_copy(sx.at[:, :, rows(p), :], rx.at[:, :, rows(p), :],
                         sx_sem.at[p], rx_sem.at[p], width=w ^ 2, tok=t)

    def beside(p):
        return peer_copy(acc.at[:, 1 - y, rows(p), :], ry.at[:, rows(p), :],
                         sy_sem.at[p], ry_sem.at[p], width=w, tok=t ^ 1)

    def along(p, k):
        there = lax.rem(z + k, 4)
        return peer_copy(sy.at[there, rows(p), :], rz.at[k - 1, rows(p), :],
                         sz_sem.at[k - 1, p], rz_sem.at[k - 1, p], width=w, tok=2 * there + y)

    @pl.loop(0, parts)
    def _(p):
        @pl.when(w == 3)
        def _():
            near(p, 0, 0).start()

        @pl.when(w == 2)
        def _():
            near(p, 0, 1).start()

    @pl.loop(0, parts)
    def _(p):
        @pl.when(w == 3)
        def _():
            near(p, 1, 2).start()

        @pl.when(w == 1)
        def _():
            near(p, 0, 0).start()

    @pl.loop(0, parts)
    def _(p):
        @pl.when(w >= 2)
        def _():
            near(p, 0, 0).wait_recv()
            far = w - 2
            sx[:, :, rows(p), :] = (g_ref[far, :, :, rows(p), :].astype(F32)
                                    + ra[0, :, :, rows(p), :].astype(F32)).astype(BF)
            across(p).start()

    @pl.loop(0, parts)
    def _(p):
        total = g_ref[w, :, :, rows(p), :].astype(F32)
        acc[:, :, rows(p), :] = total.astype(BF)

        @pl.when(w == 2)
        def _():
            near(p, 1, 2).wait_recv()
            acc[:, :, rows(p), :] = (g_ref[w, :, :, rows(p), :].astype(F32)
                                     + ra[1, :, :, rows(p), :].astype(F32)).astype(BF)

        @pl.when(w == 1)
        def _():
            across(p).wait_recv()
            acc[:, :, rows(p), :] = (g_ref[w, :, :, rows(p), :].astype(F32)
                                     + rx[:, :, rows(p), :].astype(F32)).astype(BF)

        @pl.when(w == 0)
        def _():
            near(p, 0, 0).wait_recv()
            across(p).wait_recv()
            acc[:, :, rows(p), :] = (g_ref[w, :, :, rows(p), :].astype(F32)
                                     + ra[0, :, :, rows(p), :].astype(F32)
                                     + rx[:, :, rows(p), :].astype(F32)).astype(BF)

        beside(p).start()

    @pl.loop(0, parts)
    def _(p):
        beside(p).wait_recv()
        sy[:, rows(p), :] = (acc[:, y, rows(p), :].astype(F32) + ry[:, rows(p), :].astype(F32)).astype(BF)
        for k in range(1, 4):
            along(p, k).start()

    @pl.loop(0, parts)
    def _(p):
        total = sy[z, rows(p), :].astype(F32)
        for k in range(1, 4):
            along(p, k).wait_recv()
            total = total + rz[k - 1, rows(p), :].astype(F32)
        out_ref[rows(p), :] = total

    @pl.loop(0, parts)
    def _(p):
        @pl.when(w == 3)
        def _():
            near(p, 0, 0).wait_send()
            near(p, 1, 2).wait_send()

        @pl.when(w == 2)
        def _():
            near(p, 0, 1).wait_send()

        @pl.when(w == 1)
        def _():
            near(p, 0, 0).wait_send()

        @pl.when(w >= 2)
        def _():
            across(p).wait_send()

        beside(p).wait_send()
        for k in range(1, 4):
            along(p, k).wait_send()


def reduce_fast(terms):
    groups, shards, count, width = terms.shape
    parts = count // PART
    vm = pl.BlockSpec(memory_space=pltpu.VMEM)
    dma = pltpu.SemaphoreType.DMA
    column = (4, 2, count, width)
    return pl.pallas_call(
        reduce_kernel,
        name="reduce_fast",
        out_shape=jax.ShapeDtypeStruct((count, width), F32),
        in_specs=[vm],
        out_specs=vm,
        scratch_shapes=[
            pltpu.VMEM((2,) + column, BF), pltpu.VMEM(column, BF), pltpu.VMEM(column, BF),
            pltpu.VMEM(column, BF), pltpu.VMEM((4, count, width), BF), pltpu.VMEM((4, count, width), BF),
            pltpu.VMEM((3, count, width), BF),
            dma((2, parts)), dma((2, parts)), dma((parts,)), dma((parts,)),
            dma((parts,)), dma((parts,)), dma((3, parts)), dma((3, parts))],
        compiler_params=pltpu.CompilerParams(
            collective_id=1, has_side_effects=True, vmem_limit_bytes=40 << 20),
    )(terms.reshape((groups, 4, 2, count, width)))


def columns(array):
    return jnp.broadcast_to(array[:, :, None], array.shape + (128,)).astype(BF)


def gather_all(pack):
    return lax.all_gather(pack, ("width", "tok"), axis=0, tiled=False)


def scatter_all(terms):
    flat = terms.reshape((-1,) + terms.shape[2:])
    return lax.psum_scatter(flat, ("width", "tok"), scatter_dimension=0, tiled=True)[0]


def local(tokens_in, seq_lengths, *rest):
    weights, biases, out_grad = rest[:6], rest[6:15], rest[15]
    groups = lax.axis_size("width")
    shards = lax.axis_size("tok")
    level = lax.axis_index("width")
    tokens, width = tokens_in.shape
    owned = weights[0].shape[0]
    owned_ff = weights[4].shape[0]
    feat = owned * shards
    units = owned_ff * shards

    small = jnp.concatenate(biases)
    small = jnp.pad(small, (0, width - small.shape[0]))[None, :]
    small = jnp.pad(small, ((0, 7), (0, 0)))
    got = gather_all(jnp.concatenate(weights[:3] + (small,), axis=0))
    got = got.reshape((groups, shards) + got.shape[1:])
    late = gather_all(jnp.concatenate(weights[3:], axis=0))
    late = late.reshape((groups, shards) + late.shape[1:])

    def rows(source, lower, count):
        return source[:, :, lower : lower + count].reshape(groups, count * shards, width)

    wq, wk, wv = (rows(got, n * owned, owned) for n in range(3))
    wo = rows(late, 0, owned)
    we, ws = rows(late, owned, owned_ff), rows(late, owned + owned_ff, owned_ff)
    row = got[:, :, 3 * owned]
    sizes = [b.shape[0] for b in biases]
    starts = [sum(sizes[:n]) for n in range(9)]
    vecs = [row[:, :, a : a + n].reshape(groups, n * shards) for a, n in zip(starts, sizes)]
    eb = jnp.pad(vecs[3][:, None, :].astype(F32), ((0, 0), (0, 7), (0, 0)))
    order = [vecs[0], vecs[1], vecs[2], vecs[4]] + vecs[5:]
    vec = jnp.stack([v.reshape(-1) for v in order]).astype(F32)
    bias = jnp.pad(jnp.stack([vecs[0], vecs[1]], axis=1).astype(F32), ((0, 0), (0, 6), (0, 0)))
    bcol = jnp.pad(jnp.stack([vecs[0], vecs[1]], axis=2), ((0, 0), (0, 0), (0, 126)))

    ends = jnp.cumsum(seq_lengths[0])
    positions = jnp.arange(tokens, dtype=jnp.int32)
    segment = jnp.sum((positions[:, None] >= ends[None, :]).astype(jnp.int32), axis=1)
    lows = jnp.sum((segment[None, :] < segment[::BR, None]).astype(jnp.int32), axis=1)
    highs = jnp.sum((segment[None, :] <= segment[BR - 1 :: BR, None]).astype(jnp.int32), axis=1)
    bounds = jnp.stack([lows // BC, (highs + BC - 1) // BC])
    segc = jnp.broadcast_to(segment[:, None], (tokens, 128))
    segr = jnp.broadcast_to(segment[None, :], (8, tokens))
    scal = level[None].astype(jnp.int32)

    ctx, lse = run_fwd(scal, bounds, tokens_in, wq, wk, wv, bias, segc, segr)
    result, s1g, do, dot, dwo, vg, ebg, de, ds = run_middle(
        scal, tokens_in, ctx, wo, we, ws, vec, eb, out_grad[0])
    mine = jnp.arange(groups) <= level

    def pieces(term):
        return term.reshape((groups, shards, -1) + term.shape[2:])

    def split(line):
        return line.reshape(groups, shards, -1)

    def only(term):
        return jnp.where(mine.reshape((groups,) + (1,) * (term.ndim - 1)), term, jnp.zeros_like(term))

    def packed(*terms):
        return only(jnp.concatenate([pieces(t) for t in terms], axis=2))

    def lined(*lines):
        line = jnp.concatenate(lines, axis=2).astype(BF)
        line = jnp.pad(line, ((0, 0), (0, 0), (0, width - line.shape[2])))
        return jnp.pad(line[:, :, None, :], ((0, 0), (0, 0), (0, 7), (0, 0)))

    line = lined(only(split(ebg[:, 0])), *(split(vg[n]) for n in range(2, 8)))
    first = jnp.concatenate([packed(dwo, de, ds), line], axis=2)
    first, s1g = lax.optimization_barrier((first, s1g))
    early = scatter_all(first)
    input_grad, dwq, dwk, dwv, db = run_bwd(
        scal, bounds, tokens_in, wq, wk, wv, bias, bcol, segc, segr, ctx, lse, do, dot, s1g)

    line = lined(only(split(db[:, 0])), only(split(db[:, 8])))
    second = jnp.concatenate([packed(dwq, dwk, dwv), line], axis=2)
    if groups == 4 and shards == 8 and owned % 8 == 0:
        final = reduce_fast(second)
    else:
        final = scatter_all(second).astype(F32)
    early = early.astype(F32)
    outs = [final[n * owned : (n + 1) * owned] for n in range(3)]
    outs += [early[:owned], early[owned : owned + owned_ff], early[owned + owned_ff : owned + 2 * owned_ff]]
    late = final[3 * owned]
    soon = early[owned + 2 * owned_ff]
    vecs = [soon[owned_ff + n * owned : owned_ff + (n + 1) * owned] for n in range(6)]
    outs += [late[:owned], late[owned : 2 * owned], vecs[0], soon[:owned_ff]] + vecs[1:]
    return (result[None], input_grad[None]) + tuple(outs)


def solution(mesh):
    both = ("width", "tok")
    placed = (P("tok", None), P("tok", None)) + (P(both, None),) * 6 + (P(both),) * 9
    return jax.shard_map(
        local,
        mesh=mesh,
        in_specs=placed + (P("width", "tok", None),),
        out_specs=(P("width", "tok", None), P("width", "tok", None))
        + (P(both, None),) * 6 + (P(both),) * 9,
        check_vma=False,
    )
```

```python
import functools
import math

import jax
import jax.numpy as jnp
from jax import lax
from jax.experimental import pallas as pl
from jax.experimental.pallas import tpu as pltpu
from jax.sharding import PartitionSpec as P

HEADS = 12
HEAD_DIM = 64
norm_eps = 1e-12
BF = jnp.bfloat16
F32 = jnp.float32
BR = 128
BC = 256
RT = 256
MASKED = -1e30


def nt(left, right):
    return lax.dot_general(left, right, (((1,), (1,)), ((), ())), preferred_element_type=F32)


def tn(left, right):
    return lax.dot_general(left, right, (((0,), (0,)), ((), ())), preferred_element_type=F32)


def nn(left, right):
    return jnp.dot(left, right, preferred_element_type=F32)


def rows_at(index, size):
    return pl.ds(pl.multiple_of(index * size, size), size)


def head_of(shape, axis):
    return lax.broadcasted_iota(jnp.int32, shape, axis) // HEAD_DIM


def attn_fwd(scal, bounds, x_ref, wq_ref, wk_ref, wv_ref, bias_ref, segc_ref, segr_ref,
             ctx_ref, lse_ref, q_s, kt_s, v_s, s_s, m_s):
    heads = q_s.shape[1] // HEAD_DIM
    tokens = x_ref.shape[0]

    @pl.when(pl.program_id(0) <= scal[0])
    def _():
        wq, wk, wv = wq_ref[0], wk_ref[0], wv_ref[0]

        @pl.loop(0, tokens // RT)
        def _(i):
            r = rows_at(i, RT)
            xb = x_ref[r, :]
            q = (nt(xb, wq) + bias_ref[0, 0:1, :]).astype(BF).astype(F32)
            q_s[r, :] = (q * 0.125).astype(BF)
            v = (nt(xb, wv) + bias_ref[0, 1:2, :]).astype(BF)
            kt = nt(wk, xb).astype(BF)
            for h in range(heads):
                v_s[h, r, :] = jnp.where(head_of(v.shape, 1) == h, v, jnp.zeros_like(v))
                kt_s[h, :, r] = jnp.where(head_of(kt.shape, 0) == h, kt, jnp.zeros_like(kt))

        @pl.loop(0, tokens // BR)
        def _(i):
            r = rows_at(i, BR)
            qb = q_s[r, :]
            seg = segc_ref[r, :]
            seg = jnp.concatenate([seg] * (BC // 128), axis=1)
            lo, hi = bounds[0, i], bounds[1, i]
            m_s[...] = jnp.full_like(m_s, MASKED)

            @pl.loop(lo, hi)
            def _(j):
                c = rows_at(j, BC)
                keep = seg == segr_ref[0:1, c]
                for h in range(heads):
                    s = jnp.where(keep, nn(qb, kt_s[h, :, c]), MASKED)
                    s_s[h, :, c] = s
                    m_s[h] = jnp.maximum(m_s[h], s)

            tops = [jnp.max(m_s[h], axis=1, keepdims=True) for h in range(heads)]
            zero = jnp.zeros((BR, 1), F32)

            def second(j, carry):
                out, sums = carry
                c = rows_at(j, BC)
                new = []
                for h in range(heads):
                    e = jnp.exp(s_s[h, :, c] - tops[h])
                    out = out + nn(e.astype(BF), v_s[h, c, :])
                    new.append(sums[h] + jnp.sum(e, axis=1, keepdims=True))
                return out, tuple(new)

            out, sums = lax.fori_loop(
                lo, hi, second, (jnp.zeros((BR, q_s.shape[1]), F32), (zero,) * heads))
            lane = head_of(out.shape, 1)
            div = jnp.broadcast_to(sums[0], out.shape)
            col = lax.broadcasted_iota(jnp.int32, (BR, 128), 1)
            lse = jnp.broadcast_to(tops[0] + jnp.log(sums[0]), (BR, 128))
            for h in range(1, heads):
                div = jnp.where(lane == h, sums[h], div)
                lse = jnp.where(col == h, tops[h] + jnp.log(sums[h]), lse)
            ctx_ref[0, r, :] = (out / div).astype(BF)
            lse_ref[0, r, :] = lse


def attn_bwd(scal, bounds, x_ref, wq_ref, wk_ref, wv_ref, bias_ref, bcol_ref, segc_ref, segr_ref,
             ctx_ref, lse_ref, do_ref, dot_ref, s1g_ref,
             ig_ref, dwq_ref, dwk_ref, dwv_ref, db_ref,
             q_s, qt_s, k_s, kt_s, vt_s, dq_s, dkt_s, dvt_s, kt_f, vt_f):
    heads = q_s.shape[1] // HEAD_DIM
    tokens = x_ref.shape[0]

    @pl.when(pl.program_id(0) == 0)
    def _():
        ig_ref[...] = s1g_ref[...]

    @pl.when(pl.program_id(0) <= scal[0])
    def _():
        wq, wk, wv = wq_ref[0], wk_ref[0], wv_ref[0]
        qcol = bcol_ref[0, :, 0:1].astype(F32)
        vcol = bcol_ref[0, :, 1:2].astype(F32)

        @pl.loop(0, tokens // RT)
        def _(i):
            r = rows_at(i, RT)
            xb = x_ref[r, :]
            q = (nt(xb, wq) + bias_ref[0, 0:1, :]).astype(BF).astype(F32)
            q_s[r, :] = (q * 0.125).astype(BF)
            qt = (nt(wq, xb) + qcol).astype(BF).astype(F32)
            qt_s[:, r] = (qt * 0.125).astype(BF)
            k = nt(xb, wk).astype(BF)
            kt = nt(wk, xb).astype(BF)
            vt = (nt(wv, xb) + vcol).astype(BF)
            for h in range(heads):
                k_s[h, r, :] = jnp.where(head_of(k.shape, 1) == h, k, jnp.zeros_like(k))
                kt_s[h, :, r] = jnp.where(head_of(kt.shape, 0) == h, kt, jnp.zeros_like(kt))
                vt_s[h, :, r] = jnp.where(head_of(vt.shape, 0) == h, vt, jnp.zeros_like(vt))

        kt_f[...] = jnp.zeros_like(kt_f)
        vt_f[...] = jnp.zeros_like(vt_f)

        @pl.loop(0, tokens // BR)
        def _(i):
            r = rows_at(i, BR)
            qb = q_s[r, :]
            dob = do_ref[0, r, :]
            seg = segc_ref[r, :]
            seg = jnp.concatenate([seg] * (BC // 128), axis=1)
            prod = dob.astype(F32) * ctx_ref[0, r, :].astype(F32)
            lane = head_of(prod.shape, 1)
            inner = [jnp.sum(jnp.where(lane == h, prod, 0.0), axis=1, keepdims=True) for h in range(heads)]
            lses = [lse_ref[0, r, h : h + 1] for h in range(heads)]
            qts = [qt_s[h * HEAD_DIM : (h + 1) * HEAD_DIM, r] for h in range(heads)]
            dots = [dot_ref[0, h * HEAD_DIM : (h + 1) * HEAD_DIM, r] for h in range(heads)]

            def block(j, dq):
                c = rows_at(j, BC)
                keep = seg == segr_ref[0:1, c]
                for h in range(heads):
                    hs = slice(h * HEAD_DIM, (h + 1) * HEAD_DIM)
                    s = jnp.where(keep, nn(qb, kt_s[h, :, c]), MASKED)
                    p = jnp.exp(s - lses[h])
                    dp = nn(dob, vt_s[h, :, c])
                    ds = (p * (dp - inner[h])).astype(BF)
                    dq = dq + nn(ds, k_s[h, c, :])
                    kt_f[hs, c] += nn(qts[h], ds)
                    vt_f[hs, c] += nn(dots[h], p.astype(BF))
                return dq

            dq = lax.fori_loop(bounds[0, i], bounds[1, i], block, jnp.zeros(qb.shape, F32))
            dq_s[r, :] = (dq * 0.125).astype(BF)

        dkt_s[...] = kt_f[...].astype(BF)
        dvt_s[...] = vt_f[...].astype(BF)

        @pl.loop(0, tokens // RT)
        def _(i):
            r = rows_at(i, RT)
            ig_ref[r, :] += nn(dq_s[r, :], wq) + tn(dkt_s[:, r], wk) + tn(dvt_s[:, r], wv)

        x = x_ref[...]
        dwq_ref[0] = tn(dq_s[...], x).astype(BF)
        dwk_ref[0] = nn(dkt_s[...], x).astype(BF)
        dwv_ref[0] = nn(dvt_s[...], x).astype(BF)
        ones = jnp.ones((8, tokens), BF)
        db_ref[0, 0:8, :] = nn(ones, dq_s[...])
        db_ref[0, 8:16, :] = nt(ones, dvt_s[...])


def normal_parts(value):
    phi = jnp.exp(-0.5 * value * value) * (1.0 / math.sqrt(2.0 * math.pi))
    cum = 0.5 + 0.5 * lax.erf(value * math.sqrt(0.5))
    return cum, phi


def middle(scal, x_ref, ctx_ref, wo_ref, e_ref, s_ref, vec_ref, eb_ref, c_ref,
           lo_ref, s1g_ref, do_ref, dot_ref, dwo_ref, vg_ref, ebg_ref, de_hbm, ds_hbm,
           nl_s, n1_s, r1_s, br_s, act_s, gp_s, ug_s, bg_s, stage, sems):
    tokens, width = x_ref.shape
    used = scal[0] + 1
    tiles = tokens // RT
    ob, sb = vec_ref[2:3, :], vec_ref[3:4, :]
    g1, b1 = vec_ref[4:5, :], vec_ref[5:6, :]
    g2, b2 = vec_ref[6:7, :], vec_ref[7:8, :]

    def mean(v):
        return jnp.sum(v, axis=1, keepdims=True) * (1.0 / width)

    @pl.loop(0, tiles)
    def _(i):
        r = rows_at(i, RT)
        total = lax.fori_loop(
            0, used, lambda q, t: t + nn(ctx_ref[q, r, :], wo_ref[q]), jnp.zeros((RT, width), F32))
        v = x_ref[r, :].astype(F32) + (total + ob)
        v = v - mean(v)
        rstd = lax.rsqrt(mean(v * v) + norm_eps)
        n = v * rstd
        n1_s[r, :] = n
        r1_s[r, :] = jnp.broadcast_to(rstd, (RT, 128))
        normed = n * g1 + b1
        nl_s[r, :] = normed.astype(BF)
        br_s[r, :] = normed + sb

    @pl.loop(0, used)
    def _(q):
        @pl.loop(0, tiles)
        def _(i):
            r = rows_at(i, RT)
            u = nt(nl_s[r, :], e_ref[q]) + eb_ref[q, 0:1, :]
            cum, phi = normal_parts(u)
            act = (u * cum).astype(BF)
            act_s[q, r, :] = act
            gp_s[q, r, :] = (cum + u * phi).astype(BF)
            br_s[r, :] += nn(act, s_ref[q])

    zero = jnp.zeros((1, width), F32)

    def second_norm(i, sums):
        r = rows_at(i, RT)
        v = br_s[r, :]
        v = v - mean(v)
        rstd = lax.rsqrt(mean(v * v) + norm_eps)
        n = v * rstd
        lo_ref[r, :] = (n * g2 + b2).astype(BF)
        c = c_ref[r, :].astype(F32)
        m = c * g2
        g = rstd * (m - mean(m) - n * mean(m * n))
        s1g_ref[r, :] = g
        bg = g.astype(BF)
        bg_s[r, :] = bg
        return (sums[0] + jnp.sum(c * n, axis=0, keepdims=True),
                sums[1] + jnp.sum(c, axis=0, keepdims=True),
                sums[2] + jnp.sum(bg.astype(F32), axis=0, keepdims=True))

    g2g, b2g, sbg = lax.fori_loop(0, tiles, second_norm, (zero, zero, zero))
    vg_ref[6:7, :] = g2g
    vg_ref[7:8, :] = b2g
    vg_ref[3:4, :] = sbg

    def moved(kind, q, out_hbm):
        return pltpu.make_async_copy(stage.at[kind], out_hbm.at[q], sems.at[kind])

    @pl.loop(0, used)
    def _(q):
        def tile(i, total):
            r = rows_at(i, RT)
            d = nt(bg_s[r, :], s_ref[q]) * gp_s[q, r, :].astype(F32)
            ug = d.astype(BF)
            ug_s[r, :] = ug
            s1g_ref[r, :] += nn(ug, e_ref[q])
            return total + jnp.sum(ug.astype(F32), axis=0, keepdims=True)

        ebg_ref[q, 0:1, :] = lax.fori_loop(0, tiles, tile, zero)

        @pl.when(q > 0)
        def _():
            moved(0, q - 1, de_hbm).wait()
            moved(1, q - 1, ds_hbm).wait()

        for n in range(width // RT):
            cols = slice(n * RT, (n + 1) * RT)
            stage[0, cols, :] = tn(ug_s[:, cols], nl_s[...]).astype(BF)
            stage[1, cols, :] = tn(act_s[q, :, cols], bg_s[...]).astype(BF)
        moved(0, q, de_hbm).start()
        moved(1, q, ds_hbm).start()

    def first_norm(i, sums):
        r = rows_at(i, RT)
        g = s1g_ref[r, :]
        n = n1_s[r, :]
        m = g * g1
        out = r1_s[r, 0:1] * (m - mean(m) - n * mean(m * n))
        s1g_ref[r, :] = out
        ag = out.astype(BF)
        ug_s[r, :] = ag

        @pl.loop(0, used)
        def _(q):
            do_ref[q, r, :] = nt(ag, wo_ref[q]).astype(BF)
            dot_ref[q, :, r] = nt(wo_ref[q], ag).astype(BF)

        return (sums[0] + jnp.sum(g * n, axis=0, keepdims=True),
                sums[1] + jnp.sum(g, axis=0, keepdims=True),
                sums[2] + jnp.sum(ag.astype(F32), axis=0, keepdims=True))

    g1g, b1g, obg = lax.fori_loop(0, tiles, first_norm, (zero, zero, zero))
    vg_ref[4:5, :] = g1g
    vg_ref[5:6, :] = b1g
    vg_ref[2:3, :] = obg

    @pl.loop(0, used)
    def _(q):
        dwo_ref[q] = tn(ctx_ref[q], ug_s[...]).astype(BF)

    moved(0, used - 1, de_hbm).wait()
    moved(1, used - 1, ds_hbm).wait()


def run_middle(scal, x, ctx, wo, e, s, vec, eb, cot):
    groups, feat, width = wo.shape
    tokens = x.shape[0]
    vm = pl.BlockSpec(memory_space=pltpu.VMEM)
    sds = jax.ShapeDtypeStruct
    return pl.pallas_call(
        middle,
        name="middle",
        cost_estimate=pl.CostEstimate(flops=int(50e9), bytes_accessed=int(30e6), transcendentals=0),
        out_shape=(
            sds((tokens, width), BF), sds((tokens, width), F32),
            sds((groups, tokens, feat), BF), sds((groups, feat, tokens), BF),
            sds((groups, feat, width), BF), sds((8, width), F32), sds((groups, 8, width), F32),
            sds(e.shape, BF), sds(s.shape, BF)),
        in_specs=[pl.BlockSpec(memory_space=pltpu.SMEM)] + [vm] * 8,
        out_specs=(vm,) * 7 + (pl.BlockSpec(memory_space=pl.ANY),) * 2,
        scratch_shapes=[
            pltpu.VMEM((tokens, width), BF), pltpu.VMEM((tokens, width), F32),
            pltpu.VMEM((tokens, 128), F32), pltpu.VMEM((tokens, width), F32),
            pltpu.VMEM((groups, tokens, width), BF), pltpu.VMEM((groups, tokens, width), BF),
            pltpu.VMEM((tokens, width), BF), pltpu.VMEM((tokens, width), BF),
            pltpu.VMEM((2, width, width), BF), pltpu.SemaphoreType.DMA((2,))],
        compiler_params=pltpu.CompilerParams(vmem_limit_bytes=62 << 20),
    )(scal, x, ctx, wo, e, s, vec, eb, cot)


def attn_specs(tokens, width, feat):
    def at_quarter(*block):
        return pl.BlockSpec((1,) + block, lambda q, s, b: (jnp.minimum(q, s[0]), 0, 0))

    def whole(*block):
        return pl.BlockSpec(block, lambda q, s, b: (0, 0))

    return at_quarter, whole


def weight_specs(groups, feat, width):
    def one(kind):
        return pl.BlockSpec((1, feat, width), lambda q, s, b: (kind * groups + jnp.minimum(q, s[0]), 0, 0))

    return [one(kind) for kind in range(3)]


def run_fwd(scal, bounds, x, wqkv, bias, segc, segr):
    groups, feat, width = wqkv.shape[0] // 3, wqkv.shape[1], wqkv.shape[2]
    tokens = x.shape[0]
    heads = feat // HEAD_DIM
    at_quarter, whole = attn_specs(tokens, width, feat)
    sds = jax.ShapeDtypeStruct
    return pl.pallas_call(
        attn_fwd,
        name="attn_fwd",
        cost_estimate=pl.CostEstimate(flops=int(40e9), bytes_accessed=int(30e6), transcendentals=0),
        out_shape=(sds((groups, tokens, feat), BF), sds((groups, tokens, 128), F32)),
        grid_spec=pltpu.PrefetchScalarGridSpec(
            num_scalar_prefetch=2, grid=(groups,),
            in_specs=[whole(tokens, width)] + weight_specs(groups, feat, width)
            + [at_quarter(8, feat), whole(tokens, 128), whole(8, tokens)],
            out_specs=(at_quarter(tokens, feat), at_quarter(tokens, 128)),
            scratch_shapes=[
                pltpu.VMEM((tokens, feat), BF), pltpu.VMEM((heads, feat, tokens), BF),
                pltpu.VMEM((heads, tokens, feat), BF), pltpu.VMEM((heads, BR, tokens), F32),
                pltpu.VMEM((heads, BR, BC), F32)]),
        compiler_params=pltpu.CompilerParams(vmem_limit_bytes=60 << 20),
    )(scal, bounds, x, wqkv, wqkv, wqkv, bias, segc, segr)


def run_bwd(scal, bounds, x, wqkv, bias, bcol, segc, segr, ctx, lse, do, dot, s1g):
    groups, feat, width = wqkv.shape[0] // 3, wqkv.shape[1], wqkv.shape[2]
    tokens = x.shape[0]
    heads = feat // HEAD_DIM
    at_quarter, whole = attn_specs(tokens, width, feat)
    sds = jax.ShapeDtypeStruct
    return pl.pallas_call(
        attn_bwd,
        name="attn_bwd",
        cost_estimate=pl.CostEstimate(flops=int(90e9), bytes_accessed=int(30e6), transcendentals=0),
        out_shape=(sds((tokens, width), F32),) + (sds((groups, feat, width), BF),) * 3
        + (sds((groups, 16, feat), F32),),
        grid_spec=pltpu.PrefetchScalarGridSpec(
            num_scalar_prefetch=2, grid=(groups,),
            in_specs=[whole(tokens, width)] + weight_specs(groups, feat, width)
            + [at_quarter(8, feat), at_quarter(feat, 128), whole(tokens, 128), whole(8, tokens),
               at_quarter(tokens, feat), at_quarter(tokens, 128), at_quarter(tokens, feat),
               at_quarter(feat, tokens), whole(tokens, width)],
            out_specs=(whole(tokens, width),) + (at_quarter(feat, width),) * 3 + (at_quarter(16, feat),),
            scratch_shapes=[
                pltpu.VMEM((tokens, feat), BF), pltpu.VMEM((feat, tokens), BF),
                pltpu.VMEM((heads, tokens, feat), BF), pltpu.VMEM((heads, feat, tokens), BF),
                pltpu.VMEM((heads, feat, tokens), BF), pltpu.VMEM((tokens, feat), BF),
                pltpu.VMEM((feat, tokens), BF), pltpu.VMEM((feat, tokens), BF),
                pltpu.VMEM((feat, tokens), F32), pltpu.VMEM((feat, tokens), F32)]),
        compiler_params=pltpu.CompilerParams(vmem_limit_bytes=60 << 20),
    )(scal, bounds, x, wqkv, wqkv, wqkv, bias, bcol, segc, segr, ctx, lse, do, dot, s1g)


PART = 16


def peer_copy(src, dst, send, recv, **where):
    return pltpu.make_async_remote_copy(
        src_ref=src, dst_ref=dst, send_sem=send, recv_sem=recv,
        device_id=where, device_id_type=pl.DeviceIdType.MESH)


def greet(w, t):
    barrier = pltpu.get_barrier_semaphore()
    mesh_id = pl.DeviceIdType.MESH
    pl.semaphore_signal(barrier, inc=1, device_id={"width": w ^ 1, "tok": t}, device_id_type=mesh_id)
    pl.semaphore_signal(barrier, inc=1, device_id={"width": w ^ 2, "tok": t}, device_id_type=mesh_id)
    pl.semaphore_signal(barrier, inc=1, device_id={"width": w, "tok": t ^ 1}, device_id_type=mesh_id)
    for k in range(1, 4):
        other = lax.rem(t + 2 * k, 8)
        pl.semaphore_signal(barrier, inc=1, device_id={"width": w, "tok": other}, device_id_type=mesh_id)
    pl.semaphore_wait(barrier, 6)


def reduce_kernel(g_ref, out_ref, ra, sx, rx, acc, ry, sy, rz,
                  sa_sem, ra_sem, sx_sem, rx_sem, sy_sem, ry_sem, sz_sem, rz_sem):
    w = lax.axis_index("width")
    t = lax.axis_index("tok")
    y = lax.rem(t, 2)
    z = lax.div(t, 2)
    parts = g_ref.shape[3] // PART
    greet(w, t)

    def rows(p):
        return pl.ds(pl.multiple_of(p * PART, PART), PART)

    def near(p, slot, quarter):
        return peer_copy(g_ref.at[quarter, :, :, rows(p), :], ra.at[slot, :, :, rows(p), :],
                         sa_sem.at[slot, p], ra_sem.at[slot, p], width=w ^ 1, tok=t)

    def across(p):
        return peer_copy(sx.at[:, :, rows(p), :], rx.at[:, :, rows(p), :],
                         sx_sem.at[p], rx_sem.at[p], width=w ^ 2, tok=t)

    def beside(p):
        return peer_copy(acc.at[:, 1 - y, rows(p), :], ry.at[:, rows(p), :],
                         sy_sem.at[p], ry_sem.at[p], width=w, tok=t ^ 1)

    def along(p, k):
        there = lax.rem(z + k, 4)
        return peer_copy(sy.at[there, rows(p), :], rz.at[k - 1, rows(p), :],
                         sz_sem.at[k - 1, p], rz_sem.at[k - 1, p], width=w, tok=2 * there + y)

    @pl.loop(0, parts)
    def _(p):
        @pl.when(w == 3)
        def _():
            near(p, 0, 0).start()

        @pl.when(w == 2)
        def _():
            near(p, 0, 1).start()

    @pl.loop(0, parts)
    def _(p):
        @pl.when(w == 3)
        def _():
            near(p, 1, 2).start()

        @pl.when(w == 1)
        def _():
            near(p, 0, 0).start()

    @pl.loop(0, parts)
    def _(p):
        @pl.when(w >= 2)
        def _():
            near(p, 0, 0).wait_recv()
            far = w - 2
            sx[:, :, rows(p), :] = (g_ref[far, :, :, rows(p), :].astype(F32)
                                    + ra[0, :, :, rows(p), :].astype(F32)).astype(BF)
            across(p).start()

    @pl.loop(0, parts)
    def _(p):
        total = g_ref[w, :, :, rows(p), :].astype(F32)
        acc[:, :, rows(p), :] = total.astype(BF)

        @pl.when(w == 2)
        def _():
            near(p, 1, 2).wait_recv()
            acc[:, :, rows(p), :] = (g_ref[w, :, :, rows(p), :].astype(F32)
                                     + ra[1, :, :, rows(p), :].astype(F32)).astype(BF)

        @pl.when(w == 1)
        def _():
            across(p).wait_recv()
            acc[:, :, rows(p), :] = (g_ref[w, :, :, rows(p), :].astype(F32)
                                     + rx[:, :, rows(p), :].astype(F32)).astype(BF)

        @pl.when(w == 0)
        def _():
            near(p, 0, 0).wait_recv()
            across(p).wait_recv()
            acc[:, :, rows(p), :] = (g_ref[w, :, :, rows(p), :].astype(F32)
                                     + ra[0, :, :, rows(p), :].astype(F32)
                                     + rx[:, :, rows(p), :].astype(F32)).astype(BF)

        beside(p).start()

    @pl.loop(0, parts)
    def _(p):
        beside(p).wait_recv()
        sy[:, rows(p), :] = (acc[:, y, rows(p), :].astype(F32) + ry[:, rows(p), :].astype(F32)).astype(BF)
        for k in range(1, 4):
            along(p, k).start()

    @pl.loop(0, parts)
    def _(p):
        total = sy[z, rows(p), :].astype(F32)
        for k in range(1, 4):
            along(p, k).wait_recv()
            total = total + rz[k - 1, rows(p), :].astype(F32)
        out_ref[rows(p), :] = total

    @pl.loop(0, parts)
    def _(p):
        @pl.when(w == 3)
        def _():
            near(p, 0, 0).wait_send()
            near(p, 1, 2).wait_send()

        @pl.when(w == 2)
        def _():
            near(p, 0, 1).wait_send()

        @pl.when(w == 1)
        def _():
            near(p, 0, 0).wait_send()

        @pl.when(w >= 2)
        def _():
            across(p).wait_send()

        beside(p).wait_send()
        for k in range(1, 4):
            along(p, k).wait_send()


def reduce_fast(terms):
    groups, shards, count, width = terms.shape
    parts = count // PART
    vm = pl.BlockSpec(memory_space=pltpu.VMEM)
    dma = pltpu.SemaphoreType.DMA
    column = (4, 2, count, width)
    return pl.pallas_call(
        reduce_kernel,
        name="reduce_fast",
        out_shape=jax.ShapeDtypeStruct((count, width), F32),
        in_specs=[vm],
        out_specs=vm,
        scratch_shapes=[
            pltpu.VMEM((2,) + column, BF), pltpu.VMEM(column, BF), pltpu.VMEM(column, BF),
            pltpu.VMEM(column, BF), pltpu.VMEM((4, count, width), BF), pltpu.VMEM((4, count, width), BF),
            pltpu.VMEM((3, count, width), BF),
            dma((2, parts)), dma((2, parts)), dma((parts,)), dma((parts,)),
            dma((parts,)), dma((parts,)), dma((3, parts)), dma((3, parts))],
        compiler_params=pltpu.CompilerParams(
            collective_id=1, has_side_effects=True, vmem_limit_bytes=40 << 20),
    )(terms.reshape((groups, 4, 2, count, width)))


def gather_kernel(own_ref, line_ref, all_ref, lines_ref, own_sem, recv_sem, z_sem, y_sem, core_sem, x_sem):
    w = lax.axis_index("width")
    t = lax.axis_index("tok")
    y = lax.rem(t, 2)
    z = lax.div(t, 2)
    mine = (pltpu.make_async_copy(own_ref, all_ref.at[:, w, t], own_sem.at[0]),
            pltpu.make_async_copy(line_ref, lines_ref.at[w, t], own_sem.at[1]))
    for copy in mine:
        copy.start()
    greet(w, t)
    for copy in mine:
        copy.wait()

    def both(q, s, sems, **where):
        return (peer_copy(all_ref.at[:, q, s], all_ref.at[:, q, s], sems.at[0], recv_sem.at[0, q, s], **where),
                peer_copy(lines_ref.at[q, s], lines_ref.at[q, s], sems.at[1], recv_sem.at[1, q, s], **where))

    def along(k):
        return both(w, t, z_sem.at[k - 1], width=w, tok=lax.rem(t + 2 * k, 8))

    def beside(zz):
        return both(w, 2 * zz + y, y_sem.at[zz], width=w, tok=t ^ 1)

    def near(q, s):
        return both(q, s, core_sem.at[q, s], width=w ^ 1, tok=t)

    def across(s):
        return both(w, s, x_sem.at[s], width=w ^ 2, tok=t)

    def start(pair):
        for copy in pair:
            copy.start()

    def arrived(q, s):
        for copy in near(q, s):
            copy.wait_recv()

    def sent(pair):
        for copy in pair:
            copy.wait_send()

    def outward(s):
        @pl.when(w <= 1)
        def _():
            start(across(s))

        @pl.when((w == 0) | (w == 2))
        def _():
            start(near(w, s))

    for k in range(1, 4):
        start(along(k))
    start(beside(z))
    outward(t)
    for k in range(1, 4):
        zz = lax.rem(z + k, 4)
        arrived(w, 2 * zz + y)
        start(beside(zz))
        outward(2 * zz + y)

    @pl.loop(0, 4)
    def _(k):
        s = 2 * lax.rem(z + k, 4) + (1 - y)
        arrived(w, s)
        outward(s)

    @pl.loop(0, 8)
    def _(k):
        zz = lax.rem(z + lax.div(k, 2), 4)
        s = 2 * zz + lax.rem(y + k, 2)

        @pl.when(w >= 2)
        def _():
            arrived(w - 2, s)
            start(near(w - 2, s))

    @pl.loop(0, 8)
    def _(s):
        @pl.when((w == 1) | (w == 3))
        def _():
            arrived(w - 1, s)

        @pl.when(w == 3)
        def _():
            arrived(0, s)

        @pl.when(w == 2)
        def _():
            arrived(1, s)

    for k in range(1, 4):
        sent(along(k))

    @pl.loop(0, 4)
    def _(zz):
        sent(beside(zz))

    @pl.loop(0, 8)
    def _(s):
        @pl.when(w <= 1)
        def _():
            sent(across(s))

        @pl.when((w == 0) | (w == 2))
        def _():
            sent(near(w, s))

        @pl.when(w >= 2)
        def _():
            sent(near(w - 2, s))


def gather_fast(own, line):
    kinds, owned, width = own.shape
    hbm = pl.BlockSpec(memory_space=pl.ANY)
    dma = pltpu.SemaphoreType.DMA
    return pl.pallas_call(
        gather_kernel,
        name="gather_fast",
        out_shape=(jax.ShapeDtypeStruct((kinds, 4, 8, owned, width), BF),
                   jax.ShapeDtypeStruct((4, 8) + line.shape, BF)),
        in_specs=[hbm, hbm],
        out_specs=(hbm, hbm),
        scratch_shapes=[dma((2,)), dma((2, 4, 8)), dma((3, 2)), dma((4, 2)), dma((4, 8, 2)), dma((8, 2))],
        compiler_params=pltpu.CompilerParams(collective_id=2, has_side_effects=True),
        cost_estimate=pl.CostEstimate(flops=int(30e9), bytes_accessed=int(30e6), transcendentals=0),
    )(own, line)


def columns(array):
    return jnp.broadcast_to(array[:, :, None], array.shape + (128,)).astype(BF)


def gather_all(pack):
    return lax.all_gather(pack, ("width", "tok"), axis=0, tiled=False)


def scatter_all(terms):
    flat = terms.reshape((-1,) + terms.shape[2:])
    return lax.psum_scatter(flat, ("width", "tok"), scatter_dimension=0, tiled=True)[0]


def local(tokens_in, seq_lengths, *rest):
    weights, biases, out_grad = rest[:6], rest[6:15], rest[15]
    groups = lax.axis_size("width")
    shards = lax.axis_size("tok")
    level = lax.axis_index("width")
    tokens, width = tokens_in.shape
    owned = weights[0].shape[0]
    owned_ff = weights[4].shape[0]
    feat = owned * shards
    units = owned_ff * shards

    def flat(*vectors):
        line = jnp.concatenate(vectors)
        return jnp.pad(line, (0, width - line.shape[0]))[None, :]

    late = gather_all(jnp.concatenate(weights[3:] + (flat(*biases[2:]),), axis=0))
    late = late.reshape((groups, shards) + late.shape[1:])
    soon = jnp.stack(weights[:3])
    line = jnp.concatenate(biases[:2])
    if groups == 4 and shards == 8 and owned % 8 == 0:
        line = jnp.pad(line[None, :], ((0, 7), (0, 128 - line.shape[0])))
        wqkv, line = gather_fast(soon, line)
        line = line[:, :, 0, : 2 * owned]
    else:
        got = gather_all(jnp.concatenate([soon.reshape(3 * owned, width), flat(line)], axis=0))
        wqkv = jnp.swapaxes(got[:, : 3 * owned].reshape(groups * shards, 3, owned, width), 0, 1)
        line = got[:, 3 * owned, : 2 * owned].reshape(groups, shards, 2 * owned)
    wqkv = wqkv.reshape(3 * groups, feat, width)

    def rows(lower, count):
        return late[:, :, lower : lower + count].reshape(groups, count * shards, width)

    wo = rows(0, owned)
    we, ws = rows(owned, owned_ff), rows(owned + owned_ff, owned_ff)
    row = late[:, :, owned + 2 * owned_ff]
    sizes = [b.shape[0] for b in biases[2:]]
    starts = [sum(sizes[:n]) for n in range(7)]
    vecs = [row[:, :, a : a + n].reshape(groups, n * shards) for a, n in zip(starts, sizes)]
    qb = line[:, :, :owned].reshape(groups, feat)
    vb = line[:, :, owned:].reshape(groups, feat)
    eb = jnp.pad(vecs[1][:, None, :].astype(F32), ((0, 0), (0, 7), (0, 0)))
    vec = jnp.stack([v.reshape(-1) for v in [vecs[0], vecs[2]] + vecs[3:]]).astype(F32)
    vec = jnp.pad(vec, ((2, 0), (0, 0)))
    bias = jnp.pad(jnp.stack([qb, vb], axis=1).astype(F32), ((0, 0), (0, 6), (0, 0)))
    bcol = jnp.pad(jnp.stack([qb, vb], axis=2), ((0, 0), (0, 0), (0, 126)))

    ends = jnp.cumsum(seq_lengths[0])
    positions = jnp.arange(tokens, dtype=jnp.int32)
    segment = jnp.sum((positions[:, None] >= ends[None, :]).astype(jnp.int32), axis=1)
    lows = jnp.sum((segment[None, :] < segment[::BR, None]).astype(jnp.int32), axis=1)
    highs = jnp.sum((segment[None, :] <= segment[BR - 1 :: BR, None]).astype(jnp.int32), axis=1)
    bounds = jnp.stack([lows // BC, (highs + BC - 1) // BC])
    segc = jnp.broadcast_to(segment[:, None], (tokens, 128))
    segr = jnp.broadcast_to(segment[None, :], (8, tokens))
    scal = level[None].astype(jnp.int32)

    ctx, lse = run_fwd(scal, bounds, tokens_in, wqkv, bias, segc, segr)
    result, s1g, do, dot, dwo, vg, ebg, de, ds = run_middle(
        scal, tokens_in, ctx, wo, we, ws, vec, eb, out_grad[0])
    mine = jnp.arange(groups) <= level

    def pieces(term):
        return term.reshape((groups, shards, -1) + term.shape[2:])

    def split(line):
        return line.reshape(groups, shards, -1)

    def only(term):
        return jnp.where(mine.reshape((groups,) + (1,) * (term.ndim - 1)), term, jnp.zeros_like(term))

    def packed(*terms):
        return only(jnp.concatenate([pieces(t) for t in terms], axis=2))

    def lined(*lines):
        line = jnp.concatenate(lines, axis=2).astype(BF)
        line = jnp.pad(line, ((0, 0), (0, 0), (0, width - line.shape[2])))
        return jnp.pad(line[:, :, None, :], ((0, 0), (0, 0), (0, 7), (0, 0)))

    line = lined(only(split(ebg[:, 0])), *(split(vg[n]) for n in range(2, 8)))
    first = jnp.concatenate([packed(dwo, de, ds), line], axis=2)
    first, s1g = lax.optimization_barrier((first, s1g))
    early = scatter_all(first)
    input_grad, dwq, dwk, dwv, db = run_bwd(
        scal, bounds, tokens_in, wqkv, bias, bcol, segc, segr, ctx, lse, do, dot, s1g)

    line = lined(only(split(db[:, 0])), only(split(db[:, 8])))
    second = jnp.concatenate([packed(dwq, dwk, dwv), line], axis=2)
    if groups == 4 and shards == 8 and owned % 8 == 0:
        final = reduce_fast(second)
    else:
        final = scatter_all(second).astype(F32)
    early = early.astype(F32)
    outs = [final[n * owned : (n + 1) * owned] for n in range(3)]
    outs += [early[:owned], early[owned : owned + owned_ff], early[owned + owned_ff : owned + 2 * owned_ff]]
    late = final[3 * owned]
    soon = early[owned + 2 * owned_ff]
    vecs = [soon[owned_ff + n * owned : owned_ff + (n + 1) * owned] for n in range(6)]
    outs += [late[:owned], late[owned : 2 * owned], vecs[0], soon[:owned_ff]] + vecs[1:]
    return (result[None], input_grad[None]) + tuple(outs)


def solution(mesh):
    both = ("width", "tok")
    placed = (P("tok", None), P("tok", None)) + (P(both, None),) * 6 + (P(both),) * 9
    return jax.shard_map(
        local,
        mesh=mesh,
        in_specs=placed + (P("width", "tok", None),),
        out_specs=(P("width", "tok", None), P("width", "tok", None))
        + (P(both, None),) * 6 + (P(both),) * 9,
        check_vma=False,
    )
```

```python
import functools
import math

import jax
import jax.numpy as jnp
from jax import lax
from jax.experimental import pallas as pl
from jax.experimental.pallas import tpu as pltpu
from jax.sharding import PartitionSpec as P

HEADS = 12
HEAD_DIM = 64
norm_eps = 1e-12
BF = jnp.bfloat16
F32 = jnp.float32
BR = 128
BC = 256
RT = 256
MASKED = -1e30


def nt(left, right):
    return lax.dot_general(left, right, (((1,), (1,)), ((), ())), preferred_element_type=F32)


def tn(left, right):
    return lax.dot_general(left, right, (((0,), (0,)), ((), ())), preferred_element_type=F32)


def nn(left, right):
    return jnp.dot(left, right, preferred_element_type=F32)


def rows_at(index, size):
    return pl.ds(pl.multiple_of(index * size, size), size)


def head_of(shape, axis):
    return lax.broadcasted_iota(jnp.int32, shape, axis) // HEAD_DIM


def attn_fwd(bounds, x_ref, wq_ref, wk_ref, wv_ref, bias_ref, segc_ref, segr_ref,
             ctx_ref, lse_ref, q_s, kt_s, v_s, s_s, m_s):
    heads = q_s.shape[1] // HEAD_DIM
    tokens = x_ref.shape[0]

    wq, wk, wv = wq_ref[0], wk_ref[0], wv_ref[0]

    @pl.loop(0, tokens // RT)
    def _(i):
        r = rows_at(i, RT)
        xb = x_ref[r, :]
        q = (nt(xb, wq) + bias_ref[0, 0:1, :]).astype(BF).astype(F32)
        q_s[r, :] = (q * 0.125).astype(BF)
        v = (nt(xb, wv) + bias_ref[0, 1:2, :]).astype(BF)
        kt = nt(wk, xb).astype(BF)
        for h in range(heads):
            v_s[h, r, :] = jnp.where(head_of(v.shape, 1) == h, v, jnp.zeros_like(v))
            kt_s[h, :, r] = jnp.where(head_of(kt.shape, 0) == h, kt, jnp.zeros_like(kt))

    @pl.loop(0, tokens // BR)
    def _(i):
        r = rows_at(i, BR)
        qb = q_s[r, :]
        seg = segc_ref[r, :]
        seg = jnp.concatenate([seg] * (BC // 128), axis=1)
        lo, hi = bounds[0, i], bounds[1, i]
        m_s[...] = jnp.full_like(m_s, MASKED)

        @pl.loop(lo, hi)
        def _(j):
            c = rows_at(j, BC)
            keep = seg == segr_ref[0:1, c]
            for h in range(heads):
                s = jnp.where(keep, nn(qb, kt_s[h, :, c]), MASKED)
                s_s[h, :, c] = s
                m_s[h] = jnp.maximum(m_s[h], s)

        tops = [jnp.max(m_s[h], axis=1, keepdims=True) for h in range(heads)]
        zero = jnp.zeros((BR, 1), F32)

        def second(j, carry):
            out, sums = carry
            c = rows_at(j, BC)
            new = []
            for h in range(heads):
                e = jnp.exp(s_s[h, :, c] - tops[h])
                out = out + nn(e.astype(BF), v_s[h, c, :])
                new.append(sums[h] + jnp.sum(e, axis=1, keepdims=True))
            return out, tuple(new)

        out, sums = lax.fori_loop(
            lo, hi, second, (jnp.zeros((BR, q_s.shape[1]), F32), (zero,) * heads))
        lane = head_of(out.shape, 1)
        div = jnp.broadcast_to(sums[0], out.shape)
        col = lax.broadcasted_iota(jnp.int32, (BR, 128), 1)
        lse = jnp.broadcast_to(tops[0] + jnp.log(sums[0]), (BR, 128))
        for h in range(1, heads):
            div = jnp.where(lane == h, sums[h], div)
            lse = jnp.where(col == h, tops[h] + jnp.log(sums[h]), lse)
        ctx_ref[0, r, :] = (out / div).astype(BF)
        lse_ref[0, :, r] = lse.T[0:8, :]


def attn_bwd(scal, bounds, x_ref, wq_ref, wk_ref, wv_ref, bias_ref, bcol_ref, segc_ref, segr_ref,
             ctx_ref, lse_ref, do_ref, dot_ref, s1g_ref,
             ig_ref, dwq_ref, dwk_ref, dwv_ref, db_ref,
             q_s, qt_s, k_s, kt_s, vt_s, dq_s, dkt_s, dvt_s, kt_f, vt_f):
    heads = q_s.shape[1] // HEAD_DIM
    tokens = x_ref.shape[0]

    @pl.when(pl.program_id(0) == 0)
    def _():
        ig_ref[...] = s1g_ref[...]

    @pl.when(pl.program_id(0) <= scal[0])
    def _():
        wq, wk, wv = wq_ref[0], wk_ref[0], wv_ref[0]
        qcol = bcol_ref[0, :, 0:1].astype(F32)
        vcol = bcol_ref[0, :, 1:2].astype(F32)

        @pl.loop(0, tokens // RT)
        def _(i):
            r = rows_at(i, RT)
            xb = x_ref[r, :]
            q = (nt(xb, wq) + bias_ref[0, 0:1, :]).astype(BF).astype(F32)
            q_s[r, :] = (q * 0.125).astype(BF)
            qt = (nt(wq, xb) + qcol).astype(BF).astype(F32)
            qt_s[:, r] = (qt * 0.125).astype(BF)
            k = nt(xb, wk).astype(BF)
            kt = nt(wk, xb).astype(BF)
            vt = (nt(wv, xb) + vcol).astype(BF)
            for h in range(heads):
                k_s[h, r, :] = jnp.where(head_of(k.shape, 1) == h, k, jnp.zeros_like(k))
                kt_s[h, :, r] = jnp.where(head_of(kt.shape, 0) == h, kt, jnp.zeros_like(kt))
                vt_s[h, :, r] = jnp.where(head_of(vt.shape, 0) == h, vt, jnp.zeros_like(vt))

        kt_f[...] = jnp.zeros_like(kt_f)
        vt_f[...] = jnp.zeros_like(vt_f)

        @pl.loop(0, tokens // BR)
        def _(i):
            r = rows_at(i, BR)
            qb = q_s[r, :]
            dob = do_ref[0, r, :]
            seg = segc_ref[r, :]
            seg = jnp.concatenate([seg] * (BC // 128), axis=1)
            prod = dob.astype(F32) * ctx_ref[0, r, :].astype(F32)
            lane = head_of(prod.shape, 1)
            inner = [jnp.sum(jnp.where(lane == h, prod, 0.0), axis=1, keepdims=True) for h in range(heads)]
            stats = jnp.concatenate([lse_ref[0, :, r]] * 16, axis=0).T
            lses = [stats[:, h : h + 1] for h in range(heads)]
            qts = [qt_s[h * HEAD_DIM : (h + 1) * HEAD_DIM, r] for h in range(heads)]
            dots = [dot_ref[0, h * HEAD_DIM : (h + 1) * HEAD_DIM, r] for h in range(heads)]

            def block(j, dq):
                c = rows_at(j, BC)
                keep = seg == segr_ref[0:1, c]
                for h in range(heads):
                    hs = slice(h * HEAD_DIM, (h + 1) * HEAD_DIM)
                    s = jnp.where(keep, nn(qb, kt_s[h, :, c]), MASKED)
                    p = jnp.exp(s - lses[h])
                    dp = nn(dob, vt_s[h, :, c])
                    ds = (p * (dp - inner[h])).astype(BF)
                    dq = dq + nn(ds, k_s[h, c, :])
                    kt_f[hs, c] += nn(qts[h], ds)
                    vt_f[hs, c] += nn(dots[h], p.astype(BF))
                return dq

            dq = lax.fori_loop(bounds[0, i], bounds[1, i], block, jnp.zeros(qb.shape, F32))
            dq_s[r, :] = (dq * 0.125).astype(BF)

        dkt_s[...] = kt_f[...].astype(BF)
        dvt_s[...] = vt_f[...].astype(BF)

        @pl.loop(0, tokens // RT)
        def _(i):
            r = rows_at(i, RT)
            ig_ref[r, :] += nn(dq_s[r, :], wq) + tn(dkt_s[:, r], wk) + tn(dvt_s[:, r], wv)

        x = x_ref[...]
        dwq_ref[0] = tn(dq_s[...], x).astype(BF)
        dwk_ref[0] = nn(dkt_s[...], x).astype(BF)
        dwv_ref[0] = nn(dvt_s[...], x).astype(BF)
        ones = jnp.ones((8, tokens), BF)
        db_ref[0, 0:8, :] = nn(ones, dq_s[...])
        db_ref[0, 8:16, :] = nt(ones, dvt_s[...])


def normal_parts(value):
    phi = jnp.exp(-0.5 * value * value) * (1.0 / math.sqrt(2.0 * math.pi))
    cum = 0.5 + 0.5 * lax.erf(value * math.sqrt(0.5))
    return cum, phi


def middle(scal, x_ref, ctx_ref, wo_ref, e_ref, s_ref, vec_ref, eb_ref, c_ref,
           lo_ref, s1g_ref, do_ref, dot_ref, dwo_ref, vg_ref, ebg_ref, de_hbm, ds_hbm,
           nl_s, n1_s, r1_s, br_s, act_s, gp_s, ug_s, bg_s, stage, sems):
    tokens, width = x_ref.shape
    used = scal[0] + 1
    tiles = tokens // RT
    ob, sb = vec_ref[2:3, :], vec_ref[3:4, :]
    g1, b1 = vec_ref[4:5, :], vec_ref[5:6, :]
    g2, b2 = vec_ref[6:7, :], vec_ref[7:8, :]

    def mean(v):
        return jnp.sum(v, axis=1, keepdims=True) * (1.0 / width)

    @pl.loop(0, tiles)
    def _(i):
        r = rows_at(i, RT)
        total = lax.fori_loop(
            0, used, lambda q, t: t + nn(ctx_ref[q, r, :], wo_ref[q]), jnp.zeros((RT, width), F32))
        v = x_ref[r, :].astype(F32) + (total + ob)
        v = v - mean(v)
        rstd = lax.rsqrt(mean(v * v) + norm_eps)
        n = v * rstd
        n1_s[r, :] = n
        r1_s[r, :] = jnp.broadcast_to(rstd, (RT, 128))
        normed = n * g1 + b1
        nl_s[r, :] = normed.astype(BF)
        br_s[r, :] = normed + sb

    @pl.loop(0, used)
    def _(q):
        @pl.loop(0, tiles)
        def _(i):
            r = rows_at(i, RT)
            u = nt(nl_s[r, :], e_ref[q]) + eb_ref[q, 0:1, :]
            cum, phi = normal_parts(u)
            act = (u * cum).astype(BF)
            act_s[q, r, :] = act
            gp_s[q, r, :] = (cum + u * phi).astype(BF)
            br_s[r, :] += nn(act, s_ref[q])

    zero = jnp.zeros((1, width), F32)

    def second_norm(i, sums):
        r = rows_at(i, RT)
        v = br_s[r, :]
        v = v - mean(v)
        rstd = lax.rsqrt(mean(v * v) + norm_eps)
        n = v * rstd
        lo_ref[r, :] = (n * g2 + b2).astype(BF)
        c = c_ref[r, :].astype(F32)
        m = c * g2
        g = rstd * (m - mean(m) - n * mean(m * n))
        s1g_ref[r, :] = g
        bg = g.astype(BF)
        bg_s[r, :] = bg
        return (sums[0] + jnp.sum(c * n, axis=0, keepdims=True),
                sums[1] + jnp.sum(c, axis=0, keepdims=True),
                sums[2] + jnp.sum(bg.astype(F32), axis=0, keepdims=True))

    g2g, b2g, sbg = lax.fori_loop(0, tiles, second_norm, (zero, zero, zero))
    vg_ref[6:7, :] = g2g
    vg_ref[7:8, :] = b2g
    vg_ref[3:4, :] = sbg

    def moved(kind, q, out_hbm):
        return pltpu.make_async_copy(stage.at[kind], out_hbm.at[q], sems.at[kind])

    @pl.loop(0, used)
    def _(q):
        def tile(i, total):
            r = rows_at(i, RT)
            d = nt(bg_s[r, :], s_ref[q]) * gp_s[q, r, :].astype(F32)
            ug = d.astype(BF)
            ug_s[r, :] = ug
            s1g_ref[r, :] += nn(ug, e_ref[q])
            return total + jnp.sum(ug.astype(F32), axis=0, keepdims=True)

        ebg_ref[q, 0:1, :] = lax.fori_loop(0, tiles, tile, zero)

        @pl.when(q > 0)
        def _():
            moved(0, q - 1, de_hbm).wait()
            moved(1, q - 1, ds_hbm).wait()

        for n in range(width // RT):
            cols = slice(n * RT, (n + 1) * RT)
            stage[0, cols, :] = tn(ug_s[:, cols], nl_s[...]).astype(BF)
            stage[1, cols, :] = tn(act_s[q, :, cols], bg_s[...]).astype(BF)
        moved(0, q, de_hbm).start()
        moved(1, q, ds_hbm).start()

    def first_norm(i, sums):
        r = rows_at(i, RT)
        g = s1g_ref[r, :]
        n = n1_s[r, :]
        m = g * g1
        out = r1_s[r, 0:1] * (m - mean(m) - n * mean(m * n))
        s1g_ref[r, :] = out
        ag = out.astype(BF)
        ug_s[r, :] = ag

        @pl.loop(0, used)
        def _(q):
            do_ref[q, r, :] = nt(ag, wo_ref[q]).astype(BF)
            dot_ref[q, :, r] = nt(wo_ref[q], ag).astype(BF)

        return (sums[0] + jnp.sum(g * n, axis=0, keepdims=True),
                sums[1] + jnp.sum(g, axis=0, keepdims=True),
                sums[2] + jnp.sum(ag.astype(F32), axis=0, keepdims=True))

    g1g, b1g, obg = lax.fori_loop(0, tiles, first_norm, (zero, zero, zero))
    vg_ref[4:5, :] = g1g
    vg_ref[5:6, :] = b1g
    vg_ref[2:3, :] = obg

    @pl.loop(0, used)
    def _(q):
        dwo_ref[q] = tn(ctx_ref[q], ug_s[...]).astype(BF)

    moved(0, used - 1, de_hbm).wait()
    moved(1, used - 1, ds_hbm).wait()


def run_middle(scal, x, ctx, wo, e, s, vec, eb, cot):
    groups, feat, width = wo.shape
    tokens = x.shape[0]
    vm = pl.BlockSpec(memory_space=pltpu.VMEM)
    sds = jax.ShapeDtypeStruct
    return pl.pallas_call(
        middle,
        name="middle",
        cost_estimate=pl.CostEstimate(flops=int(50e9), bytes_accessed=int(30e6), transcendentals=0),
        out_shape=(
            sds((tokens, width), BF), sds((tokens, width), F32),
            sds((groups, tokens, feat), BF), sds((groups, feat, tokens), BF),
            sds((groups, feat, width), BF), sds((8, width), F32), sds((groups, 8, width), F32),
            sds(e.shape, BF), sds(s.shape, BF)),
        in_specs=[pl.BlockSpec(memory_space=pltpu.SMEM)] + [vm] * 8,
        out_specs=(vm,) * 7 + (pl.BlockSpec(memory_space=pl.ANY),) * 2,
        scratch_shapes=[
            pltpu.VMEM((tokens, width), BF), pltpu.VMEM((tokens, width), F32),
            pltpu.VMEM((tokens, 128), F32), pltpu.VMEM((tokens, width), F32),
            pltpu.VMEM((groups, tokens, width), BF), pltpu.VMEM((groups, tokens, width), BF),
            pltpu.VMEM((tokens, width), BF), pltpu.VMEM((tokens, width), BF),
            pltpu.VMEM((2, width, width), BF), pltpu.SemaphoreType.DMA((2,))],
        compiler_params=pltpu.CompilerParams(vmem_limit_bytes=62 << 20),
    )(scal, x, ctx, wo, e, s, vec, eb, cot)


def attn_specs(tokens, width, feat):
    def at_quarter(*block):
        return pl.BlockSpec((1,) + block, lambda q, s, b: (jnp.minimum(q, s[0]), 0, 0))

    def whole(*block):
        return pl.BlockSpec(block, lambda q, s, b: (0, 0))

    return at_quarter, whole


def weight_specs(groups, feat, width):
    def one(kind):
        return pl.BlockSpec((1, feat, width), lambda q, s, b: (jnp.minimum(q, s[0]), kind, 0))

    return [one(kind) for kind in range(3)]


def run_fwd(bounds, x, wqkv, bias, segc, segr):
    feat, width = wqkv.shape[1:]
    tokens = x.shape[0]
    heads = feat // HEAD_DIM

    def part(shape, kind=0):
        return pl.BlockSpec(shape, lambda i, b: (kind,) + (0,) * (len(shape) - 1))

    sds = jax.ShapeDtypeStruct
    return pl.pallas_call(
        attn_fwd,
        name="attn_fwd",
        cost_estimate=pl.CostEstimate(flops=int(10e9), bytes_accessed=int(10e6), transcendentals=0),
        out_shape=(sds((1, tokens, feat), BF), sds((1, 8, tokens), F32)),
        grid_spec=pltpu.PrefetchScalarGridSpec(
            num_scalar_prefetch=1, grid=(1,),
            in_specs=[part((tokens, width))] + [part((1, feat, width), n) for n in range(3)]
            + [part((1, 8, feat)), part((tokens, 128)), part((8, tokens))],
            out_specs=(part((1, tokens, feat)), part((1, 8, tokens))),
            scratch_shapes=[
                pltpu.VMEM((tokens, feat), BF), pltpu.VMEM((heads, feat, tokens), BF),
                pltpu.VMEM((heads, tokens, feat), BF), pltpu.VMEM((heads, BR, tokens), F32),
                pltpu.VMEM((heads, BR, BC), F32)]),
        compiler_params=pltpu.CompilerParams(vmem_limit_bytes=40 << 20),
    )(bounds, x, wqkv, wqkv, wqkv, bias, segc, segr)


def run_bwd(scal, bounds, x, wqkv, bias, bcol, segc, segr, ctx, lse, do, dot, s1g):
    groups, feat, width = wqkv.shape[0], bias.shape[2], wqkv.shape[2]
    tokens = x.shape[0]
    heads = feat // HEAD_DIM
    at_quarter, whole = attn_specs(tokens, width, feat)
    sds = jax.ShapeDtypeStruct
    return pl.pallas_call(
        attn_bwd,
        name="attn_bwd",
        cost_estimate=pl.CostEstimate(flops=int(90e9), bytes_accessed=int(30e6), transcendentals=0),
        out_shape=(sds((tokens, width), F32),) + (sds((groups, feat, width), BF),) * 3
        + (sds((groups, 16, feat), F32),),
        grid_spec=pltpu.PrefetchScalarGridSpec(
            num_scalar_prefetch=2, grid=(groups,),
            in_specs=[whole(tokens, width)] + weight_specs(groups, feat, width)
            + [at_quarter(8, feat), at_quarter(feat, 128), whole(tokens, 128), whole(8, tokens),
               at_quarter(tokens, feat), at_quarter(8, tokens), at_quarter(tokens, feat),
               at_quarter(feat, tokens), whole(tokens, width)],
            out_specs=(whole(tokens, width),) + (at_quarter(feat, width),) * 3 + (at_quarter(16, feat),),
            scratch_shapes=[
                pltpu.VMEM((tokens, feat), BF), pltpu.VMEM((feat, tokens), BF),
                pltpu.VMEM((heads, tokens, feat), BF), pltpu.VMEM((heads, feat, tokens), BF),
                pltpu.VMEM((heads, feat, tokens), BF), pltpu.VMEM((tokens, feat), BF),
                pltpu.VMEM((feat, tokens), BF), pltpu.VMEM((feat, tokens), BF),
                pltpu.VMEM((feat, tokens), F32), pltpu.VMEM((feat, tokens), F32)]),
        compiler_params=pltpu.CompilerParams(vmem_limit_bytes=60 << 20),
    )(scal, bounds, x, wqkv, wqkv, wqkv, bias, bcol, segc, segr, ctx, lse, do, dot, s1g)


PART = 16


def peer_copy(src, dst, send, recv, **where):
    return pltpu.make_async_remote_copy(
        src_ref=src, dst_ref=dst, send_sem=send, recv_sem=recv,
        device_id=where, device_id_type=pl.DeviceIdType.MESH)


def greet(w, t):
    barrier = pltpu.get_barrier_semaphore()
    mesh_id = pl.DeviceIdType.MESH
    pl.semaphore_signal(barrier, inc=1, device_id={"width": w ^ 1, "tok": t}, device_id_type=mesh_id)
    pl.semaphore_signal(barrier, inc=1, device_id={"width": w ^ 2, "tok": t}, device_id_type=mesh_id)
    pl.semaphore_signal(barrier, inc=1, device_id={"width": w, "tok": t ^ 1}, device_id_type=mesh_id)
    for k in range(1, 4):
        other = lax.rem(t + 2 * k, 8)
        pl.semaphore_signal(barrier, inc=1, device_id={"width": w, "tok": other}, device_id_type=mesh_id)
    pl.semaphore_wait(barrier, 6)


def reduce_kernel(g_ref, out_ref, ra, sx, rx, acc, ry, sy, rz,
                  sa_sem, ra_sem, sx_sem, rx_sem, sy_sem, ry_sem, sz_sem, rz_sem):
    w = lax.axis_index("width")
    t = lax.axis_index("tok")
    y = lax.rem(t, 2)
    z = lax.div(t, 2)
    parts = g_ref.shape[3] // PART
    greet(w, t)

    def rows(p):
        return pl.ds(pl.multiple_of(p * PART, PART), PART)

    def near(p, slot, quarter):
        return peer_copy(g_ref.at[quarter, :, :, rows(p), :], ra.at[slot, :, :, rows(p), :],
                         sa_sem.at[slot, p], ra_sem.at[slot, p], width=w ^ 1, tok=t)

    def across(p):
        return peer_copy(sx.at[:, :, rows(p), :], rx.at[:, :, rows(p), :],
                         sx_sem.at[p], rx_sem.at[p], width=w ^ 2, tok=t)

    def beside(p):
        return peer_copy(acc.at[:, 1 - y, rows(p), :], ry.at[:, rows(p), :],
                         sy_sem.at[p], ry_sem.at[p], width=w, tok=t ^ 1)

    def along(p, k):
        there = lax.rem(z + k, 4)
        return peer_copy(sy.at[there, rows(p), :], rz.at[k - 1, rows(p), :],
                         sz_sem.at[k - 1, p], rz_sem.at[k - 1, p], width=w, tok=2 * there + y)

    @pl.loop(0, parts)
    def _(p):
        @pl.when(w == 3)
        def _():
            near(p, 0, 0).start()

        @pl.when(w == 2)
        def _():
            near(p, 0, 1).start()

    @pl.loop(0, parts)
    def _(p):
        @pl.when(w == 3)
        def _():
            near(p, 1, 2).start()

        @pl.when(w == 1)
        def _():
            near(p, 0, 0).start()

    @pl.loop(0, parts)
    def _(p):
        @pl.when(w >= 2)
        def _():
            near(p, 0, 0).wait_recv()
            far = w - 2
            sx[:, :, rows(p), :] = (g_ref[far, :, :, rows(p), :].astype(F32)
                                    + ra[0, :, :, rows(p), :].astype(F32)).astype(BF)
            across(p).start()

    @pl.loop(0, parts)
    def _(p):
        total = g_ref[w, :, :, rows(p), :].astype(F32)
        acc[:, :, rows(p), :] = total.astype(BF)

        @pl.when(w == 2)
        def _():
            near(p, 1, 2).wait_recv()
            acc[:, :, rows(p), :] = (g_ref[w, :, :, rows(p), :].astype(F32)
                                     + ra[1, :, :, rows(p), :].astype(F32)).astype(BF)

        @pl.when(w == 1)
        def _():
            across(p).wait_recv()
            acc[:, :, rows(p), :] = (g_ref[w, :, :, rows(p), :].astype(F32)
                                     + rx[:, :, rows(p), :].astype(F32)).astype(BF)

        @pl.when(w == 0)
        def _():
            near(p, 0, 0).wait_recv()
            across(p).wait_recv()
            acc[:, :, rows(p), :] = (g_ref[w, :, :, rows(p), :].astype(F32)
                                     + ra[0, :, :, rows(p), :].astype(F32)
                                     + rx[:, :, rows(p), :].astype(F32)).astype(BF)

        beside(p).start()

    @pl.loop(0, parts)
    def _(p):
        beside(p).wait_recv()
        sy[:, rows(p), :] = (acc[:, y, rows(p), :].astype(F32) + ry[:, rows(p), :].astype(F32)).astype(BF)
        for k in range(1, 4):
            along(p, k).start()

    @pl.loop(0, parts)
    def _(p):
        total = sy[z, rows(p), :].astype(F32)
        for k in range(1, 4):
            along(p, k).wait_recv()
            total = total + rz[k - 1, rows(p), :].astype(F32)
        out_ref[rows(p), :] = total

    @pl.loop(0, parts)
    def _(p):
        @pl.when(w == 3)
        def _():
            near(p, 0, 0).wait_send()
            near(p, 1, 2).wait_send()

        @pl.when(w == 2)
        def _():
            near(p, 0, 1).wait_send()

        @pl.when(w == 1)
        def _():
            near(p, 0, 0).wait_send()

        @pl.when(w >= 2)
        def _():
            across(p).wait_send()

        beside(p).wait_send()
        for k in range(1, 4):
            along(p, k).wait_send()


def reduce_fast(terms):
    groups, shards, count, width = terms.shape
    parts = count // PART
    vm = pl.BlockSpec(memory_space=pltpu.VMEM)
    dma = pltpu.SemaphoreType.DMA
    column = (4, 2, count, width)
    return pl.pallas_call(
        reduce_kernel,
        name="reduce_fast",
        out_shape=jax.ShapeDtypeStruct((count, width), F32),
        in_specs=[vm],
        out_specs=vm,
        scratch_shapes=[
            pltpu.VMEM((2,) + column, BF), pltpu.VMEM(column, BF), pltpu.VMEM(column, BF),
            pltpu.VMEM(column, BF), pltpu.VMEM((4, count, width), BF), pltpu.VMEM((4, count, width), BF),
            pltpu.VMEM((3, count, width), BF),
            dma((2, parts)), dma((2, parts)), dma((parts,)), dma((parts,)),
            dma((parts,)), dma((parts,)), dma((3, parts)), dma((3, parts))],
        compiler_params=pltpu.CompilerParams(
            collective_id=1, has_side_effects=True, vmem_limit_bytes=40 << 20),
    )(terms.reshape((groups, 4, 2, count, width)))


def shard_kernel(own_ref, line_ref, all_ref, lines_ref, own_sem, recv_sem, z_sem, y_sem):
    w = lax.axis_index("width")
    t = lax.axis_index("tok")
    y = lax.rem(t, 2)
    z = lax.div(t, 2)
    mine = (pltpu.make_async_copy(own_ref, all_ref.at[:, t], own_sem.at[0]),
            pltpu.make_async_copy(line_ref, lines_ref.at[t], own_sem.at[1]))
    for copy in mine:
        copy.start()
    greet(w, t)
    for copy in mine:
        copy.wait()

    def both(s, sems, **where):
        return (peer_copy(all_ref.at[:, s], all_ref.at[:, s], sems.at[0], recv_sem.at[0, s], **where),
                peer_copy(lines_ref.at[s], lines_ref.at[s], sems.at[1], recv_sem.at[1, s], **where))

    def along(k):
        return both(t, z_sem.at[k - 1], width=w, tok=lax.rem(t + 2 * k, 8))

    def beside(zz):
        return both(2 * zz + y, y_sem.at[zz], width=w, tok=t ^ 1)

    def start(pair):
        for copy in pair:
            copy.start()

    def arrived(s):
        for copy in both(s, y_sem.at[0], width=w, tok=t ^ 1):
            copy.wait_recv()

    def sent(pair):
        for copy in pair:
            copy.wait_send()

    for k in range(1, 4):
        start(along(k))
    start(beside(z))
    for k in range(1, 4):
        zz = lax.rem(z + k, 4)
        arrived(2 * zz + y)
        start(beside(zz))

    @pl.loop(0, 4)
    def _(k):
        s = 2 * lax.rem(z + k, 4) + (1 - y)
        arrived(s)

    for k in range(1, 4):
        sent(along(k))

    @pl.loop(0, 4)
    def _(zz):
        sent(beside(zz))


def gather_kernel(own_ref, line_ref, ctx_ref, lse_ref, all_ref, lines_ref, ctxs_ref, lses_ref,
                  own_sem, recv_sem, z_sem, y_sem, core_sem, x_sem,
                  side_recv, side_core, side_x):
    w = lax.axis_index("width")
    t = lax.axis_index("tok")
    y = lax.rem(t, 2)
    z = lax.div(t, 2)
    mine = (pltpu.make_async_copy(own_ref, all_ref.at[w, t], own_sem.at[0]),
            pltpu.make_async_copy(line_ref, lines_ref.at[w, t], own_sem.at[1]),
            pltpu.make_async_copy(ctx_ref.at[0], ctxs_ref.at[w], own_sem.at[2]),
            pltpu.make_async_copy(lse_ref.at[0], lses_ref.at[w], own_sem.at[3]))
    for copy in mine:
        copy.start()
    greet(w, t)
    for copy in mine:
        copy.wait()

    def both(q, s, sems, **where):
        return (peer_copy(all_ref.at[q, s], all_ref.at[q, s], sems.at[0], recv_sem.at[0, q, s], **where),
                peer_copy(lines_ref.at[q, s], lines_ref.at[q, s], sems.at[1], recv_sem.at[1, q, s], **where))

    def along(k):
        return both(w, t, z_sem.at[k - 1], width=w, tok=lax.rem(t + 2 * k, 8))

    def beside(zz):
        return both(w, 2 * zz + y, y_sem.at[zz], width=w, tok=t ^ 1)

    def near(q, s):
        return both(q, s, core_sem.at[q, s], width=w ^ 1, tok=t)

    def across(s):
        return both(w, s, x_sem.at[s], width=w ^ 2, tok=t)

    def side(q, sems, **where):
        return (peer_copy(ctxs_ref.at[q], ctxs_ref.at[q], sems.at[0], side_recv.at[0, q], **where),
                peer_copy(lses_ref.at[q], lses_ref.at[q], sems.at[1], side_recv.at[1, q], **where))

    def side_near(q):
        return side(q, side_core.at[q], width=w ^ 1, tok=t)

    def side_across():
        return side(w, side_x, width=w ^ 2, tok=t)

    def start(pair):
        for copy in pair:
            copy.start()

    def arrived(q, s):
        for copy in near(q, s):
            copy.wait_recv()

    def sent(pair):
        for copy in pair:
            copy.wait_send()

    def outward(s):
        @pl.when(w <= 1)
        def _():
            start(across(s))

        @pl.when((w == 0) | (w == 2))
        def _():
            start(near(w, s))

    @pl.when(w <= 1)
    def _():
        start(side_across())

    @pl.when((w == 0) | (w == 2))
    def _():
        start(side_near(w))

    for k in range(1, 4):
        start(along(k))
    start(beside(z))
    outward(t)
    for k in range(1, 4):
        zz = lax.rem(z + k, 4)
        arrived(w, 2 * zz + y)
        start(beside(zz))
        outward(2 * zz + y)

    @pl.loop(0, 4)
    def _(k):
        s = 2 * lax.rem(z + k, 4) + (1 - y)
        arrived(w, s)
        outward(s)

    @pl.when(w >= 2)
    def _():
        for copy in side_near(w - 2):
            copy.wait_recv()
        start(side_near(w - 2))

    @pl.loop(0, 8)
    def _(k):
        zz = lax.rem(z + lax.div(k, 2), 4)
        s = 2 * zz + lax.rem(y + k, 2)

        @pl.when(w >= 2)
        def _():
            arrived(w - 2, s)
            start(near(w - 2, s))

    @pl.loop(0, 8)
    def _(s):
        @pl.when((w == 1) | (w == 3))
        def _():
            arrived(w - 1, s)

        @pl.when(w == 3)
        def _():
            arrived(0, s)

        @pl.when(w == 2)
        def _():
            arrived(1, s)

    for k in range(1, 4):
        sent(along(k))

    @pl.loop(0, 4)
    def _(zz):
        sent(beside(zz))

    @pl.loop(0, 8)
    def _(s):
        @pl.when(w <= 1)
        def _():
            sent(across(s))

        @pl.when((w == 0) | (w == 2))
        def _():
            sent(near(w, s))

        @pl.when(w >= 2)
        def _():
            sent(near(w - 2, s))

    @pl.when((w == 1) | (w == 3))
    def _():
        for copy in side_near(w - 1):
            copy.wait_recv()

    @pl.when(w == 3)
    def _():
        for copy in side_near(0):
            copy.wait_recv()

    @pl.when(w == 2)
    def _():
        for copy in side_near(1):
            copy.wait_recv()

    @pl.when(w <= 1)
    def _():
        sent(side_across())

    @pl.when((w == 0) | (w == 2))
    def _():
        sent(side_near(w))

    @pl.when(w >= 2)
    def _():
        sent(side_near(w - 2))


def shard_fast(own, line):
    hbm = pl.BlockSpec(memory_space=pl.ANY)
    dma = pltpu.SemaphoreType.DMA
    sds = jax.ShapeDtypeStruct
    return pl.pallas_call(
        shard_kernel,
        name="shard_fast",
        out_shape=(sds((own.shape[0], 8) + own.shape[1:], BF), sds((8,) + line.shape, BF)),
        in_specs=[hbm] * 2,
        out_specs=(hbm,) * 2,
        scratch_shapes=[dma((2,)), dma((2, 8)), dma((3, 2)), dma((4, 2))],
        compiler_params=pltpu.CompilerParams(collective_id=2, has_side_effects=True),
        cost_estimate=pl.CostEstimate(flops=int(10e9), bytes_accessed=int(10e6), transcendentals=0),
    )(own, line)


def gather_fast(own, line, ctx, lse):
    hbm = pl.BlockSpec(memory_space=pl.ANY)
    dma = pltpu.SemaphoreType.DMA
    sds = jax.ShapeDtypeStruct
    return pl.pallas_call(
        gather_kernel,
        name="gather_fast",
        out_shape=(sds((4, 8) + own.shape, BF), sds((4, 8) + line.shape, BF),
                   sds((4,) + ctx.shape[1:], BF), sds((4,) + lse.shape[1:], F32)),
        in_specs=[hbm] * 4,
        out_specs=(hbm,) * 4,
        scratch_shapes=[dma((4,)), dma((2, 4, 8)), dma((3, 2)), dma((4, 2)), dma((4, 8, 2)), dma((8, 2)),
                        dma((2, 4)), dma((4, 2)), dma((2,))],
        compiler_params=pltpu.CompilerParams(collective_id=3, has_side_effects=True),
        cost_estimate=pl.CostEstimate(flops=int(30e9), bytes_accessed=int(30e6), transcendentals=0),
    )(own, line, ctx, lse)


def columns(array):
    return jnp.broadcast_to(array[:, :, None], array.shape + (128,)).astype(BF)


def gather_all(pack):
    return lax.all_gather(pack, ("width", "tok"), axis=0, tiled=False)


def scatter_all(terms):
    flat = terms.reshape((-1,) + terms.shape[2:])
    return lax.psum_scatter(flat, ("width", "tok"), scatter_dimension=0, tiled=True)[0]


def local(tokens_in, seq_lengths, *rest):
    weights, biases, out_grad = rest[:6], rest[6:15], rest[15]
    groups = lax.axis_size("width")
    shards = lax.axis_size("tok")
    level = lax.axis_index("width")
    tokens, width = tokens_in.shape
    owned = weights[0].shape[0]
    owned_ff = weights[4].shape[0]
    feat = owned * shards
    units = owned_ff * shards

    def flat(*vectors):
        line = jnp.concatenate(vectors)
        return jnp.pad(line, (0, width - line.shape[0]))[None, :]

    fast = groups == 4 and shards == 8 and owned % 8 == 0
    late = gather_all(jnp.concatenate([weights[4], flat(*biases[2:])], axis=0))
    late = late.reshape((groups, shards) + late.shape[1:])
    soon = jnp.stack(weights[:3])
    line = jnp.concatenate(biases[:2])
    if fast:
        line = jnp.pad(line[None, :], ((0, 7), (0, 128 - line.shape[0])))
        own, line = shard_fast(soon, line)
        line = line[:, 0, : 2 * owned]
    else:
        own = lax.all_gather(soon, "tok", axis=1)
        line = lax.all_gather(line, "tok", axis=0)
    own = own.reshape(3, feat, width)
    qv = jnp.stack([line[:, :owned].reshape(feat), line[:, owned:].reshape(feat)])

    ends = jnp.cumsum(seq_lengths[0])
    positions = jnp.arange(tokens, dtype=jnp.int32)
    segment = jnp.sum((positions[:, None] >= ends[None, :]).astype(jnp.int32), axis=1)
    lows = jnp.sum((segment[None, :] < segment[::BR, None]).astype(jnp.int32), axis=1)
    highs = jnp.sum((segment[None, :] <= segment[BR - 1 :: BR, None]).astype(jnp.int32), axis=1)
    bounds = jnp.stack([lows // BC, (highs + BC - 1) // BC])
    segc = jnp.broadcast_to(segment[:, None], (tokens, 128))
    segr = jnp.broadcast_to(segment[None, :], (8, tokens))
    scal = level[None].astype(jnp.int32)

    def as_bias(pair):
        return jnp.pad(pair.astype(F32), ((0, 0), (0, 6), (0, 0)))

    ctx, lse = run_fwd(bounds, tokens_in, own, as_bias(qv[None]), segc, segr)
    if fast:
        ws, wo, ctx, lse = gather_fast(weights[5], weights[3], ctx, lse)
    else:
        both = gather_all(jnp.concatenate([weights[5], weights[3]], axis=0))
        both = both.reshape((groups, shards) + both.shape[1:])
        ws, wo = both[:, :, :owned_ff], both[:, :, owned_ff:]
        ctx, lse = (lax.all_gather(part[0], "width", axis=0) for part in (ctx, lse))
    ws, wo = ws.reshape(groups, units, width), wo.reshape(groups, feat, width)
    we = late[:, :, :owned_ff].reshape(groups, units, width)
    row = late[:, :, owned_ff]
    sizes = [b.shape[0] for b in biases[2:]]
    starts = [sum(sizes[:n]) for n in range(7)]
    vecs = [row[:, :, a : a + n].reshape(groups, n * shards) for a, n in zip(starts, sizes)]
    eb = jnp.pad(vecs[1][:, None, :].astype(F32), ((0, 0), (0, 7), (0, 0)))
    vec = jnp.stack([v.reshape(-1) for v in [vecs[0], vecs[2]] + vecs[3:]]).astype(F32)
    vec = jnp.pad(vec, ((2, 0), (0, 0)))

    qv = jnp.pad(qv, ((0, 6), (0, width - feat)))
    wqkv = lax.all_gather(jnp.concatenate([own.reshape(3 * feat, width), qv], axis=0), "width", axis=0)
    qv = wqkv[:, 3 * feat : 3 * feat + 2, :feat]
    bias = as_bias(qv)
    bcol = jnp.pad(jnp.swapaxes(qv, 1, 2), ((0, 0), (0, 0), (0, 126)))

    result, s1g, do, dot, dwo, vg, ebg, de, ds = run_middle(
        scal, tokens_in, ctx, wo, we, ws, vec, eb, out_grad[0])
    mine = jnp.arange(groups) <= level

    def pieces(term):
        return term.reshape((groups, shards, -1) + term.shape[2:])

    def split(line):
        return line.reshape(groups, shards, -1)

    def only(term):
        return jnp.where(mine.reshape((groups,) + (1,) * (term.ndim - 1)), term, jnp.zeros_like(term))

    def packed(*terms):
        return only(jnp.concatenate([pieces(t) for t in terms], axis=2))

    def lined(*lines):
        line = jnp.concatenate(lines, axis=2).astype(BF)
        line = jnp.pad(line, ((0, 0), (0, 0), (0, width - line.shape[2])))
        return jnp.pad(line[:, :, None, :], ((0, 0), (0, 0), (0, 7), (0, 0)))

    line = lined(only(split(ebg[:, 0])), *(split(vg[n]) for n in range(2, 8)))
    first = jnp.concatenate([packed(dwo, de, ds), line], axis=2)
    first, s1g = lax.optimization_barrier((first, s1g))
    early = scatter_all(first)
    input_grad, dwq, dwk, dwv, db = run_bwd(
        scal, bounds, tokens_in, wqkv, bias, bcol, segc, segr, ctx, lse, do, dot, s1g)

    line = lined(only(split(db[:, 0])), only(split(db[:, 8])))
    second = jnp.concatenate([packed(dwq, dwk, dwv), line], axis=2)
    if groups == 4 and shards == 8 and owned % 8 == 0:
        final = reduce_fast(second)
    else:
        final = scatter_all(second).astype(F32)
    early = early.astype(F32)
    outs = [final[n * owned : (n + 1) * owned] for n in range(3)]
    outs += [early[:owned], early[owned : owned + owned_ff], early[owned + owned_ff : owned + 2 * owned_ff]]
    late = final[3 * owned]
    soon = early[owned + 2 * owned_ff]
    vecs = [soon[owned_ff + n * owned : owned_ff + (n + 1) * owned] for n in range(6)]
    outs += [late[:owned], late[owned : 2 * owned], vecs[0], soon[:owned_ff]] + vecs[1:]
    return (result[None], input_grad[None]) + tuple(outs)


def solution(mesh):
    both = ("width", "tok")
    placed = (P("tok", None), P("tok", None)) + (P(both, None),) * 6 + (P(both),) * 9
    return jax.shard_map(
        local,
        mesh=mesh,
        in_specs=placed + (P("width", "tok", None),),
        out_specs=(P("width", "tok", None), P("width", "tok", None))
        + (P(both, None),) * 6 + (P(both),) * 9,
        check_vma=False,
    )
```

```python
import functools
import math

import jax
import jax.numpy as jnp
from jax import lax
from jax.experimental import pallas as pl
from jax.experimental.pallas import tpu as pltpu
from jax.sharding import PartitionSpec as P

HEADS = 12
HEAD_DIM = 64
norm_eps = 1e-12
BF = jnp.bfloat16
F32 = jnp.float32
BR = 128
BC = 256
RT = 256
MASKED = -1e30


def nt(left, right):
    return lax.dot_general(left, right, (((1,), (1,)), ((), ())), preferred_element_type=F32)


def tn(left, right):
    return lax.dot_general(left, right, (((0,), (0,)), ((), ())), preferred_element_type=F32)


def nn(left, right):
    return jnp.dot(left, right, preferred_element_type=F32)


def rows_at(index, size):
    return pl.ds(pl.multiple_of(index * size, size), size)


def head_of(shape, axis):
    return lax.broadcasted_iota(jnp.int32, shape, axis) // HEAD_DIM


def attn_fwd(bounds, x_ref, wq_ref, wk_ref, wv_ref, bias_ref, segc_ref, segr_ref,
             ctx_ref, lse_ref, q_s, kt_s, v_s, s_s, m_s):
    heads = q_s.shape[1] // HEAD_DIM
    tokens = x_ref.shape[0]

    wq, wk, wv = wq_ref[0], wk_ref[0], wv_ref[0]

    @pl.loop(0, tokens // RT)
    def _(i):
        r = rows_at(i, RT)
        xb = x_ref[r, :]
        q = (nt(xb, wq) + bias_ref[0, 0:1, :]).astype(BF).astype(F32)
        q_s[r, :] = (q * 0.125).astype(BF)
        v = (nt(xb, wv) + bias_ref[0, 1:2, :]).astype(BF)
        kt = nt(wk, xb).astype(BF)
        for h in range(heads):
            v_s[h, r, :] = jnp.where(head_of(v.shape, 1) == h, v, jnp.zeros_like(v))
            kt_s[h, :, r] = jnp.where(head_of(kt.shape, 0) == h, kt, jnp.zeros_like(kt))

    @pl.loop(0, tokens // BR)
    def _(i):
        r = rows_at(i, BR)
        qb = q_s[r, :]
        seg = segc_ref[r, :]
        seg = jnp.concatenate([seg] * (BC // 128), axis=1)
        lo, hi = bounds[0, i], bounds[1, i]
        m_s[...] = jnp.full_like(m_s, MASKED)

        @pl.loop(lo, hi)
        def _(j):
            c = rows_at(j, BC)
            keep = seg == segr_ref[0:1, c]
            for h in range(heads):
                s = jnp.where(keep, nn(qb, kt_s[h, :, c]), MASKED)
                s_s[h, :, c] = s
                m_s[h] = jnp.maximum(m_s[h], s)

        tops = [jnp.max(m_s[h], axis=1, keepdims=True) for h in range(heads)]
        zero = jnp.zeros((BR, 1), F32)

        def second(j, carry):
            out, sums = carry
            c = rows_at(j, BC)
            new = []
            for h in range(heads):
                e = jnp.exp(s_s[h, :, c] - tops[h])
                out = out + nn(e.astype(BF), v_s[h, c, :])
                new.append(sums[h] + jnp.sum(e, axis=1, keepdims=True))
            return out, tuple(new)

        out, sums = lax.fori_loop(
            lo, hi, second, (jnp.zeros((BR, q_s.shape[1]), F32), (zero,) * heads))
        lane = head_of(out.shape, 1)
        div = jnp.broadcast_to(sums[0], out.shape)
        col = lax.broadcasted_iota(jnp.int32, (BR, 128), 1)
        lse = jnp.broadcast_to(tops[0] + jnp.log(sums[0]), (BR, 128))
        for h in range(1, heads):
            div = jnp.where(lane == h, sums[h], div)
            lse = jnp.where(col == h, tops[h] + jnp.log(sums[h]), lse)
        ctx_ref[0, r, :] = (out / div).astype(BF)
        lse_ref[0, :, r] = lse.T[0:8, :]


def attn_bwd(scal, bounds, x_ref, wq_ref, wk_ref, wv_ref, bias_ref, bcol_ref, segc_ref, segr_ref,
             ctx_ref, lse_ref, do_ref, dot_ref, s1g_ref,
             ig_ref, pack_ref,
             q_s, qt_s, k_s, kt_s, vt_s, dq_s, dkt_s, dvt_s, kt_f, vt_f):
    heads = q_s.shape[1] // HEAD_DIM
    tokens = x_ref.shape[0]

    @pl.when(pl.program_id(0) == 0)
    def _():
        ig_ref[...] = s1g_ref[...]

    @pl.when(pl.program_id(0) <= scal[0])
    def _():
        wq, wk, wv = wq_ref[0], wk_ref[0], wv_ref[0]
        qcol = bcol_ref[0, :, 0:1].astype(F32)
        vcol = bcol_ref[0, :, 1:2].astype(F32)

        @pl.loop(0, tokens // RT)
        def _(i):
            r = rows_at(i, RT)
            xb = x_ref[r, :]
            q = (nt(xb, wq) + bias_ref[0, 0:1, :]).astype(BF).astype(F32)
            q_s[r, :] = (q * 0.125).astype(BF)
            qt = (nt(wq, xb) + qcol).astype(BF).astype(F32)
            qt_s[:, r] = (qt * 0.125).astype(BF)
            k = nt(xb, wk).astype(BF)
            kt = nt(wk, xb).astype(BF)
            vt = (nt(wv, xb) + vcol).astype(BF)
            for h in range(heads):
                k_s[h, r, :] = jnp.where(head_of(k.shape, 1) == h, k, jnp.zeros_like(k))
                kt_s[h, :, r] = jnp.where(head_of(kt.shape, 0) == h, kt, jnp.zeros_like(kt))
                vt_s[h, :, r] = jnp.where(head_of(vt.shape, 0) == h, vt, jnp.zeros_like(vt))

        kt_f[...] = jnp.zeros_like(kt_f)
        vt_f[...] = jnp.zeros_like(vt_f)

        @pl.loop(0, tokens // BR)
        def _(i):
            r = rows_at(i, BR)
            qb = q_s[r, :]
            dob = do_ref[0, r, :]
            seg = segc_ref[r, :]
            seg = jnp.concatenate([seg] * (BC // 128), axis=1)
            prod = dob.astype(F32) * ctx_ref[0, r, :].astype(F32)
            lane = head_of(prod.shape, 1)
            inner = [jnp.sum(jnp.where(lane == h, prod, 0.0), axis=1, keepdims=True) for h in range(heads)]
            stats = jnp.concatenate([lse_ref[0, :, r]] * 16, axis=0).T
            lses = [stats[:, h : h + 1] for h in range(heads)]
            qts = [qt_s[h * HEAD_DIM : (h + 1) * HEAD_DIM, r] for h in range(heads)]
            dots = [dot_ref[0, h * HEAD_DIM : (h + 1) * HEAD_DIM, r] for h in range(heads)]

            def block(j, dq):
                c = rows_at(j, BC)
                keep = seg == segr_ref[0:1, c]
                for h in range(heads):
                    hs = slice(h * HEAD_DIM, (h + 1) * HEAD_DIM)
                    s = jnp.where(keep, nn(qb, kt_s[h, :, c]), MASKED)
                    p = jnp.exp(s - lses[h])
                    dp = nn(dob, vt_s[h, :, c])
                    ds = (p * (dp - inner[h])).astype(BF)
                    dq = dq + nn(ds, k_s[h, c, :])
                    kt_f[hs, c] += nn(qts[h], ds)
                    vt_f[hs, c] += nn(dots[h], p.astype(BF))
                return dq

            dq = lax.fori_loop(bounds[0, i], bounds[1, i], block, jnp.zeros(qb.shape, F32))
            dq_s[r, :] = (dq * 0.125).astype(BF)

        dkt_s[...] = kt_f[...].astype(BF)
        dvt_s[...] = vt_f[...].astype(BF)

        @pl.loop(0, tokens // RT)
        def _(i):
            r = rows_at(i, RT)
            ig_ref[r, :] += nn(dq_s[r, :], wq) + tn(dkt_s[:, r], wk) + tn(dvt_s[:, r], wv)

        x = x_ref[...]
        chunks = pack_ref.shape[1]
        part = wq.shape[0] // chunks
        terms = (tn(dq_s[...], x), nn(dkt_s[...], x), nn(dvt_s[...], x))
        for n, term in enumerate(terms):
            pack_ref[0, :, n * part : (n + 1) * part, :] = term.astype(BF).reshape(chunks, part, x.shape[1])
        ones = jnp.ones((8, tokens), BF)
        pack_ref[0, :, 3 * part :, :] = jnp.zeros((chunks, 8, x.shape[1]), BF)
        for n, line in enumerate((nn(ones, dq_s[...]), nt(ones, dvt_s[...]))):
            for k in range(chunks):
                pack_ref[0, k, 3 * part :, n * 256 : n * 256 + part] = line[:, k * part : (k + 1) * part].astype(BF)


def normal_parts(value):
    phi = jnp.exp(-0.5 * value * value) * (1.0 / math.sqrt(2.0 * math.pi))
    cum = 0.5 + 0.5 * lax.erf(value * math.sqrt(0.5))
    return cum, phi


def middle(scal, x_ref, ctx_ref, wo_ref, e_hbm, s_hbm, vec_ref, eb_ref, c_ref,
           lo_ref, s1g_ref, do_ref, dot_ref, vg_ref, ebg_ref, pack_hbm,
           nl_s, n1_s, r1_s, br_s, act_s, gp_s, ug_s, bg_s, stage, sems,
           e_s, s_s, in_sem, dwo_s, dwo_sem, zero_sem):
    tokens, width = x_ref.shape
    used = scal[0] + 1
    groups, chunks, each, _ = e_s.shape
    feat = dwo_s.shape[2]
    units = chunks * each

    def loads(q):
        return (pltpu.make_async_copy(e_hbm.at[q, :, 0:each, :], e_s.at[q], in_sem.at[0, q]),
                pltpu.make_async_copy(s_hbm.at[q], s_s.at[q], in_sem.at[1, q]))

    @pl.loop(0, used)
    def _(q):
        for copy in loads(q):
            copy.start()

    def e_at(q):
        return e_s[q].reshape(units, width)

    def s_at(q):
        return s_s[q].reshape(units, width)

    tiles = tokens // RT
    ob, sb = vec_ref[2:3, :], vec_ref[3:4, :]
    g1, b1 = vec_ref[4:5, :], vec_ref[5:6, :]
    g2, b2 = vec_ref[6:7, :], vec_ref[7:8, :]

    def mean(v):
        return jnp.sum(v, axis=1, keepdims=True) * (1.0 / width)

    @pl.loop(0, tiles)
    def _(i):
        r = rows_at(i, RT)
        total = lax.fori_loop(
            0, used, lambda q, t: t + nn(ctx_ref[q, r, :], wo_ref[q]), jnp.zeros((RT, width), F32))
        v = x_ref[r, :].astype(F32) + (total + ob)
        v = v - mean(v)
        rstd = lax.rsqrt(mean(v * v) + norm_eps)
        n = v * rstd
        n1_s[r, :] = n
        r1_s[r, :] = jnp.broadcast_to(rstd, (RT, 128))
        normed = n * g1 + b1
        nl_s[r, :] = normed.astype(BF)
        br_s[r, :] = normed + sb

    @pl.loop(0, used)
    def _(q):
        for copy in loads(q):
            copy.wait()

        @pl.loop(0, tiles)
        def _(i):
            r = rows_at(i, RT)
            u = nt(nl_s[r, :], e_at(q)) + eb_ref[q, 0:1, :]
            cum, phi = normal_parts(u)
            act = (u * cum).astype(BF)
            act_s[q, r, :] = act
            gp_s[q, r, :] = (cum + u * phi).astype(BF)
            br_s[r, :] += nn(act, s_at(q))

    zero = jnp.zeros((1, width), F32)

    def second_norm(i, sums):
        r = rows_at(i, RT)
        v = br_s[r, :]
        v = v - mean(v)
        rstd = lax.rsqrt(mean(v * v) + norm_eps)
        n = v * rstd
        lo_ref[r, :] = (n * g2 + b2).astype(BF)
        c = c_ref[r, :].astype(F32)
        m = c * g2
        g = rstd * (m - mean(m) - n * mean(m * n))
        s1g_ref[r, :] = g
        bg = g.astype(BF)
        bg_s[r, :] = bg
        return (sums[0] + jnp.sum(c * n, axis=0, keepdims=True),
                sums[1] + jnp.sum(c, axis=0, keepdims=True),
                sums[2] + jnp.sum(bg.astype(F32), axis=0, keepdims=True))

    g2g, b2g, sbg = lax.fori_loop(0, tiles, second_norm, (zero, zero, zero))
    vg_ref[6:7, :] = g2g
    vg_ref[7:8, :] = b2g
    vg_ref[3:4, :] = sbg

    def slot(kind):
        return slice(feat + kind * each, feat + (kind + 1) * each)

    def moved(kind, q):
        return pltpu.make_async_copy(stage.at[kind], pack_hbm.at[q, :, slot(kind), :], sems.at[kind])

    def put(kind, n, value):
        count = value.shape[0]
        value = value.astype(BF)
        if chunks == 1:
            stage[kind, 0, n * count : (n + 1) * count, :] = value
        else:
            some = count // each
            stage[kind, n * some : (n + 1) * some] = value.reshape(some, each, width)

    @pl.loop(0, used)
    def _(q):
        def tile(i, total):
            r = rows_at(i, RT)
            d = nt(bg_s[r, :], s_at(q)) * gp_s[q, r, :].astype(F32)
            ug = d.astype(BF)
            ug_s[r, :] = ug
            s1g_ref[r, :] += nn(ug, e_at(q))
            return total + jnp.sum(ug.astype(F32), axis=0, keepdims=True)

        ebg_ref[q, 0:1, :] = lax.fori_loop(0, tiles, tile, zero)

        @pl.when(q > 0)
        def _():
            moved(0, q - 1).wait()
            moved(1, q - 1).wait()

        half = units // 2
        for n in range(2):
            cols = slice(n * half, (n + 1) * half)
            put(0, n, tn(ug_s[:, cols], nl_s[...]))
            put(1, n, tn(act_s[q, :, cols], bg_s[...]))
        moved(0, q).start()
        moved(1, q).start()

    def first_norm(i, sums):
        r = rows_at(i, RT)
        g = s1g_ref[r, :]
        n = n1_s[r, :]
        m = g * g1
        out = r1_s[r, 0:1] * (m - mean(m) - n * mean(m * n))
        s1g_ref[r, :] = out
        ag = out.astype(BF)
        ug_s[r, :] = ag

        @pl.loop(0, used)
        def _(q):
            do_ref[q, r, :] = nt(ag, wo_ref[q]).astype(BF)
            dot_ref[q, :, r] = nt(wo_ref[q], ag).astype(BF)

        return (sums[0] + jnp.sum(g * n, axis=0, keepdims=True),
                sums[1] + jnp.sum(g, axis=0, keepdims=True),
                sums[2] + jnp.sum(ag.astype(F32), axis=0, keepdims=True))

    g1g, b1g, obg = lax.fori_loop(0, tiles, first_norm, (zero, zero, zero))
    vg_ref[4:5, :] = g1g
    vg_ref[5:6, :] = b1g
    vg_ref[2:3, :] = obg

    def moved_out(q):
        return pltpu.make_async_copy(dwo_s.at[q], pack_hbm.at[q, :, 0:feat, :], dwo_sem.at[q])

    @pl.loop(0, used)
    def _(q):
        dwo_s[q] = tn(ctx_ref[q], ug_s[...]).astype(BF).reshape(chunks, feat, width)
        moved_out(q).start()

    moved(0, used - 1).wait()
    moved(1, used - 1).wait()
    stage[0] = jnp.zeros_like(stage[0])

    def cleared(q):
        zeros = stage.at[0]
        return (pltpu.make_async_copy(zeros.at[:, 0:feat, :], pack_hbm.at[q, :, 0:feat, :], zero_sem.at[0, q]),
                pltpu.make_async_copy(zeros, pack_hbm.at[q, :, slot(0), :], zero_sem.at[1, q]),
                pltpu.make_async_copy(zeros, pack_hbm.at[q, :, slot(1), :], zero_sem.at[2, q]))

    @pl.loop(used, groups)
    def _(q):
        for copy in cleared(q):
            copy.start()

    @pl.loop(0, used)
    def _(q):
        moved_out(q).wait()

    @pl.loop(used, groups)
    def _(q):
        for copy in cleared(q):
            copy.wait()


def run_middle(scal, x, ctx, wo, e, s, vec, eb, cot):
    groups, feat, width = wo.shape
    chunks, each = s.shape[1:3]
    tokens = x.shape[0]
    vm = pl.BlockSpec(memory_space=pltpu.VMEM)
    hbm = pl.BlockSpec(memory_space=pl.ANY)
    dma = pltpu.SemaphoreType.DMA
    sds = jax.ShapeDtypeStruct
    part = feat // chunks
    return pl.pallas_call(
        middle,
        name="middle",
        cost_estimate=pl.CostEstimate(flops=int(50e9), bytes_accessed=int(30e6), transcendentals=0),
        out_shape=(
            sds((tokens, width), BF), sds((tokens, width), F32),
            sds((groups, tokens, feat), BF), sds((groups, feat, tokens), BF),
            sds((8, width), F32), sds((groups, 8, width), F32),
            sds((groups, chunks, part + 2 * each + 8, width), BF)),
        in_specs=[pl.BlockSpec(memory_space=pltpu.SMEM)] + [vm] * 3 + [hbm] * 2 + [vm] * 3,
        out_specs=(vm,) * 6 + (hbm,),
        scratch_shapes=[
            pltpu.VMEM((tokens, width), BF), pltpu.VMEM((tokens, width), F32),
            pltpu.VMEM((tokens, 128), F32), pltpu.VMEM((tokens, width), F32),
            pltpu.VMEM((groups, tokens, width), BF), pltpu.VMEM((groups, tokens, width), BF),
            pltpu.VMEM((tokens, width), BF), pltpu.VMEM((tokens, width), BF),
            pltpu.VMEM((2, chunks, each, width), BF), dma((2,)),
            pltpu.VMEM((groups, chunks, each, width), BF), pltpu.VMEM((groups, chunks, each, width), BF),
            dma((2, groups)), pltpu.VMEM((groups, chunks, part, width), BF), dma((groups,)),
            dma((3, groups))],
        compiler_params=pltpu.CompilerParams(vmem_limit_bytes=62 << 20),
    )(scal, x, ctx, wo, e, s, vec, eb, cot)


def attn_specs(tokens, width, feat):
    def at_quarter(*block):
        return pl.BlockSpec((1,) + block, lambda q, s, b: (jnp.minimum(q, s[0]), 0, 0))

    def whole(*block):
        return pl.BlockSpec(block, lambda q, s, b: (0, 0))

    return at_quarter, whole


def weight_specs(groups, feat, width):
    def one(kind):
        return pl.BlockSpec((1, feat, width), lambda q, s, b: (jnp.minimum(q, s[0]), kind, 0))

    return [one(kind) for kind in range(3)]


def run_fwd(bounds, x, wqkv, bias, segc, segr):
    feat, width = wqkv.shape[1:]
    tokens = x.shape[0]
    heads = feat // HEAD_DIM

    def part(shape, kind=0):
        return pl.BlockSpec(shape, lambda i, b: (kind,) + (0,) * (len(shape) - 1))

    sds = jax.ShapeDtypeStruct
    return pl.pallas_call(
        attn_fwd,
        name="attn_fwd",
        cost_estimate=pl.CostEstimate(flops=int(10e9), bytes_accessed=int(10e6), transcendentals=0),
        out_shape=(sds((1, tokens, feat), BF), sds((1, 8, tokens), F32)),
        grid_spec=pltpu.PrefetchScalarGridSpec(
            num_scalar_prefetch=1, grid=(1,),
            in_specs=[part((tokens, width))] + [part((1, feat, width), n) for n in range(3)]
            + [part((1, 8, feat)), part((tokens, 128)), part((8, tokens))],
            out_specs=(part((1, tokens, feat)), part((1, 8, tokens))),
            scratch_shapes=[
                pltpu.VMEM((tokens, feat), BF), pltpu.VMEM((heads, feat, tokens), BF),
                pltpu.VMEM((heads, tokens, feat), BF), pltpu.VMEM((heads, BR, tokens), F32),
                pltpu.VMEM((heads, BR, BC), F32)]),
        compiler_params=pltpu.CompilerParams(vmem_limit_bytes=40 << 20),
    )(bounds, x, wqkv, wqkv, wqkv, bias, segc, segr)


def run_bwd(chunks, scal, bounds, x, wqkv, bias, bcol, segc, segr, ctx, lse, do, dot, s1g):
    groups, feat, width = wqkv.shape[0], bias.shape[2], wqkv.shape[2]
    part = feat // chunks
    tokens = x.shape[0]
    heads = feat // HEAD_DIM
    at_quarter, whole = attn_specs(tokens, width, feat)
    sds = jax.ShapeDtypeStruct
    return pl.pallas_call(
        attn_bwd,
        name="attn_bwd",
        cost_estimate=pl.CostEstimate(flops=int(90e9), bytes_accessed=int(30e6), transcendentals=0),
        out_shape=(sds((tokens, width), F32), sds((groups, chunks, 3 * part + 8, width), BF)),
        grid_spec=pltpu.PrefetchScalarGridSpec(
            num_scalar_prefetch=2, grid=(groups,),
            in_specs=[whole(tokens, width)] + weight_specs(groups, feat, width)
            + [at_quarter(8, feat), at_quarter(feat, 128), whole(tokens, 128), whole(8, tokens),
               at_quarter(tokens, feat), at_quarter(8, tokens), at_quarter(tokens, feat),
               at_quarter(feat, tokens), whole(tokens, width)],
            out_specs=(whole(tokens, width), pl.BlockSpec(
                (1, chunks, 3 * part + 8, width), lambda q, s, b: (jnp.minimum(q, s[0]), 0, 0, 0))),
            scratch_shapes=[
                pltpu.VMEM((tokens, feat), BF), pltpu.VMEM((feat, tokens), BF),
                pltpu.VMEM((heads, tokens, feat), BF), pltpu.VMEM((heads, feat, tokens), BF),
                pltpu.VMEM((heads, feat, tokens), BF), pltpu.VMEM((tokens, feat), BF),
                pltpu.VMEM((feat, tokens), BF), pltpu.VMEM((feat, tokens), BF),
                pltpu.VMEM((feat, tokens), F32), pltpu.VMEM((feat, tokens), F32)]),
        compiler_params=pltpu.CompilerParams(vmem_limit_bytes=60 << 20),
    )(scal, bounds, x, wqkv, wqkv, wqkv, bias, bcol, segc, segr, ctx, lse, do, dot, s1g)


PART = 16


def peer_copy(src, dst, send, recv, **where):
    return pltpu.make_async_remote_copy(
        src_ref=src, dst_ref=dst, send_sem=send, recv_sem=recv,
        device_id=where, device_id_type=pl.DeviceIdType.MESH)


def greet(w, t):
    barrier = pltpu.get_barrier_semaphore()
    mesh_id = pl.DeviceIdType.MESH
    pl.semaphore_signal(barrier, inc=1, device_id={"width": w ^ 1, "tok": t}, device_id_type=mesh_id)
    pl.semaphore_signal(barrier, inc=1, device_id={"width": w ^ 2, "tok": t}, device_id_type=mesh_id)
    pl.semaphore_signal(barrier, inc=1, device_id={"width": w, "tok": t ^ 1}, device_id_type=mesh_id)
    for k in range(1, 4):
        other = lax.rem(t + 2 * k, 8)
        pl.semaphore_signal(barrier, inc=1, device_id={"width": w, "tok": other}, device_id_type=mesh_id)
    pl.semaphore_wait(barrier, 6)


def reduce_kernel(g_ref, out_ref, ra, sx, rx, acc, ry, sy, rz,
                  sa_sem, ra_sem, sx_sem, rx_sem, sy_sem, ry_sem, sz_sem, rz_sem):
    w = lax.axis_index("width")
    t = lax.axis_index("tok")
    y = lax.rem(t, 2)
    z = lax.div(t, 2)
    parts = g_ref.shape[3] // PART
    greet(w, t)

    def rows(p):
        return pl.ds(pl.multiple_of(p * PART, PART), PART)

    def near(p, slot, quarter):
        return peer_copy(g_ref.at[quarter, :, :, rows(p), :], ra.at[slot, :, :, rows(p), :],
                         sa_sem.at[slot, p], ra_sem.at[slot, p], width=w ^ 1, tok=t)

    def across(p):
        return peer_copy(sx.at[:, :, rows(p), :], rx.at[:, :, rows(p), :],
                         sx_sem.at[p], rx_sem.at[p], width=w ^ 2, tok=t)

    def beside(p):
        return peer_copy(acc.at[:, 1 - y, rows(p), :], ry.at[:, rows(p), :],
                         sy_sem.at[p], ry_sem.at[p], width=w, tok=t ^ 1)

    def along(p, k):
        there = lax.rem(z + k, 4)
        return peer_copy(sy.at[there, rows(p), :], rz.at[k - 1, rows(p), :],
                         sz_sem.at[k - 1, p], rz_sem.at[k - 1, p], width=w, tok=2 * there + y)

    @pl.loop(0, parts)
    def _(p):
        @pl.when(w == 3)
        def _():
            near(p, 0, 0).start()

        @pl.when(w == 2)
        def _():
            near(p, 0, 1).start()

    @pl.loop(0, parts)
    def _(p):
        @pl.when(w == 3)
        def _():
            near(p, 1, 2).start()

        @pl.when(w == 1)
        def _():
            near(p, 0, 0).start()

    @pl.loop(0, parts)
    def _(p):
        @pl.when(w >= 2)
        def _():
            near(p, 0, 0).wait_recv()
            far = w - 2
            sx[:, :, rows(p), :] = (g_ref[far, :, :, rows(p), :].astype(F32)
                                    + ra[0, :, :, rows(p), :].astype(F32)).astype(BF)
            across(p).start()

    @pl.loop(0, parts)
    def _(p):
        total = g_ref[w, :, :, rows(p), :].astype(F32)
        acc[:, :, rows(p), :] = total.astype(BF)

        @pl.when(w == 2)
        def _():
            near(p, 1, 2).wait_recv()
            acc[:, :, rows(p), :] = (g_ref[w, :, :, rows(p), :].astype(F32)
                                     + ra[1, :, :, rows(p), :].astype(F32)).astype(BF)

        @pl.when(w == 1)
        def _():
            across(p).wait_recv()
            acc[:, :, rows(p), :] = (g_ref[w, :, :, rows(p), :].astype(F32)
                                     + rx[:, :, rows(p), :].astype(F32)).astype(BF)

        @pl.when(w == 0)
        def _():
            near(p, 0, 0).wait_recv()
            across(p).wait_recv()
            acc[:, :, rows(p), :] = (g_ref[w, :, :, rows(p), :].astype(F32)
                                     + ra[0, :, :, rows(p), :].astype(F32)
                                     + rx[:, :, rows(p), :].astype(F32)).astype(BF)

        beside(p).start()

    @pl.loop(0, parts)
    def _(p):
        beside(p).wait_recv()
        sy[:, rows(p), :] = (acc[:, y, rows(p), :].astype(F32) + ry[:, rows(p), :].astype(F32)).astype(BF)
        for k in range(1, 4):
            along(p, k).start()

    @pl.loop(0, parts)
    def _(p):
        total = sy[z, rows(p), :].astype(F32)
        for k in range(1, 4):
            along(p, k).wait_recv()
            total = total + rz[k - 1, rows(p), :].astype(F32)
        out_ref[rows(p), :] = total

    @pl.loop(0, parts)
    def _(p):
        @pl.when(w == 3)
        def _():
            near(p, 0, 0).wait_send()
            near(p, 1, 2).wait_send()

        @pl.when(w == 2)
        def _():
            near(p, 0, 1).wait_send()

        @pl.when(w == 1)
        def _():
            near(p, 0, 0).wait_send()

        @pl.when(w >= 2)
        def _():
            across(p).wait_send()

        beside(p).wait_send()
        for k in range(1, 4):
            along(p, k).wait_send()


def reduce_fast(terms):
    groups, shards, count, width = terms.shape
    parts = count // PART
    vm = pl.BlockSpec(memory_space=pltpu.VMEM)
    dma = pltpu.SemaphoreType.DMA
    column = (4, 2, count, width)
    return pl.pallas_call(
        reduce_kernel,
        name="reduce_fast",
        out_shape=jax.ShapeDtypeStruct((count, width), F32),
        in_specs=[vm],
        out_specs=vm,
        scratch_shapes=[
            pltpu.VMEM((2,) + column, BF), pltpu.VMEM(column, BF), pltpu.VMEM(column, BF),
            pltpu.VMEM(column, BF), pltpu.VMEM((4, count, width), BF), pltpu.VMEM((4, count, width), BF),
            pltpu.VMEM((3, count, width), BF),
            dma((2, parts)), dma((2, parts)), dma((parts,)), dma((parts,)),
            dma((parts,)), dma((parts,)), dma((3, parts)), dma((3, parts))],
        compiler_params=pltpu.CompilerParams(
            collective_id=1, has_side_effects=True, vmem_limit_bytes=40 << 20),
    )(terms.reshape((groups, 4, 2, count, width)))


def shard_kernel(own_ref, line_ref, all_ref, lines_ref, own_sem, recv_sem, z_sem, y_sem):
    w = lax.axis_index("width")
    t = lax.axis_index("tok")
    y = lax.rem(t, 2)
    z = lax.div(t, 2)
    mine = (pltpu.make_async_copy(own_ref, all_ref.at[:, t], own_sem.at[0]),
            pltpu.make_async_copy(line_ref, lines_ref.at[t], own_sem.at[1]))
    for copy in mine:
        copy.start()
    greet(w, t)
    for copy in mine:
        copy.wait()

    def both(s, sems, **where):
        return (peer_copy(all_ref.at[:, s], all_ref.at[:, s], sems.at[0], recv_sem.at[0, s], **where),
                peer_copy(lines_ref.at[s], lines_ref.at[s], sems.at[1], recv_sem.at[1, s], **where))

    def along(k):
        return both(t, z_sem.at[k - 1], width=w, tok=lax.rem(t + 2 * k, 8))

    def beside(zz):
        return both(2 * zz + y, y_sem.at[zz], width=w, tok=t ^ 1)

    def start(pair):
        for copy in pair:
            copy.start()

    def arrived(s):
        for copy in both(s, y_sem.at[0], width=w, tok=t ^ 1):
            copy.wait_recv()

    def sent(pair):
        for copy in pair:
            copy.wait_send()

    for k in range(1, 4):
        start(along(k))
    start(beside(z))
    for k in range(1, 4):
        zz = lax.rem(z + k, 4)
        arrived(2 * zz + y)
        start(beside(zz))

    @pl.loop(0, 4)
    def _(k):
        s = 2 * lax.rem(z + k, 4) + (1 - y)
        arrived(s)

    for k in range(1, 4):
        sent(along(k))

    @pl.loop(0, 4)
    def _(zz):
        sent(beside(zz))


def gather_kernel(own_ref, line_ref, ctx_ref, lse_ref, all_ref, lines_ref, ctxs_ref, lses_ref,
                  own_sem, recv_sem, z_sem, y_sem, core_sem, x_sem,
                  side_recv, side_core, side_x):
    w = lax.axis_index("width")
    t = lax.axis_index("tok")
    y = lax.rem(t, 2)
    z = lax.div(t, 2)
    mine = (pltpu.make_async_copy(own_ref, all_ref.at[w, t], own_sem.at[0]),
            pltpu.make_async_copy(line_ref, lines_ref.at[w, t], own_sem.at[1]),
            pltpu.make_async_copy(ctx_ref.at[0], ctxs_ref.at[w], own_sem.at[2]),
            pltpu.make_async_copy(lse_ref.at[0], lses_ref.at[w], own_sem.at[3]))
    for copy in mine:
        copy.start()
    greet(w, t)
    for copy in mine:
        copy.wait()

    def both(q, s, sems, **where):
        return (peer_copy(all_ref.at[q, s], all_ref.at[q, s], sems.at[0], recv_sem.at[0, q, s], **where),
                peer_copy(lines_ref.at[q, s], lines_ref.at[q, s], sems.at[1], recv_sem.at[1, q, s], **where))

    def along(k):
        return both(w, t, z_sem.at[k - 1], width=w, tok=lax.rem(t + 2 * k, 8))

    def beside(zz):
        return both(w, 2 * zz + y, y_sem.at[zz], width=w, tok=t ^ 1)

    def near(q, s):
        return both(q, s, core_sem.at[q, s], width=w ^ 1, tok=t)

    def across(s):
        return both(w, s, x_sem.at[s], width=w ^ 2, tok=t)

    def side(q, sems, **where):
        return (peer_copy(ctxs_ref.at[q], ctxs_ref.at[q], sems.at[0], side_recv.at[0, q], **where),
                peer_copy(lses_ref.at[q], lses_ref.at[q], sems.at[1], side_recv.at[1, q], **where))

    def side_near(q):
        return side(q, side_core.at[q], width=w ^ 1, tok=t)

    def side_across():
        return side(w, side_x, width=w ^ 2, tok=t)

    def start(pair):
        for copy in pair:
            copy.start()

    def arrived(q, s):
        for copy in near(q, s):
            copy.wait_recv()

    def sent(pair):
        for copy in pair:
            copy.wait_send()

    def outward(s):
        @pl.when(w <= 1)
        def _():
            start(across(s))

        @pl.when((w == 0) | (w == 2))
        def _():
            start(near(w, s))

    @pl.when(w <= 1)
    def _():
        start(side_across())

    @pl.when((w == 0) | (w == 2))
    def _():
        start(side_near(w))

    for k in range(1, 4):
        start(along(k))
    start(beside(z))
    outward(t)
    for k in range(1, 4):
        zz = lax.rem(z + k, 4)
        arrived(w, 2 * zz + y)
        start(beside(zz))
        outward(2 * zz + y)

    @pl.loop(0, 4)
    def _(k):
        s = 2 * lax.rem(z + k, 4) + (1 - y)
        arrived(w, s)
        outward(s)

    @pl.when(w >= 2)
    def _():
        for copy in side_near(w - 2):
            copy.wait_recv()
        start(side_near(w - 2))

    @pl.loop(0, 8)
    def _(k):
        zz = lax.rem(z + lax.div(k, 2), 4)
        s = 2 * zz + lax.rem(y + k, 2)

        @pl.when(w >= 2)
        def _():
            arrived(w - 2, s)
            start(near(w - 2, s))

    @pl.loop(0, 8)
    def _(s):
        @pl.when((w == 1) | (w == 3))
        def _():
            arrived(w - 1, s)

        @pl.when(w == 3)
        def _():
            arrived(0, s)

        @pl.when(w == 2)
        def _():
            arrived(1, s)

    for k in range(1, 4):
        sent(along(k))

    @pl.loop(0, 4)
    def _(zz):
        sent(beside(zz))

    @pl.loop(0, 8)
    def _(s):
        @pl.when(w <= 1)
        def _():
            sent(across(s))

        @pl.when((w == 0) | (w == 2))
        def _():
            sent(near(w, s))

        @pl.when(w >= 2)
        def _():
            sent(near(w - 2, s))

    @pl.when((w == 1) | (w == 3))
    def _():
        for copy in side_near(w - 1):
            copy.wait_recv()

    @pl.when(w == 3)
    def _():
        for copy in side_near(0):
            copy.wait_recv()

    @pl.when(w == 2)
    def _():
        for copy in side_near(1):
            copy.wait_recv()

    @pl.when(w <= 1)
    def _():
        sent(side_across())

    @pl.when((w == 0) | (w == 2))
    def _():
        sent(side_near(w))

    @pl.when(w >= 2)
    def _():
        sent(side_near(w - 2))


def shard_fast(own, line):
    hbm = pl.BlockSpec(memory_space=pl.ANY)
    dma = pltpu.SemaphoreType.DMA
    sds = jax.ShapeDtypeStruct
    return pl.pallas_call(
        shard_kernel,
        name="shard_fast",
        out_shape=(sds((own.shape[0], 8) + own.shape[1:], BF), sds((8,) + line.shape, BF)),
        in_specs=[hbm] * 2,
        out_specs=(hbm,) * 2,
        scratch_shapes=[dma((2,)), dma((2, 8)), dma((3, 2)), dma((4, 2))],
        compiler_params=pltpu.CompilerParams(collective_id=2, has_side_effects=True),
        cost_estimate=pl.CostEstimate(flops=int(10e9), bytes_accessed=int(10e6), transcendentals=0),
    )(own, line)


def gather_fast(own, line, ctx, lse):
    hbm = pl.BlockSpec(memory_space=pl.ANY)
    dma = pltpu.SemaphoreType.DMA
    sds = jax.ShapeDtypeStruct
    return pl.pallas_call(
        gather_kernel,
        name="gather_fast",
        out_shape=(sds((4, 8) + own.shape, BF), sds((4, 8) + line.shape, BF),
                   sds((4,) + ctx.shape[1:], BF), sds((4,) + lse.shape[1:], F32)),
        in_specs=[hbm] * 4,
        out_specs=(hbm,) * 4,
        scratch_shapes=[dma((4,)), dma((2, 4, 8)), dma((3, 2)), dma((4, 2)), dma((4, 8, 2)), dma((8, 2)),
                        dma((2, 4)), dma((4, 2)), dma((2,))],
        compiler_params=pltpu.CompilerParams(collective_id=3, has_side_effects=True),
        cost_estimate=pl.CostEstimate(flops=int(30e9), bytes_accessed=int(30e6), transcendentals=0),
    )(own, line, ctx, lse)


def columns(array):
    return jnp.broadcast_to(array[:, :, None], array.shape + (128,)).astype(BF)


def gather_all(pack):
    return lax.all_gather(pack, ("width", "tok"), axis=0, tiled=False)


def scatter_all(terms):
    flat = terms.reshape((-1,) + terms.shape[2:])
    return lax.psum_scatter(flat, ("width", "tok"), scatter_dimension=0, tiled=True)[0]


def local(tokens_in, seq_lengths, *rest):
    weights, biases, out_grad = rest[:6], rest[6:15], rest[15]
    groups = lax.axis_size("width")
    shards = lax.axis_size("tok")
    level = lax.axis_index("width")
    tokens, width = tokens_in.shape
    owned = weights[0].shape[0]
    owned_ff = weights[4].shape[0]
    feat = owned * shards
    units = owned_ff * shards

    def flat(*vectors):
        line = jnp.concatenate(vectors)
        return jnp.pad(line, (0, width - line.shape[0]))[None, :]

    fast = groups == 4 and shards == 8 and owned % 8 == 0
    late = gather_all(jnp.concatenate([weights[4], flat(*biases[2:])], axis=0))
    late = late.reshape((groups, shards) + late.shape[1:])
    soon = jnp.stack(weights[:3])
    line = jnp.concatenate(biases[:2])
    if fast:
        line = jnp.pad(line[None, :], ((0, 7), (0, 128 - line.shape[0])))
        own, line = shard_fast(soon, line)
        line = line[:, 0, : 2 * owned]
    else:
        own = lax.all_gather(soon, "tok", axis=1)
        line = lax.all_gather(line, "tok", axis=0)
    own = own.reshape(3, feat, width)
    qv = jnp.stack([line[:, :owned].reshape(feat), line[:, owned:].reshape(feat)])

    ends = jnp.cumsum(seq_lengths[0])
    positions = jnp.arange(tokens, dtype=jnp.int32)
    segment = jnp.sum((positions[:, None] >= ends[None, :]).astype(jnp.int32), axis=1)
    lows = jnp.sum((segment[None, :] < segment[::BR, None]).astype(jnp.int32), axis=1)
    highs = jnp.sum((segment[None, :] <= segment[BR - 1 :: BR, None]).astype(jnp.int32), axis=1)
    bounds = jnp.stack([lows // BC, (highs + BC - 1) // BC])
    segc = jnp.broadcast_to(segment[:, None], (tokens, 128))
    segr = jnp.broadcast_to(segment[None, :], (8, tokens))
    scal = level[None].astype(jnp.int32)

    def as_bias(pair):
        return jnp.pad(pair.astype(F32), ((0, 0), (0, 6), (0, 0)))

    ctx, lse = run_fwd(bounds, tokens_in, own, as_bias(qv[None]), segc, segr)
    if fast:
        ws, wo, ctx, lse = gather_fast(weights[5], weights[3], ctx, lse)
    else:
        both = gather_all(jnp.concatenate([weights[5], weights[3]], axis=0))
        both = both.reshape((groups, shards) + both.shape[1:])
        ws, wo = both[:, :, :owned_ff], both[:, :, owned_ff:]
        ctx, lse = (lax.all_gather(part[0], "width", axis=0) for part in (ctx, lse))
    wo = wo.reshape(groups, feat, width)
    we, chunks = late, shards
    if not fast:
        we, ws, chunks = late[:, :, :owned_ff].reshape(groups, 1, units, width), ws.reshape(groups, 1, units, width), 1
    row = late[:, :, owned_ff]
    sizes = [b.shape[0] for b in biases[2:]]
    starts = [sum(sizes[:n]) for n in range(7)]
    vecs = [row[:, :, a : a + n].reshape(groups, n * shards) for a, n in zip(starts, sizes)]
    eb = jnp.pad(vecs[1][:, None, :].astype(F32), ((0, 0), (0, 7), (0, 0)))
    vec = jnp.stack([v.reshape(-1) for v in [vecs[0], vecs[2]] + vecs[3:]]).astype(F32)
    vec = jnp.pad(vec, ((2, 0), (0, 0)))

    qv = jnp.pad(qv, ((0, 6), (0, width - feat)))
    own, wo = lax.optimization_barrier((own, wo))
    wqkv = lax.all_gather(jnp.concatenate([own.reshape(3 * feat, width), qv], axis=0), "width", axis=0)
    qv = wqkv[:, 3 * feat : 3 * feat + 2, :feat]
    bias = as_bias(qv)
    bcol = jnp.pad(jnp.swapaxes(qv, 1, 2), ((0, 0), (0, 0), (0, 126)))

    result, s1g, do, dot, vg, ebg, first = run_middle(
        scal, tokens_in, ctx, wo, we, ws, vec, eb, out_grad[0])
    mine = jnp.arange(groups) <= level

    def split(line):
        return line.reshape(groups, shards, -1)

    def only(term):
        return jnp.where(mine.reshape((groups,) + (1,) * (term.ndim - 1)), term, jnp.zeros_like(term))

    def parted(term, sizes):
        if fast:
            return term
        out, at = [], 0
        for size in sizes:
            out.append(term[:, 0, at : at + size * shards].reshape(groups, shards, size, width))
            at = at + size * shards
        return jnp.concatenate(out + [jnp.zeros((groups, shards, 8, width), BF)], axis=2)

    def lined(*lines):
        line = jnp.concatenate(lines, axis=2).astype(BF)
        line = jnp.pad(line, ((0, 0), (0, 0), (0, width - line.shape[2])))
        return jnp.pad(line[:, :, None, :], ((0, 0), (0, 0), (0, 7), (0, 0)))

    line = lined(only(split(ebg[:, 0])), *(split(vg[n]) for n in range(2, 8)))
    first = parted(first, (owned, owned_ff, owned_ff))
    first = lax.dynamic_update_slice(first, line, (0, 0, first.shape[2] - 8, 0))
    first, s1g = lax.optimization_barrier((first, s1g))
    early = scatter_all(first)
    input_grad, second = run_bwd(
        chunks, scal, bounds, tokens_in, wqkv, bias, bcol, segc, segr, ctx, lse, do, dot, s1g)

    if fast:
        final = reduce_fast(second)
        late = [final[3 * owned, :owned], final[3 * owned, 256 : 256 + owned]]
    else:
        line = only(jnp.concatenate([split(second[:, 0, 3 * feat, n : n + feat]) for n in (0, 256)], axis=2))
        second = only(parted(second, (owned,) * 3))
        line = jnp.pad(line, ((0, 0), (0, 0), (0, width - line.shape[2])))[:, :, None, :]
        second = lax.dynamic_update_slice(second, line, (0, 0, 3 * owned, 0))
        final = scatter_all(second).astype(F32)
        late = [final[3 * owned, :owned], final[3 * owned, owned : 2 * owned]]
    early = early.astype(F32)
    outs = [final[n * owned : (n + 1) * owned] for n in range(3)]
    outs += [early[:owned], early[owned : owned + owned_ff], early[owned + owned_ff : owned + 2 * owned_ff]]
    soon = early[owned + 2 * owned_ff]
    vecs = [soon[owned_ff + n * owned : owned_ff + (n + 1) * owned] for n in range(6)]
    outs += late + [vecs[0], soon[:owned_ff]] + vecs[1:]
    return (result[None], input_grad[None]) + tuple(outs)


def solution(mesh):
    both = ("width", "tok")
    placed = (P("tok", None), P("tok", None)) + (P(both, None),) * 6 + (P(both),) * 9
    return jax.shard_map(
        local,
        mesh=mesh,
        in_specs=placed + (P("width", "tok", None),),
        out_specs=(P("width", "tok", None), P("width", "tok", None))
        + (P(both, None),) * 6 + (P(both),) * 9,
        check_vma=False,
    )
```

```python
import functools
import math

import jax
import jax.numpy as jnp
from jax import lax
from jax.experimental import pallas as pl
from jax.experimental.pallas import tpu as pltpu
from jax.sharding import PartitionSpec as P

HEADS = 12
HEAD_DIM = 64
norm_eps = 1e-12
BF = jnp.bfloat16
F32 = jnp.float32
BR = 256
BC = 512
RT = 256
MASKED = -1e30


def nt(left, right):
    return lax.dot_general(left, right, (((1,), (1,)), ((), ())), preferred_element_type=F32)


def tn(left, right):
    return lax.dot_general(left, right, (((0,), (0,)), ((), ())), preferred_element_type=F32)


def nn(left, right):
    return jnp.dot(left, right, preferred_element_type=F32)


def rows_at(index, size):
    return pl.ds(pl.multiple_of(index * size, size), size)


def head_of(shape, axis):
    return lax.broadcasted_iota(jnp.int32, shape, axis) // HEAD_DIM


def attn_fwd(bounds, x_ref, wq_ref, wk_ref, wv_ref, bias_ref, segc_ref, segr_ref,
             ctx_ref, lse_ref, q_s, kt_s, v_s, s_s, m_s):
    heads = q_s.shape[1] // HEAD_DIM
    tokens = x_ref.shape[0]

    wq, wk, wv = wq_ref[0], wk_ref[0], wv_ref[0]

    @pl.loop(0, tokens // RT)
    def _(i):
        r = rows_at(i, RT)
        xb = x_ref[r, :]
        q = (nt(xb, wq) + bias_ref[0, 0:1, :]).astype(BF).astype(F32)
        q_s[r, :] = (q * 0.125).astype(BF)
        v = (nt(xb, wv) + bias_ref[0, 1:2, :]).astype(BF)
        kt = nt(wk, xb).astype(BF)
        for h in range(heads):
            v_s[h, r, :] = jnp.where(head_of(v.shape, 1) == h, v, jnp.zeros_like(v))
            kt_s[h, :, r] = jnp.where(head_of(kt.shape, 0) == h, kt, jnp.zeros_like(kt))

    @pl.loop(0, tokens // BR)
    def _(i):
        r = rows_at(i, BR)
        qb = q_s[r, :]
        seg = segc_ref[r, :]
        seg = jnp.concatenate([seg] * (BC // 128), axis=1)
        lo, hi = bounds[0, i], bounds[1, i]
        m_s[...] = jnp.full_like(m_s, MASKED)

        @pl.loop(lo, hi)
        def _(j):
            c = rows_at(j, BC)
            keep = seg == segr_ref[0:1, c]
            for h in range(heads):
                s = jnp.where(keep, nn(qb, kt_s[h, :, c]), MASKED)
                s_s[h, :, c] = s
                m_s[h] = jnp.maximum(m_s[h], s)

        tops = [jnp.max(m_s[h], axis=1, keepdims=True) for h in range(heads)]
        zero = jnp.zeros((BR, 1), F32)

        def second(j, carry):
            out, sums = carry
            c = rows_at(j, BC)
            new = []
            for h in range(heads):
                e = jnp.exp(s_s[h, :, c] - tops[h])
                out = out + nn(e.astype(BF), v_s[h, c, :])
                new.append(sums[h] + jnp.sum(e, axis=1, keepdims=True))
            return out, tuple(new)

        out, sums = lax.fori_loop(
            lo, hi, second, (jnp.zeros((BR, q_s.shape[1]), F32), (zero,) * heads))
        lane = head_of(out.shape, 1)
        div = jnp.broadcast_to(sums[0], out.shape)
        col = lax.broadcasted_iota(jnp.int32, (BR, 128), 1)
        lse = jnp.broadcast_to(tops[0] + jnp.log(sums[0]), (BR, 128))
        for h in range(1, heads):
            div = jnp.where(lane == h, sums[h], div)
            lse = jnp.where(col == h, tops[h] + jnp.log(sums[h]), lse)
        ctx_ref[0, r, :] = (out / div).astype(BF)
        lse_ref[0, :, r] = lse.T[0:8, :]


def attn_bwd(scal, bounds, x_ref, wq_ref, wk_ref, wv_ref, bias_ref, bcol_ref, segc_ref, segr_ref,
             ctx_ref, lse_ref, do_ref, dot_ref, s1g_ref, rest_ref,
             ig_ref, pack_ref,
             q_s, qt_s, k_s, kt_s, vt_s, dq_s, dkt_s, dvt_s, kt_f, vt_f):
    heads = q_s.shape[1] // HEAD_DIM
    tokens = x_ref.shape[0]

    @pl.when(pl.program_id(0) == 0)
    def _():
        ig_ref[...] = s1g_ref[...]

    @pl.when(pl.program_id(0) <= scal[0])
    def _():
        wq, wk, wv = wq_ref[0], wk_ref[0], wv_ref[0]
        qcol = bcol_ref[0, :, 0:1].astype(F32)
        vcol = bcol_ref[0, :, 1:2].astype(F32)

        @pl.loop(0, tokens // RT)
        def _(i):
            r = rows_at(i, RT)
            xb = x_ref[r, :]
            q = (nt(xb, wq) + bias_ref[0, 0:1, :]).astype(BF).astype(F32)
            q_s[r, :] = (q * 0.125).astype(BF)
            qt = (nt(wq, xb) + qcol).astype(BF).astype(F32)
            qt_s[:, r] = (qt * 0.125).astype(BF)
            k = nt(xb, wk).astype(BF)
            kt = nt(wk, xb).astype(BF)
            vt = (nt(wv, xb) + vcol).astype(BF)
            for h in range(heads):
                k_s[h, r, :] = jnp.where(head_of(k.shape, 1) == h, k, jnp.zeros_like(k))
                kt_s[h, :, r] = jnp.where(head_of(kt.shape, 0) == h, kt, jnp.zeros_like(kt))
                vt_s[h, :, r] = jnp.where(head_of(vt.shape, 0) == h, vt, jnp.zeros_like(vt))

        kt_f[...] = jnp.zeros_like(kt_f)
        vt_f[...] = jnp.zeros_like(vt_f)

        @pl.loop(0, tokens // BR)
        def _(i):
            r = rows_at(i, BR)
            qb = q_s[r, :]
            dob = do_ref[0, r, :]
            seg = segc_ref[r, :]
            seg = jnp.concatenate([seg] * (BC // 128), axis=1)
            prod = dob.astype(F32) * ctx_ref[0, r, :].astype(F32)
            lane = head_of(prod.shape, 1)
            inner = [jnp.sum(jnp.where(lane == h, prod, 0.0), axis=1, keepdims=True) for h in range(heads)]
            stats = jnp.concatenate([lse_ref[0, :, r]] * 16, axis=0).T
            lses = [stats[:, h : h + 1] for h in range(heads)]
            qts = [qt_s[h * HEAD_DIM : (h + 1) * HEAD_DIM, r] for h in range(heads)]
            dots = [dot_ref[0, h * HEAD_DIM : (h + 1) * HEAD_DIM, r] for h in range(heads)]

            def block(j, dq):
                c = rows_at(j, BC)
                keep = seg == segr_ref[0:1, c]
                for h in range(heads):
                    hs = slice(h * HEAD_DIM, (h + 1) * HEAD_DIM)
                    s = jnp.where(keep, nn(qb, kt_s[h, :, c]), MASKED)
                    p = jnp.exp(s - lses[h])
                    dp = nn(dob, vt_s[h, :, c])
                    ds = (p * (dp - inner[h])).astype(BF)
                    dq = dq + nn(ds, k_s[h, c, :])
                    kt_f[hs, c] += nn(qts[h], ds)
                    vt_f[hs, c] += nn(dots[h], p.astype(BF))
                return dq

            dq = lax.fori_loop(bounds[0, i], bounds[1, i], block, jnp.zeros(qb.shape, F32))
            dq_s[r, :] = (dq * 0.125).astype(BF)

        dkt_s[...] = kt_f[...].astype(BF)
        dvt_s[...] = vt_f[...].astype(BF)

        @pl.loop(0, tokens // RT)
        def _(i):
            r = rows_at(i, RT)
            ig_ref[r, :] += nn(dq_s[r, :], wq) + tn(dkt_s[:, r], wk) + tn(dvt_s[:, r], wv)

        x = x_ref[...]
        chunks = pack_ref.shape[1]
        part, extra = wq.shape[0] // chunks, rest_ref.shape[2]
        pack_ref[0, :, 0:extra, :] = rest_ref[0]
        terms = (tn(dq_s[...], x), nn(dkt_s[...], x), nn(dvt_s[...], x))
        for n, term in enumerate(terms):
            pack_ref[0, :, extra + n * part : extra + (n + 1) * part, :] = term.astype(BF).reshape(chunks, part, x.shape[1])
        ones = jnp.ones((8, tokens), BF)
        pack_ref[0, :, extra + 3 * part :, :] = jnp.zeros((chunks, 8, x.shape[1]), BF)
        for n, line in enumerate((nn(ones, dq_s[...]), nt(ones, dvt_s[...]))):
            for k in range(chunks):
                pack_ref[0, k, extra + 3 * part :, n * 256 : n * 256 + part] = line[:, k * part : (k + 1) * part].astype(BF)


def normal_parts(value):
    phi = jnp.exp(-0.5 * value * value) * (1.0 / math.sqrt(2.0 * math.pi))
    cum = 0.5 + 0.5 * lax.erf(value * math.sqrt(0.5))
    return cum, phi


def middle(scal, x_ref, ctx_ref, wo_ref, e_hbm, s_hbm, vec_ref, eb_ref, c_ref,
           lo_ref, s1g_ref, do_ref, dot_ref, vg_ref, ebg_ref, pack_hbm, rest_hbm,
           nl_s, n1_s, r1_s, br_s, act_s, gp_s, ug_s, bg_s, stage, sems,
           e_s, s_s, in_sem, dwo_s, dwo_sem, zero_sem):
    tokens, width = x_ref.shape
    used = scal[0] + 1
    groups, chunks, each, _ = e_s.shape
    feat = dwo_s.shape[2]
    units = chunks * each

    def loads(q):
        return (pltpu.make_async_copy(e_hbm.at[q, :, 0:each, :], e_s.at[q], in_sem.at[0, q]),
                pltpu.make_async_copy(s_hbm.at[q], s_s.at[q], in_sem.at[1, q]))

    @pl.loop(0, used)
    def _(q):
        for copy in loads(q):
            copy.start()

    def e_at(q):
        return e_s[q].reshape(units, width)

    def s_at(q):
        return s_s[q].reshape(units, width)

    tiles = tokens // RT
    ob, sb = vec_ref[2:3, :], vec_ref[3:4, :]
    g1, b1 = vec_ref[4:5, :], vec_ref[5:6, :]
    g2, b2 = vec_ref[6:7, :], vec_ref[7:8, :]

    def mean(v):
        return jnp.sum(v, axis=1, keepdims=True) * (1.0 / width)

    @pl.loop(0, tiles)
    def _(i):
        r = rows_at(i, RT)
        total = lax.fori_loop(
            0, used, lambda q, t: t + nn(ctx_ref[q, r, :], wo_ref[q]), jnp.zeros((RT, width), F32))
        v = x_ref[r, :].astype(F32) + (total + ob)
        v = v - mean(v)
        rstd = lax.rsqrt(mean(v * v) + norm_eps)
        n = v * rstd
        n1_s[r, :] = n
        r1_s[r, :] = jnp.broadcast_to(rstd, (RT, 128))
        normed = n * g1 + b1
        nl_s[r, :] = normed.astype(BF)
        br_s[r, :] = normed + sb

    @pl.loop(0, used)
    def _(q):
        for copy in loads(q):
            copy.wait()

        @pl.loop(0, tiles)
        def _(i):
            r = rows_at(i, RT)
            u = nt(nl_s[r, :], e_at(q)) + eb_ref[q, 0:1, :]
            cum, phi = normal_parts(u)
            act = (u * cum).astype(BF)
            act_s[q, r, :] = act
            gp_s[q, r, :] = (cum + u * phi).astype(BF)
            br_s[r, :] += nn(act, s_at(q))

    zero = jnp.zeros((1, width), F32)

    def second_norm(i, sums):
        r = rows_at(i, RT)
        v = br_s[r, :]
        v = v - mean(v)
        rstd = lax.rsqrt(mean(v * v) + norm_eps)
        n = v * rstd
        lo_ref[r, :] = (n * g2 + b2).astype(BF)
        c = c_ref[r, :].astype(F32)
        m = c * g2
        g = rstd * (m - mean(m) - n * mean(m * n))
        s1g_ref[r, :] = g
        bg = g.astype(BF)
        bg_s[r, :] = bg
        return (sums[0] + jnp.sum(c * n, axis=0, keepdims=True),
                sums[1] + jnp.sum(c, axis=0, keepdims=True),
                sums[2] + jnp.sum(bg.astype(F32), axis=0, keepdims=True))

    g2g, b2g, sbg = lax.fori_loop(0, tiles, second_norm, (zero, zero, zero))
    vg_ref[6:7, :] = g2g
    vg_ref[7:8, :] = b2g
    vg_ref[3:4, :] = sbg

    def slot(kind):
        return slice(feat + kind * each, feat + (kind + 1) * each)

    cut = each // 3
    head = slice(feat + each, feat + each + cut)

    def moved(kind, q):
        if kind == 0:
            return pltpu.make_async_copy(stage.at[0], pack_hbm.at[q, :, slot(0), :], sems.at[0])
        if kind == 1:
            return pltpu.make_async_copy(stage.at[1, :, 0:cut, :], pack_hbm.at[q, :, head, :], sems.at[1])
        return pltpu.make_async_copy(stage.at[1, :, cut:each, :], rest_hbm.at[q], sems.at[2])

    def put(kind, n, value):
        count = value.shape[0]
        value = value.astype(BF)
        if chunks == 1:
            stage[kind, 0, n * count : (n + 1) * count, :] = value
        else:
            some = count // each
            stage[kind, n * some : (n + 1) * some] = value.reshape(some, each, width)

    @pl.loop(0, used)
    def _(q):
        def tile(i, total):
            r = rows_at(i, RT)
            d = nt(bg_s[r, :], s_at(q)) * gp_s[q, r, :].astype(F32)
            ug = d.astype(BF)
            ug_s[r, :] = ug
            s1g_ref[r, :] += nn(ug, e_at(q))
            return total + jnp.sum(ug.astype(F32), axis=0, keepdims=True)

        ebg_ref[q, 0:1, :] = lax.fori_loop(0, tiles, tile, zero)

        @pl.when(q > 0)
        def _():
            moved(0, q - 1).wait()
            moved(1, q - 1).wait()
            moved(2, q - 1).wait()

        half = units // 2
        for n in range(2):
            cols = slice(n * half, (n + 1) * half)
            put(0, n, tn(ug_s[:, cols], nl_s[...]))
            put(1, n, tn(act_s[q, :, cols], bg_s[...]))
        moved(0, q).start()
        moved(1, q).start()
        moved(2, q).start()

    def first_norm(i, sums):
        r = rows_at(i, RT)
        g = s1g_ref[r, :]
        n = n1_s[r, :]
        m = g * g1
        out = r1_s[r, 0:1] * (m - mean(m) - n * mean(m * n))
        s1g_ref[r, :] = out
        ag = out.astype(BF)
        ug_s[r, :] = ag

        @pl.loop(0, used)
        def _(q):
            do_ref[q, r, :] = nt(ag, wo_ref[q]).astype(BF)
            dot_ref[q, :, r] = nt(wo_ref[q], ag).astype(BF)

        return (sums[0] + jnp.sum(g * n, axis=0, keepdims=True),
                sums[1] + jnp.sum(g, axis=0, keepdims=True),
                sums[2] + jnp.sum(ag.astype(F32), axis=0, keepdims=True))

    g1g, b1g, obg = lax.fori_loop(0, tiles, first_norm, (zero, zero, zero))
    vg_ref[4:5, :] = g1g
    vg_ref[5:6, :] = b1g
    vg_ref[2:3, :] = obg

    def moved_out(q):
        return pltpu.make_async_copy(dwo_s.at[q], pack_hbm.at[q, :, 0:feat, :], dwo_sem.at[q])

    @pl.loop(0, used)
    def _(q):
        dwo_s[q] = tn(ctx_ref[q], ug_s[...]).astype(BF).reshape(chunks, feat, width)
        moved_out(q).start()

    moved(0, used - 1).wait()
    moved(1, used - 1).wait()
    moved(2, used - 1).wait()
    stage[0] = jnp.zeros_like(stage[0])

    def cleared(q):
        zeros = stage.at[0]
        return (pltpu.make_async_copy(zeros.at[:, 0:feat, :], pack_hbm.at[q, :, 0:feat, :], zero_sem.at[0, q]),
                pltpu.make_async_copy(zeros, pack_hbm.at[q, :, slot(0), :], zero_sem.at[1, q]),
                pltpu.make_async_copy(zeros.at[:, 0:cut, :], pack_hbm.at[q, :, head, :], zero_sem.at[2, q]))

    @pl.loop(used, groups)
    def _(q):
        for copy in cleared(q):
            copy.start()

    @pl.loop(0, used)
    def _(q):
        moved_out(q).wait()

    @pl.loop(used, groups)
    def _(q):
        for copy in cleared(q):
            copy.wait()


def run_middle(scal, x, ctx, wo, e, s, vec, eb, cot):
    groups, feat, width = wo.shape
    chunks, each = s.shape[1:3]
    tokens = x.shape[0]
    vm = pl.BlockSpec(memory_space=pltpu.VMEM)
    hbm = pl.BlockSpec(memory_space=pl.ANY)
    dma = pltpu.SemaphoreType.DMA
    sds = jax.ShapeDtypeStruct
    part = feat // chunks
    return pl.pallas_call(
        middle,
        name="middle",
        cost_estimate=pl.CostEstimate(flops=int(50e9), bytes_accessed=int(30e6), transcendentals=0),
        out_shape=(
            sds((tokens, width), BF), sds((tokens, width), F32),
            sds((groups, tokens, feat), BF), sds((groups, feat, tokens), BF),
            sds((8, width), F32), sds((groups, 8, width), F32),
            sds((groups, chunks, part + each + each // 3 + 8, width), BF),
            sds((groups, chunks, each - each // 3, width), BF)),
        in_specs=[pl.BlockSpec(memory_space=pltpu.SMEM)] + [vm] * 3 + [hbm] * 2 + [vm] * 3,
        out_specs=(vm,) * 6 + (hbm,) * 2,
        scratch_shapes=[
            pltpu.VMEM((tokens, width), BF), pltpu.VMEM((tokens, width), F32),
            pltpu.VMEM((tokens, 128), F32), pltpu.VMEM((tokens, width), F32),
            pltpu.VMEM((groups, tokens, width), BF), pltpu.VMEM((groups, tokens, width), BF),
            pltpu.VMEM((tokens, width), BF), pltpu.VMEM((tokens, width), BF),
            pltpu.VMEM((2, chunks, each, width), BF), dma((3,)),
            pltpu.VMEM((groups, chunks, each, width), BF), pltpu.VMEM((groups, chunks, each, width), BF),
            dma((2, groups)), pltpu.VMEM((groups, chunks, part, width), BF), dma((groups,)),
            dma((3, groups))],
        compiler_params=pltpu.CompilerParams(vmem_limit_bytes=62 << 20),
    )(scal, x, ctx, wo, e, s, vec, eb, cot)


def attn_specs(tokens, width, feat):
    def at_quarter(*block):
        return pl.BlockSpec((1,) + block, lambda q, s, b: (jnp.minimum(q, s[0]), 0, 0))

    def whole(*block):
        return pl.BlockSpec(block, lambda q, s, b: (0, 0))

    return at_quarter, whole


def weight_specs(groups, feat, width):
    def one(kind):
        return pl.BlockSpec((1, feat, width), lambda q, s, b: (jnp.minimum(q, s[0]), kind, 0))

    return [one(kind) for kind in range(3)]


def run_fwd(bounds, x, wqkv, bias, segc, segr):
    feat, width = wqkv.shape[1:]
    tokens = x.shape[0]
    heads = feat // HEAD_DIM

    def part(shape, kind=0):
        return pl.BlockSpec(shape, lambda i, b: (kind,) + (0,) * (len(shape) - 1))

    sds = jax.ShapeDtypeStruct
    return pl.pallas_call(
        attn_fwd,
        name="attn_fwd",
        cost_estimate=pl.CostEstimate(flops=int(10e9), bytes_accessed=int(10e6), transcendentals=0),
        out_shape=(sds((1, tokens, feat), BF), sds((1, 8, tokens), F32)),
        grid_spec=pltpu.PrefetchScalarGridSpec(
            num_scalar_prefetch=1, grid=(1,),
            in_specs=[part((tokens, width))] + [part((1, feat, width), n) for n in range(3)]
            + [part((1, 8, feat)), part((tokens, 128)), part((8, tokens))],
            out_specs=(part((1, tokens, feat)), part((1, 8, tokens))),
            scratch_shapes=[
                pltpu.VMEM((tokens, feat), BF), pltpu.VMEM((heads, feat, tokens), BF),
                pltpu.VMEM((heads, tokens, feat), BF), pltpu.VMEM((heads, BR, tokens), F32),
                pltpu.VMEM((heads, BR, BC), F32)]),
        compiler_params=pltpu.CompilerParams(vmem_limit_bytes=40 << 20),
    )(bounds, x, wqkv, wqkv, wqkv, bias, segc, segr)


def run_bwd(chunks, scal, bounds, x, wqkv, bias, bcol, segc, segr, ctx, lse, do, dot, s1g, rest):
    groups, feat, width = wqkv.shape[0], bias.shape[2], wqkv.shape[2]
    part, extra = feat // chunks, rest.shape[2]
    tokens = x.shape[0]
    heads = feat // HEAD_DIM
    at_quarter, whole = attn_specs(tokens, width, feat)
    sds = jax.ShapeDtypeStruct
    return pl.pallas_call(
        attn_bwd,
        name="attn_bwd",
        cost_estimate=pl.CostEstimate(flops=int(90e9), bytes_accessed=int(30e6), transcendentals=0),
        out_shape=(sds((tokens, width), F32), sds((groups, chunks, extra + 3 * part + 8, width), BF)),
        grid_spec=pltpu.PrefetchScalarGridSpec(
            num_scalar_prefetch=2, grid=(groups,),
            in_specs=[whole(tokens, width)] + weight_specs(groups, feat, width)
            + [at_quarter(8, feat), at_quarter(feat, 128), whole(tokens, 128), whole(8, tokens),
               at_quarter(tokens, feat), at_quarter(8, tokens), at_quarter(tokens, feat),
               at_quarter(feat, tokens), whole(tokens, width), pl.BlockSpec(
                (1, chunks, extra, width), lambda q, s, b: (jnp.minimum(q, s[0]), 0, 0, 0))],
            out_specs=(whole(tokens, width), pl.BlockSpec(
                (1, chunks, extra + 3 * part + 8, width), lambda q, s, b: (jnp.minimum(q, s[0]), 0, 0, 0))),
            scratch_shapes=[
                pltpu.VMEM((tokens, feat), BF), pltpu.VMEM((feat, tokens), BF),
                pltpu.VMEM((heads, tokens, feat), BF), pltpu.VMEM((heads, feat, tokens), BF),
                pltpu.VMEM((heads, feat, tokens), BF), pltpu.VMEM((tokens, feat), BF),
                pltpu.VMEM((feat, tokens), BF), pltpu.VMEM((feat, tokens), BF),
                pltpu.VMEM((feat, tokens), F32), pltpu.VMEM((feat, tokens), F32)]),
        compiler_params=pltpu.CompilerParams(vmem_limit_bytes=60 << 20),
    )(scal, bounds, x, wqkv, wqkv, wqkv, bias, bcol, segc, segr, ctx, lse, do, dot, s1g, rest)


PART = 16


def peer_copy(src, dst, send, recv, **where):
    return pltpu.make_async_remote_copy(
        src_ref=src, dst_ref=dst, send_sem=send, recv_sem=recv,
        device_id=where, device_id_type=pl.DeviceIdType.MESH)


def greet(w, t):
    barrier = pltpu.get_barrier_semaphore()
    mesh_id = pl.DeviceIdType.MESH
    pl.semaphore_signal(barrier, inc=1, device_id={"width": w ^ 1, "tok": t}, device_id_type=mesh_id)
    pl.semaphore_signal(barrier, inc=1, device_id={"width": w ^ 2, "tok": t}, device_id_type=mesh_id)
    pl.semaphore_signal(barrier, inc=1, device_id={"width": w, "tok": t ^ 1}, device_id_type=mesh_id)
    for k in range(1, 4):
        other = lax.rem(t + 2 * k, 8)
        pl.semaphore_signal(barrier, inc=1, device_id={"width": w, "tok": other}, device_id_type=mesh_id)
    pl.semaphore_wait(barrier, 6)


def reduce_kernel(g_ref, out_ref, ra, sx, rx, acc, ry, sy, rz,
                  sa_sem, ra_sem, sx_sem, rx_sem, sy_sem, ry_sem, sz_sem, rz_sem):
    w = lax.axis_index("width")
    t = lax.axis_index("tok")
    y = lax.rem(t, 2)
    z = lax.div(t, 2)
    parts = g_ref.shape[3] // PART
    greet(w, t)

    def rows(p):
        return pl.ds(pl.multiple_of(p * PART, PART), PART)

    def near(p, slot, quarter):
        return peer_copy(g_ref.at[quarter, :, :, rows(p), :], ra.at[slot, :, :, rows(p), :],
                         sa_sem.at[slot, p], ra_sem.at[slot, p], width=w ^ 1, tok=t)

    def across(p):
        return peer_copy(sx.at[:, :, rows(p), :], rx.at[:, :, rows(p), :],
                         sx_sem.at[p], rx_sem.at[p], width=w ^ 2, tok=t)

    def beside(p):
        return peer_copy(acc.at[:, 1 - y, rows(p), :], ry.at[:, rows(p), :],
                         sy_sem.at[p], ry_sem.at[p], width=w, tok=t ^ 1)

    def along(p, k):
        there = lax.rem(z + k, 4)
        return peer_copy(sy.at[there, rows(p), :], rz.at[k - 1, rows(p), :],
                         sz_sem.at[k - 1, p], rz_sem.at[k - 1, p], width=w, tok=2 * there + y)

    @pl.loop(0, parts)
    def _(p):
        @pl.when(w == 3)
        def _():
            near(p, 0, 0).start()

        @pl.when(w == 2)
        def _():
            near(p, 0, 1).start()

    @pl.loop(0, parts)
    def _(p):
        @pl.when(w == 3)
        def _():
            near(p, 1, 2).start()

        @pl.when(w == 1)
        def _():
            near(p, 0, 0).start()

    @pl.loop(0, parts)
    def _(p):
        @pl.when(w >= 2)
        def _():
            near(p, 0, 0).wait_recv()
            far = w - 2
            sx[:, :, rows(p), :] = (g_ref[far, :, :, rows(p), :].astype(F32)
                                    + ra[0, :, :, rows(p), :].astype(F32)).astype(BF)
            across(p).start()

    @pl.loop(0, parts)
    def _(p):
        total = g_ref[w, :, :, rows(p), :].astype(F32)
        acc[:, :, rows(p), :] = total.astype(BF)

        @pl.when(w == 2)
        def _():
            near(p, 1, 2).wait_recv()
            acc[:, :, rows(p), :] = (g_ref[w, :, :, rows(p), :].astype(F32)
                                     + ra[1, :, :, rows(p), :].astype(F32)).astype(BF)

        @pl.when(w == 1)
        def _():
            across(p).wait_recv()
            acc[:, :, rows(p), :] = (g_ref[w, :, :, rows(p), :].astype(F32)
                                     + rx[:, :, rows(p), :].astype(F32)).astype(BF)

        @pl.when(w == 0)
        def _():
            near(p, 0, 0).wait_recv()
            across(p).wait_recv()
            acc[:, :, rows(p), :] = (g_ref[w, :, :, rows(p), :].astype(F32)
                                     + ra[0, :, :, rows(p), :].astype(F32)
                                     + rx[:, :, rows(p), :].astype(F32)).astype(BF)

        beside(p).start()

    @pl.loop(0, parts)
    def _(p):
        beside(p).wait_recv()
        sy[:, rows(p), :] = (acc[:, y, rows(p), :].astype(F32) + ry[:, rows(p), :].astype(F32)).astype(BF)
        for k in range(1, 4):
            along(p, k).start()

    @pl.loop(0, parts)
    def _(p):
        total = sy[z, rows(p), :].astype(F32)
        for k in range(1, 4):
            along(p, k).wait_recv()
            total = total + rz[k - 1, rows(p), :].astype(F32)
        out_ref[rows(p), :] = total

    @pl.loop(0, parts)
    def _(p):
        @pl.when(w == 3)
        def _():
            near(p, 0, 0).wait_send()
            near(p, 1, 2).wait_send()

        @pl.when(w == 2)
        def _():
            near(p, 0, 1).wait_send()

        @pl.when(w == 1)
        def _():
            near(p, 0, 0).wait_send()

        @pl.when(w >= 2)
        def _():
            across(p).wait_send()

        beside(p).wait_send()
        for k in range(1, 4):
            along(p, k).wait_send()


def reduce_fast(terms):
    groups, shards, count, width = terms.shape
    parts = count // PART
    vm = pl.BlockSpec(memory_space=pltpu.VMEM)
    dma = pltpu.SemaphoreType.DMA
    column = (4, 2, count, width)
    return pl.pallas_call(
        reduce_kernel,
        name="reduce_fast",
        out_shape=jax.ShapeDtypeStruct((count, width), F32),
        in_specs=[vm],
        out_specs=vm,
        scratch_shapes=[
            pltpu.VMEM((2,) + column, BF), pltpu.VMEM(column, BF), pltpu.VMEM(column, BF),
            pltpu.VMEM(column, BF), pltpu.VMEM((4, count, width), BF), pltpu.VMEM((4, count, width), BF),
            pltpu.VMEM((3, count, width), BF),
            dma((2, parts)), dma((2, parts)), dma((parts,)), dma((parts,)),
            dma((parts,)), dma((parts,)), dma((3, parts)), dma((3, parts))],
        compiler_params=pltpu.CompilerParams(
            collective_id=1, has_side_effects=True, vmem_limit_bytes=40 << 20),
    )(terms.reshape((groups, 4, 2, count, width)))


def shard_kernel(own_ref, line_ref, all_ref, lines_ref, own_sem, recv_sem, z_sem, y_sem):
    w = lax.axis_index("width")
    t = lax.axis_index("tok")
    y = lax.rem(t, 2)
    z = lax.div(t, 2)
    mine = (pltpu.make_async_copy(own_ref, all_ref.at[:, t], own_sem.at[0]),
            pltpu.make_async_copy(line_ref, lines_ref.at[t], own_sem.at[1]))
    for copy in mine:
        copy.start()
    greet(w, t)
    for copy in mine:
        copy.wait()

    def both(s, sems, **where):
        return (peer_copy(all_ref.at[:, s], all_ref.at[:, s], sems.at[0], recv_sem.at[0, s], **where),
                peer_copy(lines_ref.at[s], lines_ref.at[s], sems.at[1], recv_sem.at[1, s], **where))

    def along(k):
        return both(t, z_sem.at[k - 1], width=w, tok=lax.rem(t + 2 * k, 8))

    def beside(zz):
        return both(2 * zz + y, y_sem.at[zz], width=w, tok=t ^ 1)

    def start(pair):
        for copy in pair:
            copy.start()

    def arrived(s):
        for copy in both(s, y_sem.at[0], width=w, tok=t ^ 1):
            copy.wait_recv()

    def sent(pair):
        for copy in pair:
            copy.wait_send()

    for k in range(1, 4):
        start(along(k))
    start(beside(z))
    for k in range(1, 4):
        zz = lax.rem(z + k, 4)
        arrived(2 * zz + y)
        start(beside(zz))

    @pl.loop(0, 4)
    def _(k):
        s = 2 * lax.rem(z + k, 4) + (1 - y)
        arrived(s)

    for k in range(1, 4):
        sent(along(k))

    @pl.loop(0, 4)
    def _(zz):
        sent(beside(zz))


def gather_kernel(own_ref, line_ref, ctx_ref, lse_ref, all_ref, lines_ref, ctxs_ref, lses_ref,
                  own_sem, recv_sem, z_sem, y_sem, core_sem, x_sem,
                  side_recv, side_core, side_x):
    w = lax.axis_index("width")
    t = lax.axis_index("tok")
    y = lax.rem(t, 2)
    z = lax.div(t, 2)
    mine = (pltpu.make_async_copy(own_ref, all_ref.at[w, t], own_sem.at[0]),
            pltpu.make_async_copy(line_ref, lines_ref.at[w, t], own_sem.at[1]),
            pltpu.make_async_copy(ctx_ref.at[0], ctxs_ref.at[w], own_sem.at[2]),
            pltpu.make_async_copy(lse_ref.at[0], lses_ref.at[w], own_sem.at[3]))
    for copy in mine:
        copy.start()
    greet(w, t)
    for copy in mine:
        copy.wait()

    def both(q, s, sems, **where):
        return (peer_copy(all_ref.at[q, s], all_ref.at[q, s], sems.at[0], recv_sem.at[0, q, s], **where),
                peer_copy(lines_ref.at[q, s], lines_ref.at[q, s], sems.at[1], recv_sem.at[1, q, s], **where))

    def along(k):
        return both(w, t, z_sem.at[k - 1], width=w, tok=lax.rem(t + 2 * k, 8))

    def beside(zz):
        return both(w, 2 * zz + y, y_sem.at[zz], width=w, tok=t ^ 1)

    def near(q, s):
        return both(q, s, core_sem.at[q, s], width=w ^ 1, tok=t)

    def across(s):
        return both(w, s, x_sem.at[s], width=w ^ 2, tok=t)

    def side(q, sems, **where):
        return (peer_copy(ctxs_ref.at[q], ctxs_ref.at[q], sems.at[0], side_recv.at[0, q], **where),
                peer_copy(lses_ref.at[q], lses_ref.at[q], sems.at[1], side_recv.at[1, q], **where))

    def side_near(q):
        return side(q, side_core.at[q], width=w ^ 1, tok=t)

    def side_across():
        return side(w, side_x, width=w ^ 2, tok=t)

    def start(pair):
        for copy in pair:
            copy.start()

    def arrived(q, s):
        for copy in near(q, s):
            copy.wait_recv()

    def sent(pair):
        for copy in pair:
            copy.wait_send()

    def outward(s):
        @pl.when(w <= 1)
        def _():
            start(across(s))

        @pl.when((w == 0) | (w == 2))
        def _():
            start(near(w, s))

    @pl.when(w <= 1)
    def _():
        start(side_across())

    @pl.when((w == 0) | (w == 2))
    def _():
        start(side_near(w))

    for k in range(1, 4):
        start(along(k))
    start(beside(z))
    outward(t)
    for k in range(1, 4):
        zz = lax.rem(z + k, 4)
        arrived(w, 2 * zz + y)
        start(beside(zz))
        outward(2 * zz + y)

    @pl.loop(0, 4)
    def _(k):
        s = 2 * lax.rem(z + k, 4) + (1 - y)
        arrived(w, s)
        outward(s)

    @pl.when(w >= 2)
    def _():
        for copy in side_near(w - 2):
            copy.wait_recv()
        start(side_near(w - 2))

    @pl.loop(0, 8)
    def _(k):
        zz = lax.rem(z + lax.div(k, 2), 4)
        s = 2 * zz + lax.rem(y + k, 2)

        @pl.when(w >= 2)
        def _():
            arrived(w - 2, s)
            start(near(w - 2, s))

    @pl.loop(0, 8)
    def _(s):
        @pl.when((w == 1) | (w == 3))
        def _():
            arrived(w - 1, s)

        @pl.when(w == 3)
        def _():
            arrived(0, s)

        @pl.when(w == 2)
        def _():
            arrived(1, s)

    for k in range(1, 4):
        sent(along(k))

    @pl.loop(0, 4)
    def _(zz):
        sent(beside(zz))

    @pl.loop(0, 8)
    def _(s):
        @pl.when(w <= 1)
        def _():
            sent(across(s))

        @pl.when((w == 0) | (w == 2))
        def _():
            sent(near(w, s))

        @pl.when(w >= 2)
        def _():
            sent(near(w - 2, s))

    @pl.when((w == 1) | (w == 3))
    def _():
        for copy in side_near(w - 1):
            copy.wait_recv()

    @pl.when(w == 3)
    def _():
        for copy in side_near(0):
            copy.wait_recv()

    @pl.when(w == 2)
    def _():
        for copy in side_near(1):
            copy.wait_recv()

    @pl.when(w <= 1)
    def _():
        sent(side_across())

    @pl.when((w == 0) | (w == 2))
    def _():
        sent(side_near(w))

    @pl.when(w >= 2)
    def _():
        sent(side_near(w - 2))


def shard_fast(own, line):
    hbm = pl.BlockSpec(memory_space=pl.ANY)
    dma = pltpu.SemaphoreType.DMA
    sds = jax.ShapeDtypeStruct
    return pl.pallas_call(
        shard_kernel,
        name="shard_fast",
        out_shape=(sds((own.shape[0], 8) + own.shape[1:], BF), sds((8,) + line.shape, BF)),
        in_specs=[hbm] * 2,
        out_specs=(hbm,) * 2,
        scratch_shapes=[dma((2,)), dma((2, 8)), dma((3, 2)), dma((4, 2))],
        compiler_params=pltpu.CompilerParams(collective_id=2, has_side_effects=True),
        cost_estimate=pl.CostEstimate(flops=int(10e9), bytes_accessed=int(10e6), transcendentals=0),
    )(own, line)


def gather_fast(own, line, ctx, lse):
    hbm = pl.BlockSpec(memory_space=pl.ANY)
    dma = pltpu.SemaphoreType.DMA
    sds = jax.ShapeDtypeStruct
    return pl.pallas_call(
        gather_kernel,
        name="gather_fast",
        out_shape=(sds((4, 8) + own.shape, BF), sds((4, 8) + line.shape, BF),
                   sds((4,) + ctx.shape[1:], BF), sds((4,) + lse.shape[1:], F32)),
        in_specs=[hbm] * 4,
        out_specs=(hbm,) * 4,
        scratch_shapes=[dma((4,)), dma((2, 4, 8)), dma((3, 2)), dma((4, 2)), dma((4, 8, 2)), dma((8, 2)),
                        dma((2, 4)), dma((4, 2)), dma((2,))],
        compiler_params=pltpu.CompilerParams(collective_id=3, has_side_effects=True),
        cost_estimate=pl.CostEstimate(flops=int(30e9), bytes_accessed=int(30e6), transcendentals=0),
    )(own, line, ctx, lse)


def columns(array):
    return jnp.broadcast_to(array[:, :, None], array.shape + (128,)).astype(BF)


def gather_all(pack):
    return lax.all_gather(pack, ("width", "tok"), axis=0, tiled=False)


def scatter_all(terms):
    flat = terms.reshape((-1,) + terms.shape[2:])
    return lax.psum_scatter(flat, ("width", "tok"), scatter_dimension=0, tiled=True)[0]


def local(tokens_in, seq_lengths, *rest):
    weights, biases, out_grad = rest[:6], rest[6:15], rest[15]
    groups = lax.axis_size("width")
    shards = lax.axis_size("tok")
    level = lax.axis_index("width")
    tokens, width = tokens_in.shape
    owned = weights[0].shape[0]
    owned_ff = weights[4].shape[0]
    feat = owned * shards
    units = owned_ff * shards

    def flat(*vectors):
        line = jnp.concatenate(vectors)
        return jnp.pad(line, (0, width - line.shape[0]))[None, :]

    fast = groups == 4 and shards == 8 and owned % 8 == 0
    late = gather_all(jnp.concatenate([weights[4], flat(*biases[2:])], axis=0))
    late = late.reshape((groups, shards) + late.shape[1:])
    soon = jnp.stack(weights[:3])
    line = jnp.concatenate(biases[:2])
    if fast:
        line = jnp.pad(line[None, :], ((0, 7), (0, 128 - line.shape[0])))
        own, line = shard_fast(soon, line)
        line = line[:, 0, : 2 * owned]
    else:
        own = lax.all_gather(soon, "tok", axis=1)
        line = lax.all_gather(line, "tok", axis=0)
    own = own.reshape(3, feat, width)
    qv = jnp.stack([line[:, :owned].reshape(feat), line[:, owned:].reshape(feat)])

    ends = jnp.cumsum(seq_lengths[0])
    positions = jnp.arange(tokens, dtype=jnp.int32)
    segment = jnp.sum((positions[:, None] >= ends[None, :]).astype(jnp.int32), axis=1)
    lows = jnp.sum((segment[None, :] < segment[::BR, None]).astype(jnp.int32), axis=1)
    highs = jnp.sum((segment[None, :] <= segment[BR - 1 :: BR, None]).astype(jnp.int32), axis=1)
    bounds = jnp.stack([lows // BC, (highs + BC - 1) // BC])
    segc = jnp.broadcast_to(segment[:, None], (tokens, 128))
    segr = jnp.broadcast_to(segment[None, :], (8, tokens))
    scal = level[None].astype(jnp.int32)

    def as_bias(pair):
        return jnp.pad(pair.astype(F32), ((0, 0), (0, 6), (0, 0)))

    ctx, lse = run_fwd(bounds, tokens_in, own, as_bias(qv[None]), segc, segr)
    if fast:
        ws, wo, ctx, lse = gather_fast(weights[5], weights[3], ctx, lse)
    else:
        both = gather_all(jnp.concatenate([weights[5], weights[3]], axis=0))
        both = both.reshape((groups, shards) + both.shape[1:])
        ws, wo = both[:, :, :owned_ff], both[:, :, owned_ff:]
        ctx, lse = (lax.all_gather(part[0], "width", axis=0) for part in (ctx, lse))
    wo = wo.reshape(groups, feat, width)
    we, chunks = late, shards
    if not fast:
        we, ws, chunks = late[:, :, :owned_ff].reshape(groups, 1, units, width), ws.reshape(groups, 1, units, width), 1
    row = late[:, :, owned_ff]
    sizes = [b.shape[0] for b in biases[2:]]
    starts = [sum(sizes[:n]) for n in range(7)]
    vecs = [row[:, :, a : a + n].reshape(groups, n * shards) for a, n in zip(starts, sizes)]
    eb = jnp.pad(vecs[1][:, None, :].astype(F32), ((0, 0), (0, 7), (0, 0)))
    vec = jnp.stack([v.reshape(-1) for v in [vecs[0], vecs[2]] + vecs[3:]]).astype(F32)
    vec = jnp.pad(vec, ((2, 0), (0, 0)))

    qv = jnp.pad(qv, ((0, 6), (0, width - feat)))
    own, wo = lax.optimization_barrier((own, wo))
    wqkv = lax.all_gather(jnp.concatenate([own.reshape(3 * feat, width), qv], axis=0), "width", axis=0)
    qv = wqkv[:, 3 * feat : 3 * feat + 2, :feat]
    bias = as_bias(qv)
    bcol = jnp.pad(jnp.swapaxes(qv, 1, 2), ((0, 0), (0, 0), (0, 126)))

    result, s1g, do, dot, vg, ebg, first, rest = run_middle(
        scal, tokens_in, ctx, wo, we, ws, vec, eb, out_grad[0])
    mine = jnp.arange(groups) <= level

    def split(line):
        return line.reshape(groups, shards, -1)

    def only(term):
        return jnp.where(mine.reshape((groups,) + (1,) * (term.ndim - 1)), term, jnp.zeros_like(term))

    def parted(term, sizes):
        if fast:
            return term
        out, at = [], 0
        for size in sizes:
            out.append(term[:, 0, at : at + size * shards].reshape(groups, shards, size, width))
            at = at + size * shards
        return jnp.concatenate(out + [jnp.zeros((groups, shards, 8, width), BF)], axis=2)

    def lined(*lines):
        line = jnp.concatenate(lines, axis=2).astype(BF)
        line = jnp.pad(line, ((0, 0), (0, 0), (0, width - line.shape[2])))
        return jnp.pad(line[:, :, None, :], ((0, 0), (0, 0), (0, 7), (0, 0)))

    line = lined(only(split(ebg[:, 0])), *(split(vg[n]) for n in range(2, 8)))
    if not fast:
        first = jnp.concatenate([first[:, :, :-8], rest], axis=2)
        first = parted(first, (owned, owned_ff, owned_ff))
    first = lax.dynamic_update_slice(first, line, (0, 0, first.shape[2] - 8, 0))
    first, s1g = lax.optimization_barrier((first, s1g))
    early = scatter_all(first)
    input_grad, second = run_bwd(
        chunks, scal, bounds, tokens_in, wqkv, bias, bcol, segc, segr, ctx, lse, do, dot, s1g, rest)

    if fast:
        final = reduce_fast(second)
        shrunk, final = final[: rest.shape[2]], final[rest.shape[2] :]
        late = [final[3 * owned, :owned], final[3 * owned, 256 : 256 + owned]]
    else:
        second = second[:, :, rest.shape[2] :]
        line = only(jnp.concatenate([split(second[:, 0, 3 * feat, n : n + feat]) for n in (0, 256)], axis=2))
        second = only(parted(second, (owned,) * 3))
        line = jnp.pad(line, ((0, 0), (0, 0), (0, width - line.shape[2])))[:, :, None, :]
        second = lax.dynamic_update_slice(second, line, (0, 0, 3 * owned, 0))
        final = scatter_all(second).astype(F32)
        late = [final[3 * owned, :owned], final[3 * owned, owned : 2 * owned]]
    early = early.astype(F32)
    outs = [final[n * owned : (n + 1) * owned] for n in range(3)]
    last = early[owned + owned_ff : early.shape[0] - 8]
    if fast:
        last = jnp.concatenate([last, shrunk], axis=0)
    outs += [early[:owned], early[owned : owned + owned_ff], last]
    soon = early[-8]
    vecs = [soon[owned_ff + n * owned : owned_ff + (n + 1) * owned] for n in range(6)]
    outs += late + [vecs[0], soon[:owned_ff]] + vecs[1:]
    return (result[None], input_grad[None]) + tuple(outs)


def solution(mesh):
    both = ("width", "tok")
    placed = (P("tok", None), P("tok", None)) + (P(both, None),) * 6 + (P(both),) * 9
    return jax.shard_map(
        local,
        mesh=mesh,
        in_specs=placed + (P("width", "tok", None),),
        out_specs=(P("width", "tok", None), P("width", "tok", None))
        + (P(both, None),) * 6 + (P(both),) * 9,
        check_vma=False,
    )
```

```python
import functools
import math

import jax
import jax.numpy as jnp
from jax import lax
from jax.experimental import pallas as pl
from jax.experimental.pallas import tpu as pltpu
from jax.sharding import PartitionSpec as P

HEADS = 12
HEAD_DIM = 64
norm_eps = 1e-12
BF = jnp.bfloat16
F32 = jnp.float32
BR = 512
BC = 512
RT = 512
MT = 512
MASKED = -1e30


def nt(left, right):
    return lax.dot_general(left, right, (((1,), (1,)), ((), ())), preferred_element_type=F32)


def tn(left, right):
    return lax.dot_general(left, right, (((0,), (0,)), ((), ())), preferred_element_type=F32)


def nn(left, right):
    return jnp.dot(left, right, preferred_element_type=F32)


def rows_at(index, size):
    return pl.ds(pl.multiple_of(index * size, size), size)


def head_of(shape, axis):
    return lax.broadcasted_iota(jnp.int32, shape, axis) // HEAD_DIM


def attn_fwd(bounds, x_ref, wq_ref, wk_ref, wv_ref, bias_ref, segc_ref, segr_ref,
             ctx_ref, lse_ref, q_s, kt_s, v_s, s_s, m_s):
    heads = q_s.shape[1] // HEAD_DIM
    tokens = x_ref.shape[0]

    wq, wk, wv = wq_ref[0], wk_ref[0], wv_ref[0]

    @pl.loop(0, tokens // RT)
    def _(i):
        r = rows_at(i, RT)
        xb = x_ref[r, :]
        q = (nt(xb, wq) + bias_ref[0, 0:1, :]).astype(BF).astype(F32)
        q_s[r, :] = (q * 0.125).astype(BF)
        v = (nt(xb, wv) + bias_ref[0, 1:2, :]).astype(BF)
        kt = nt(wk, xb).astype(BF)
        for h in range(heads):
            v_s[h, r, :] = jnp.where(head_of(v.shape, 1) == h, v, jnp.zeros_like(v))
            kt_s[h, :, r] = jnp.where(head_of(kt.shape, 0) == h, kt, jnp.zeros_like(kt))

    @pl.loop(0, tokens // BR)
    def _(i):
        r = rows_at(i, BR)
        qb = q_s[r, :]
        seg = segc_ref[r, :]
        seg = jnp.concatenate([seg] * (BC // 128), axis=1)
        lo, hi = bounds[0, i], bounds[1, i]
        m_s[...] = jnp.full_like(m_s, MASKED)

        @pl.loop(lo, hi)
        def _(j):
            c = rows_at(j, BC)
            keep = seg == segr_ref[0:1, c]
            for h in range(heads):
                s = jnp.where(keep, nn(qb, kt_s[h, :, c]), MASKED)
                s_s[h, :, c] = s
                m_s[h] = jnp.maximum(m_s[h], s)

        tops = [jnp.max(m_s[h], axis=1, keepdims=True) for h in range(heads)]
        zero = jnp.zeros((BR, 1), F32)

        def second(j, carry):
            out, sums = carry
            c = rows_at(j, BC)
            new = []
            for h in range(heads):
                e = jnp.exp(s_s[h, :, c] - tops[h])
                out = out + nn(e.astype(BF), v_s[h, c, :])
                new.append(sums[h] + jnp.sum(e, axis=1, keepdims=True))
            return out, tuple(new)

        out, sums = lax.fori_loop(
            lo, hi, second, (jnp.zeros((BR, q_s.shape[1]), F32), (zero,) * heads))
        lane = head_of(out.shape, 1)
        div = jnp.broadcast_to(sums[0], out.shape)
        col = lax.broadcasted_iota(jnp.int32, (BR, 128), 1)
        lse = jnp.broadcast_to(tops[0] + jnp.log(sums[0]), (BR, 128))
        for h in range(1, heads):
            div = jnp.where(lane == h, sums[h], div)
            lse = jnp.where(col == h, tops[h] + jnp.log(sums[h]), lse)
        ctx_ref[0, r, :] = (out / div).astype(BF)
        lse_ref[0, :, r] = lse.T[0:8, :]


def attn_bwd(scal, bounds, x_ref, wq_ref, wk_ref, wv_ref, bias_ref, bcol_ref, segc_ref, segr_ref,
             ctx_ref, lse_ref, do_ref, dot_ref, s1g_ref, rest_ref,
             ig_ref, pack_ref,
             q_s, qt_s, k_s, kt_s, vt_s, dq_s, dkt_s, dvt_s, kt_f, vt_f):
    heads = q_s.shape[1] // HEAD_DIM
    tokens = x_ref.shape[0]

    @pl.when(pl.program_id(0) == 0)
    def _():
        ig_ref[...] = s1g_ref[...]

    @pl.when(pl.program_id(0) <= scal[0])
    def _():
        wq, wk, wv = wq_ref[0], wk_ref[0], wv_ref[0]
        qcol = bcol_ref[0, :, 0:1].astype(F32)
        vcol = bcol_ref[0, :, 1:2].astype(F32)

        @pl.loop(0, tokens // RT)
        def _(i):
            r = rows_at(i, RT)
            xb = x_ref[r, :]
            q = (nt(xb, wq) + bias_ref[0, 0:1, :]).astype(BF).astype(F32)
            q_s[r, :] = (q * 0.125).astype(BF)
            qt = (nt(wq, xb) + qcol).astype(BF).astype(F32)
            qt_s[:, r] = (qt * 0.125).astype(BF)
            k = nt(xb, wk).astype(BF)
            kt = nt(wk, xb).astype(BF)
            vt = (nt(wv, xb) + vcol).astype(BF)
            for h in range(heads):
                k_s[h, r, :] = jnp.where(head_of(k.shape, 1) == h, k, jnp.zeros_like(k))
                kt_s[h, :, r] = jnp.where(head_of(kt.shape, 0) == h, kt, jnp.zeros_like(kt))
                vt_s[h, :, r] = jnp.where(head_of(vt.shape, 0) == h, vt, jnp.zeros_like(vt))

        kt_f[...] = jnp.zeros_like(kt_f)
        vt_f[...] = jnp.zeros_like(vt_f)

        @pl.loop(0, tokens // BR)
        def _(i):
            r = rows_at(i, BR)
            qb = q_s[r, :]
            dob = do_ref[0, r, :]
            seg = segc_ref[r, :]
            seg = jnp.concatenate([seg] * (BC // 128), axis=1)
            prod = dob.astype(F32) * ctx_ref[0, r, :].astype(F32)
            lane = head_of(prod.shape, 1)
            inner = [jnp.sum(jnp.where(lane == h, prod, 0.0), axis=1, keepdims=True) for h in range(heads)]
            stats = jnp.concatenate([lse_ref[0, :, r]] * 16, axis=0).T
            lses = [stats[:, h : h + 1] for h in range(heads)]
            qts = [qt_s[h * HEAD_DIM : (h + 1) * HEAD_DIM, r] for h in range(heads)]
            dots = [dot_ref[0, h * HEAD_DIM : (h + 1) * HEAD_DIM, r] for h in range(heads)]

            def block(j, dq):
                c = rows_at(j, BC)
                keep = seg == segr_ref[0:1, c]
                for h in range(heads):
                    hs = slice(h * HEAD_DIM, (h + 1) * HEAD_DIM)
                    s = jnp.where(keep, nn(qb, kt_s[h, :, c]), MASKED)
                    p = jnp.exp(s - lses[h])
                    dp = nn(dob, vt_s[h, :, c])
                    ds = (p * (dp - inner[h])).astype(BF)
                    dq = dq + nn(ds, k_s[h, c, :])
                    kt_f[hs, c] += nn(qts[h], ds)
                    vt_f[hs, c] += nn(dots[h], p.astype(BF))
                return dq

            dq = lax.fori_loop(bounds[0, i], bounds[1, i], block, jnp.zeros(qb.shape, F32))
            dq_s[r, :] = (dq * 0.125).astype(BF)

        dkt_s[...] = kt_f[...].astype(BF)
        dvt_s[...] = vt_f[...].astype(BF)

        @pl.loop(0, tokens // RT)
        def _(i):
            r = rows_at(i, RT)
            ig_ref[r, :] += nn(dq_s[r, :], wq) + tn(dkt_s[:, r], wk) + tn(dvt_s[:, r], wv)

        x = x_ref[...]
        chunks = pack_ref.shape[1]
        part, extra = wq.shape[0] // chunks, rest_ref.shape[2]
        pack_ref[0, :, 0:extra, :] = rest_ref[0]
        terms = (tn(dq_s[...], x), nn(dkt_s[...], x), nn(dvt_s[...], x))
        for n, term in enumerate(terms):
            pack_ref[0, :, extra + n * part : extra + (n + 1) * part, :] = term.astype(BF).reshape(chunks, part, x.shape[1])
        ones = jnp.ones((8, tokens), BF)
        pack_ref[0, :, extra + 3 * part :, :] = jnp.zeros((chunks, 8, x.shape[1]), BF)
        for n, line in enumerate((nn(ones, dq_s[...]), nt(ones, dvt_s[...]))):
            for k in range(chunks):
                pack_ref[0, k, extra + 3 * part :, n * 256 : n * 256 + part] = line[:, k * part : (k + 1) * part].astype(BF)


def normal_parts(value):
    phi = jnp.exp(-0.5 * value * value) * (1.0 / math.sqrt(2.0 * math.pi))
    cum = 0.5 + 0.5 * lax.erf(value * math.sqrt(0.5))
    return cum, phi


def middle(scal, x_ref, ctx_ref, wo_ref, e_hbm, s_hbm, vec_ref, eb_ref, c_ref,
           lo_ref, s1g_ref, do_ref, dot_ref, vg_ref, ebg_ref, pack_hbm, rest_hbm,
           nl_s, n1_s, r1_s, br_s, act_s, gp_s, ug_s, bg_s, stage, sems,
           e_s, s_s, in_sem, dwo_s, dwo_sem, zero_sem):
    tokens, width = x_ref.shape
    used = scal[0] + 1
    groups, chunks, each, _ = e_s.shape
    feat = dwo_s.shape[2]
    units = chunks * each

    def loads(q):
        return (pltpu.make_async_copy(e_hbm.at[q, :, 0:each, :], e_s.at[q], in_sem.at[0, q]),
                pltpu.make_async_copy(s_hbm.at[q], s_s.at[q], in_sem.at[1, q]))

    @pl.loop(0, used)
    def _(q):
        for copy in loads(q):
            copy.start()

    def e_at(q):
        return e_s[q].reshape(units, width)

    def s_at(q):
        return s_s[q].reshape(units, width)

    tiles = tokens // MT
    ob, sb = vec_ref[2:3, :], vec_ref[3:4, :]
    g1, b1 = vec_ref[4:5, :], vec_ref[5:6, :]
    g2, b2 = vec_ref[6:7, :], vec_ref[7:8, :]

    def mean(v):
        return jnp.sum(v, axis=1, keepdims=True) * (1.0 / width)

    @pl.loop(0, tiles)
    def _(i):
        r = rows_at(i, MT)
        total = lax.fori_loop(
            0, used, lambda q, t: t + nn(ctx_ref[q, r, :], wo_ref[q]), jnp.zeros((MT, width), F32))
        v = x_ref[r, :].astype(F32) + (total + ob)
        v = v - mean(v)
        rstd = lax.rsqrt(mean(v * v) + norm_eps)
        n = v * rstd
        n1_s[r, :] = n
        r1_s[r, :] = jnp.broadcast_to(rstd, (MT, 128))
        normed = n * g1 + b1
        nl_s[r, :] = normed.astype(BF)
        br_s[r, :] = normed + sb

    @pl.loop(0, used)
    def _(q):
        for copy in loads(q):
            copy.wait()

        @pl.loop(0, tiles)
        def _(i):
            r = rows_at(i, MT)
            u = nt(nl_s[r, :], e_at(q)) + eb_ref[q, 0:1, :]
            cum, phi = normal_parts(u)
            act = (u * cum).astype(BF)
            act_s[q, r, :] = act
            gp_s[q, r, :] = (cum + u * phi).astype(BF)
            br_s[r, :] += nn(act, s_at(q))

    zero = jnp.zeros((1, width), F32)

    def second_norm(i, sums):
        r = rows_at(i, MT)
        v = br_s[r, :]
        v = v - mean(v)
        rstd = lax.rsqrt(mean(v * v) + norm_eps)
        n = v * rstd
        lo_ref[r, :] = (n * g2 + b2).astype(BF)
        c = c_ref[r, :].astype(F32)
        m = c * g2
        g = rstd * (m - mean(m) - n * mean(m * n))
        s1g_ref[r, :] = g
        bg = g.astype(BF)
        bg_s[r, :] = bg
        return (sums[0] + jnp.sum(c * n, axis=0, keepdims=True),
                sums[1] + jnp.sum(c, axis=0, keepdims=True),
                sums[2] + jnp.sum(bg.astype(F32), axis=0, keepdims=True))

    g2g, b2g, sbg = lax.fori_loop(0, tiles, second_norm, (zero, zero, zero))
    vg_ref[6:7, :] = g2g
    vg_ref[7:8, :] = b2g
    vg_ref[3:4, :] = sbg

    def slot(kind):
        return slice(feat + kind * each, feat + (kind + 1) * each)

    cut = each // 2
    head = slice(feat + each, feat + each + cut)

    def moved(kind, q):
        if kind == 0:
            return pltpu.make_async_copy(stage.at[0], pack_hbm.at[q, :, slot(0), :], sems.at[0])
        if kind == 1:
            return pltpu.make_async_copy(stage.at[1, :, 0:cut, :], pack_hbm.at[q, :, head, :], sems.at[1])
        return pltpu.make_async_copy(stage.at[1, :, cut:each, :], rest_hbm.at[q], sems.at[2])

    def put(kind, n, value):
        count = value.shape[0]
        value = value.astype(BF)
        if chunks == 1:
            stage[kind, 0, n * count : (n + 1) * count, :] = value
        else:
            some = count // each
            stage[kind, n * some : (n + 1) * some] = value.reshape(some, each, width)

    @pl.loop(0, used)
    def _(q):
        def tile(i, total):
            r = rows_at(i, MT)
            d = nt(bg_s[r, :], s_at(q)) * gp_s[q, r, :].astype(F32)
            ug = d.astype(BF)
            ug_s[r, :] = ug
            s1g_ref[r, :] += nn(ug, e_at(q))
            return total + jnp.sum(ug.astype(F32), axis=0, keepdims=True)

        ebg_ref[q, 0:1, :] = lax.fori_loop(0, tiles, tile, zero)

        @pl.when(q > 0)
        def _():
            moved(0, q - 1).wait()
            moved(1, q - 1).wait()
            moved(2, q - 1).wait()

        half = units // 2
        for n in range(2):
            cols = slice(n * half, (n + 1) * half)
            put(0, n, tn(ug_s[:, cols], nl_s[...]))
            put(1, n, tn(act_s[q, :, cols], bg_s[...]))
        moved(0, q).start()
        moved(1, q).start()
        moved(2, q).start()

    def first_norm(i, sums):
        r = rows_at(i, MT)
        g = s1g_ref[r, :]
        n = n1_s[r, :]
        m = g * g1
        out = r1_s[r, 0:1] * (m - mean(m) - n * mean(m * n))
        s1g_ref[r, :] = out
        ag = out.astype(BF)
        ug_s[r, :] = ag

        @pl.loop(0, used)
        def _(q):
            do_ref[q, r, :] = nt(ag, wo_ref[q]).astype(BF)
            dot_ref[q, :, r] = nt(wo_ref[q], ag).astype(BF)

        return (sums[0] + jnp.sum(g * n, axis=0, keepdims=True),
                sums[1] + jnp.sum(g, axis=0, keepdims=True),
                sums[2] + jnp.sum(ag.astype(F32), axis=0, keepdims=True))

    g1g, b1g, obg = lax.fori_loop(0, tiles, first_norm, (zero, zero, zero))
    vg_ref[4:5, :] = g1g
    vg_ref[5:6, :] = b1g
    vg_ref[2:3, :] = obg

    def moved_out(q):
        return pltpu.make_async_copy(dwo_s.at[q], pack_hbm.at[q, :, 0:feat, :], dwo_sem.at[q])

    @pl.loop(0, used)
    def _(q):
        dwo_s[q] = tn(ctx_ref[q], ug_s[...]).astype(BF).reshape(chunks, feat, width)
        moved_out(q).start()

    moved(0, used - 1).wait()
    moved(1, used - 1).wait()
    moved(2, used - 1).wait()
    stage[0] = jnp.zeros_like(stage[0])

    def cleared(q):
        zeros = stage.at[0]
        return (pltpu.make_async_copy(zeros.at[:, 0:feat, :], pack_hbm.at[q, :, 0:feat, :], zero_sem.at[0, q]),
                pltpu.make_async_copy(zeros, pack_hbm.at[q, :, slot(0), :], zero_sem.at[1, q]),
                pltpu.make_async_copy(zeros.at[:, 0:cut, :], pack_hbm.at[q, :, head, :], zero_sem.at[2, q]))

    @pl.loop(used, groups)
    def _(q):
        for copy in cleared(q):
            copy.start()

    @pl.loop(0, used)
    def _(q):
        moved_out(q).wait()

    @pl.loop(used, groups)
    def _(q):
        for copy in cleared(q):
            copy.wait()


def run_middle(scal, x, ctx, wo, e, s, vec, eb, cot):
    groups, feat, width = wo.shape
    chunks, each = s.shape[1:3]
    tokens = x.shape[0]
    vm = pl.BlockSpec(memory_space=pltpu.VMEM)
    hbm = pl.BlockSpec(memory_space=pl.ANY)
    dma = pltpu.SemaphoreType.DMA
    sds = jax.ShapeDtypeStruct
    part = feat // chunks
    return pl.pallas_call(
        middle,
        name="middle",
        cost_estimate=pl.CostEstimate(flops=int(50e9), bytes_accessed=int(30e6), transcendentals=0),
        out_shape=(
            sds((tokens, width), BF), sds((tokens, width), F32),
            sds((groups, tokens, feat), BF), sds((groups, feat, tokens), BF),
            sds((8, width), F32), sds((groups, 8, width), F32),
            sds((groups, chunks, part + each + each // 2 + 8, width), BF),
            sds((groups, chunks, each - each // 2, width), BF)),
        in_specs=[pl.BlockSpec(memory_space=pltpu.SMEM)] + [vm] * 3 + [hbm] * 2 + [vm] * 3,
        out_specs=(vm,) * 6 + (hbm,) * 2,
        scratch_shapes=[
            pltpu.VMEM((tokens, width), BF), pltpu.VMEM((tokens, width), F32),
            pltpu.VMEM((tokens, 128), F32), pltpu.VMEM((tokens, width), F32),
            pltpu.VMEM((groups, tokens, width), BF), pltpu.VMEM((groups, tokens, width), BF),
            pltpu.VMEM((tokens, width), BF), pltpu.VMEM((tokens, width), BF),
            pltpu.VMEM((2, chunks, each, width), BF), dma((3,)),
            pltpu.VMEM((groups, chunks, each, width), BF), pltpu.VMEM((groups, chunks, each, width), BF),
            dma((2, groups)), pltpu.VMEM((groups, chunks, part, width), BF), dma((groups,)),
            dma((3, groups))],
        compiler_params=pltpu.CompilerParams(vmem_limit_bytes=67043328),
    )(scal, x, ctx, wo, e, s, vec, eb, cot)


def attn_specs(tokens, width, feat):
    def at_quarter(*block):
        return pl.BlockSpec((1,) + block, lambda q, s, b: (jnp.minimum(q, s[0]), 0, 0))

    def whole(*block):
        return pl.BlockSpec(block, lambda q, s, b: (0, 0))

    return at_quarter, whole


def weight_specs(groups, feat, width):
    def one(kind):
        return pl.BlockSpec((1, feat, width), lambda q, s, b: (jnp.minimum(q, s[0]), kind, 0))

    return [one(kind) for kind in range(3)]


def run_fwd(bounds, x, wqkv, bias, segc, segr):
    feat, width = wqkv.shape[1:]
    tokens = x.shape[0]
    heads = feat // HEAD_DIM

    def part(shape, kind=0):
        return pl.BlockSpec(shape, lambda i, b: (kind,) + (0,) * (len(shape) - 1))

    sds = jax.ShapeDtypeStruct
    return pl.pallas_call(
        attn_fwd,
        name="attn_fwd",
        cost_estimate=pl.CostEstimate(flops=int(10e9), bytes_accessed=int(10e6), transcendentals=0),
        out_shape=(sds((1, tokens, feat), BF), sds((1, 8, tokens), F32)),
        grid_spec=pltpu.PrefetchScalarGridSpec(
            num_scalar_prefetch=1, grid=(1,),
            in_specs=[part((tokens, width))] + [part((1, feat, width), n) for n in range(3)]
            + [part((1, 8, feat)), part((tokens, 128)), part((8, tokens))],
            out_specs=(part((1, tokens, feat)), part((1, 8, tokens))),
            scratch_shapes=[
                pltpu.VMEM((tokens, feat), BF), pltpu.VMEM((heads, feat, tokens), BF),
                pltpu.VMEM((heads, tokens, feat), BF), pltpu.VMEM((heads, BR, tokens), F32),
                pltpu.VMEM((heads, BR, BC), F32)]),
        compiler_params=pltpu.CompilerParams(vmem_limit_bytes=40 << 20),
    )(bounds, x, wqkv, wqkv, wqkv, bias, segc, segr)


def run_bwd(chunks, scal, bounds, x, wqkv, bias, bcol, segc, segr, ctx, lse, do, dot, s1g, rest):
    groups, feat, width = wqkv.shape[0], bias.shape[2], wqkv.shape[2]
    part, extra = feat // chunks, rest.shape[2]
    tokens = x.shape[0]
    heads = feat // HEAD_DIM
    at_quarter, whole = attn_specs(tokens, width, feat)
    sds = jax.ShapeDtypeStruct
    return pl.pallas_call(
        attn_bwd,
        name="attn_bwd",
        cost_estimate=pl.CostEstimate(flops=int(90e9), bytes_accessed=int(30e6), transcendentals=0),
        out_shape=(sds((tokens, width), F32), sds((groups, chunks, extra + 3 * part + 8, width), BF)),
        grid_spec=pltpu.PrefetchScalarGridSpec(
            num_scalar_prefetch=2, grid=(groups,),
            in_specs=[whole(tokens, width)] + weight_specs(groups, feat, width)
            + [at_quarter(8, feat), at_quarter(feat, 128), whole(tokens, 128), whole(8, tokens),
               at_quarter(tokens, feat), at_quarter(8, tokens), at_quarter(tokens, feat),
               at_quarter(feat, tokens), whole(tokens, width), pl.BlockSpec(
                (1, chunks, extra, width), lambda q, s, b: (jnp.minimum(q, s[0]), 0, 0, 0))],
            out_specs=(whole(tokens, width), pl.BlockSpec(
                (1, chunks, extra + 3 * part + 8, width), lambda q, s, b: (jnp.minimum(q, s[0]), 0, 0, 0))),
            scratch_shapes=[
                pltpu.VMEM((tokens, feat), BF), pltpu.VMEM((feat, tokens), BF),
                pltpu.VMEM((heads, tokens, feat), BF), pltpu.VMEM((heads, feat, tokens), BF),
                pltpu.VMEM((heads, feat, tokens), BF), pltpu.VMEM((tokens, feat), BF),
                pltpu.VMEM((feat, tokens), BF), pltpu.VMEM((feat, tokens), BF),
                pltpu.VMEM((feat, tokens), F32), pltpu.VMEM((feat, tokens), F32)]),
        compiler_params=pltpu.CompilerParams(vmem_limit_bytes=60 << 20),
    )(scal, bounds, x, wqkv, wqkv, wqkv, bias, bcol, segc, segr, ctx, lse, do, dot, s1g, rest)


PART = 16


def peer_copy(src, dst, send, recv, **where):
    return pltpu.make_async_remote_copy(
        src_ref=src, dst_ref=dst, send_sem=send, recv_sem=recv,
        device_id=where, device_id_type=pl.DeviceIdType.MESH)


def greet(w, t):
    barrier = pltpu.get_barrier_semaphore()
    mesh_id = pl.DeviceIdType.MESH
    pl.semaphore_signal(barrier, inc=1, device_id={"width": w ^ 1, "tok": t}, device_id_type=mesh_id)
    pl.semaphore_signal(barrier, inc=1, device_id={"width": w ^ 2, "tok": t}, device_id_type=mesh_id)
    pl.semaphore_signal(barrier, inc=1, device_id={"width": w, "tok": t ^ 1}, device_id_type=mesh_id)
    for k in range(1, 4):
        other = lax.rem(t + 2 * k, 8)
        pl.semaphore_signal(barrier, inc=1, device_id={"width": w, "tok": other}, device_id_type=mesh_id)
    pl.semaphore_wait(barrier, 6)


def reduce_kernel(g_ref, out_ref, ra, sx, rx, acc, ry, sy, rz,
                  sa_sem, ra_sem, sx_sem, rx_sem, sy_sem, ry_sem, sz_sem, rz_sem):
    w = lax.axis_index("width")
    t = lax.axis_index("tok")
    y = lax.rem(t, 2)
    z = lax.div(t, 2)
    parts = g_ref.shape[3] // PART
    greet(w, t)

    def rows(p):
        return pl.ds(pl.multiple_of(p * PART, PART), PART)

    def near(p, slot, quarter):
        return peer_copy(g_ref.at[quarter, :, :, rows(p), :], ra.at[slot, :, :, rows(p), :],
                         sa_sem.at[slot, p], ra_sem.at[slot, p], width=w ^ 1, tok=t)

    def across(p):
        return peer_copy(sx.at[:, :, rows(p), :], rx.at[:, :, rows(p), :],
                         sx_sem.at[p], rx_sem.at[p], width=w ^ 2, tok=t)

    def beside(p):
        return peer_copy(acc.at[:, 1 - y, rows(p), :], ry.at[:, rows(p), :],
                         sy_sem.at[p], ry_sem.at[p], width=w, tok=t ^ 1)

    def along(p, k):
        there = lax.rem(z + k, 4)
        return peer_copy(sy.at[there, rows(p), :], rz.at[k - 1, rows(p), :],
                         sz_sem.at[k - 1, p], rz_sem.at[k - 1, p], width=w, tok=2 * there + y)

    @pl.loop(0, parts)
    def _(p):
        @pl.when(w == 3)
        def _():
            near(p, 0, 0).start()

        @pl.when(w == 2)
        def _():
            near(p, 0, 1).start()

    @pl.loop(0, parts)
    def _(p):
        @pl.when(w == 3)
        def _():
            near(p, 1, 2).start()

        @pl.when(w == 1)
        def _():
            near(p, 0, 0).start()

    @pl.loop(0, parts)
    def _(p):
        @pl.when(w >= 2)
        def _():
            near(p, 0, 0).wait_recv()
            far = w - 2
            sx[:, :, rows(p), :] = (g_ref[far, :, :, rows(p), :].astype(F32)
                                    + ra[0, :, :, rows(p), :].astype(F32)).astype(BF)
            across(p).start()

    @pl.loop(0, parts)
    def _(p):
        total = g_ref[w, :, :, rows(p), :].astype(F32)
        acc[:, :, rows(p), :] = total.astype(BF)

        @pl.when(w == 2)
        def _():
            near(p, 1, 2).wait_recv()
            acc[:, :, rows(p), :] = (g_ref[w, :, :, rows(p), :].astype(F32)
                                     + ra[1, :, :, rows(p), :].astype(F32)).astype(BF)

        @pl.when(w == 1)
        def _():
            across(p).wait_recv()
            acc[:, :, rows(p), :] = (g_ref[w, :, :, rows(p), :].astype(F32)
                                     + rx[:, :, rows(p), :].astype(F32)).astype(BF)

        @pl.when(w == 0)
        def _():
            near(p, 0, 0).wait_recv()
            across(p).wait_recv()
            acc[:, :, rows(p), :] = (g_ref[w, :, :, rows(p), :].astype(F32)
                                     + ra[0, :, :, rows(p), :].astype(F32)
                                     + rx[:, :, rows(p), :].astype(F32)).astype(BF)

        beside(p).start()

    @pl.loop(0, parts)
    def _(p):
        beside(p).wait_recv()
        sy[:, rows(p), :] = (acc[:, y, rows(p), :].astype(F32) + ry[:, rows(p), :].astype(F32)).astype(BF)
        for k in range(1, 4):
            along(p, k).start()

    @pl.loop(0, parts)
    def _(p):
        total = sy[z, rows(p), :].astype(F32)
        for k in range(1, 4):
            along(p, k).wait_recv()
            total = total + rz[k - 1, rows(p), :].astype(F32)
        out_ref[rows(p), :] = total

    @pl.loop(0, parts)
    def _(p):
        @pl.when(w == 3)
        def _():
            near(p, 0, 0).wait_send()
            near(p, 1, 2).wait_send()

        @pl.when(w == 2)
        def _():
            near(p, 0, 1).wait_send()

        @pl.when(w == 1)
        def _():
            near(p, 0, 0).wait_send()

        @pl.when(w >= 2)
        def _():
            across(p).wait_send()

        beside(p).wait_send()
        for k in range(1, 4):
            along(p, k).wait_send()


def reduce_fast(terms):
    groups, shards, count, width = terms.shape
    parts = count // PART
    vm = pl.BlockSpec(memory_space=pltpu.VMEM)
    dma = pltpu.SemaphoreType.DMA
    column = (4, 2, count, width)
    return pl.pallas_call(
        reduce_kernel,
        name="reduce_fast",
        out_shape=jax.ShapeDtypeStruct((count, width), F32),
        in_specs=[vm],
        out_specs=vm,
        scratch_shapes=[
            pltpu.VMEM((2,) + column, BF), pltpu.VMEM(column, BF), pltpu.VMEM(column, BF),
            pltpu.VMEM(column, BF), pltpu.VMEM((4, count, width), BF), pltpu.VMEM((4, count, width), BF),
            pltpu.VMEM((3, count, width), BF),
            dma((2, parts)), dma((2, parts)), dma((parts,)), dma((parts,)),
            dma((parts,)), dma((parts,)), dma((3, parts)), dma((3, parts))],
        compiler_params=pltpu.CompilerParams(
            collective_id=1, has_side_effects=True, vmem_limit_bytes=40 << 20),
    )(terms.reshape((groups, 4, 2, count, width)))


def shard_kernel(own_ref, line_ref, all_ref, lines_ref, own_sem, recv_sem, z_sem, y_sem):
    w = lax.axis_index("width")
    t = lax.axis_index("tok")
    y = lax.rem(t, 2)
    z = lax.div(t, 2)
    mine = (pltpu.make_async_copy(own_ref, all_ref.at[:, t], own_sem.at[0]),
            pltpu.make_async_copy(line_ref, lines_ref.at[t], own_sem.at[1]))
    for copy in mine:
        copy.start()
    greet(w, t)
    for copy in mine:
        copy.wait()

    def both(s, sems, **where):
        return (peer_copy(all_ref.at[:, s], all_ref.at[:, s], sems.at[0], recv_sem.at[0, s], **where),
                peer_copy(lines_ref.at[s], lines_ref.at[s], sems.at[1], recv_sem.at[1, s], **where))

    def along(k):
        return both(t, z_sem.at[k - 1], width=w, tok=lax.rem(t + 2 * k, 8))

    def beside(zz):
        return both(2 * zz + y, y_sem.at[zz], width=w, tok=t ^ 1)

    def start(pair):
        for copy in pair:
            copy.start()

    def arrived(s):
        for copy in both(s, y_sem.at[0], width=w, tok=t ^ 1):
            copy.wait_recv()

    def sent(pair):
        for copy in pair:
            copy.wait_send()

    for k in range(1, 4):
        start(along(k))
    start(beside(z))
    for k in range(1, 4):
        zz = lax.rem(z + k, 4)
        arrived(2 * zz + y)
        start(beside(zz))

    @pl.loop(0, 4)
    def _(k):
        s = 2 * lax.rem(z + k, 4) + (1 - y)
        arrived(s)

    for k in range(1, 4):
        sent(along(k))

    @pl.loop(0, 4)
    def _(zz):
        sent(beside(zz))


def gather_kernel(own_ref, line_ref, ctx_ref, lse_ref, all_ref, lines_ref, ctxs_ref, lses_ref,
                  own_sem, recv_sem, z_sem, y_sem, core_sem, x_sem,
                  side_recv, side_core, side_x):
    w = lax.axis_index("width")
    t = lax.axis_index("tok")
    y = lax.rem(t, 2)
    z = lax.div(t, 2)
    mine = (pltpu.make_async_copy(own_ref, all_ref.at[w, t], own_sem.at[0]),
            pltpu.make_async_copy(line_ref, lines_ref.at[w, t], own_sem.at[1]),
            pltpu.make_async_copy(ctx_ref.at[0], ctxs_ref.at[w], own_sem.at[2]),
            pltpu.make_async_copy(lse_ref.at[0], lses_ref.at[w], own_sem.at[3]))
    for copy in mine:
        copy.start()
    greet(w, t)
    for copy in mine:
        copy.wait()

    def both(q, s, sems, **where):
        return (peer_copy(all_ref.at[q, s], all_ref.at[q, s], sems.at[0], recv_sem.at[0, q, s], **where),
                peer_copy(lines_ref.at[q, s], lines_ref.at[q, s], sems.at[1], recv_sem.at[1, q, s], **where))

    def along(k):
        return both(w, t, z_sem.at[k - 1], width=w, tok=lax.rem(t + 2 * k, 8))

    def beside(zz):
        return both(w, 2 * zz + y, y_sem.at[zz], width=w, tok=t ^ 1)

    def near(q, s):
        return both(q, s, core_sem.at[q, s], width=w ^ 1, tok=t)

    def across(s):
        return both(w, s, x_sem.at[s], width=w ^ 2, tok=t)

    def side(q, sems, **where):
        return (peer_copy(ctxs_ref.at[q], ctxs_ref.at[q], sems.at[0], side_recv.at[0, q], **where),
                peer_copy(lses_ref.at[q], lses_ref.at[q], sems.at[1], side_recv.at[1, q], **where))

    def side_near(q):
        return side(q, side_core.at[q], width=w ^ 1, tok=t)

    def side_across():
        return side(w, side_x, width=w ^ 2, tok=t)

    def start(pair):
        for copy in pair:
            copy.start()

    def arrived(q, s):
        for copy in near(q, s):
            copy.wait_recv()

    def sent(pair):
        for copy in pair:
            copy.wait_send()

    def outward(s):
        @pl.when(w <= 1)
        def _():
            start(across(s))

        @pl.when((w == 0) | (w == 2))
        def _():
            start(near(w, s))

    @pl.when(w <= 1)
    def _():
        start(side_across())

    @pl.when((w == 0) | (w == 2))
    def _():
        start(side_near(w))

    for k in range(1, 4):
        start(along(k))
    start(beside(z))
    outward(t)
    for k in range(1, 4):
        zz = lax.rem(z + k, 4)
        arrived(w, 2 * zz + y)
        start(beside(zz))
        outward(2 * zz + y)

    @pl.loop(0, 4)
    def _(k):
        s = 2 * lax.rem(z + k, 4) + (1 - y)
        arrived(w, s)
        outward(s)

    @pl.when(w >= 2)
    def _():
        for copy in side_near(w - 2):
            copy.wait_recv()
        start(side_near(w - 2))

    @pl.loop(0, 8)
    def _(k):
        zz = lax.rem(z + lax.div(k, 2), 4)
        s = 2 * zz + lax.rem(y + k, 2)

        @pl.when(w >= 2)
        def _():
            arrived(w - 2, s)
            start(near(w - 2, s))

    @pl.loop(0, 8)
    def _(s):
        @pl.when((w == 1) | (w == 3))
        def _():
            arrived(w - 1, s)

        @pl.when(w == 3)
        def _():
            arrived(0, s)

        @pl.when(w == 2)
        def _():
            arrived(1, s)

    for k in range(1, 4):
        sent(along(k))

    @pl.loop(0, 4)
    def _(zz):
        sent(beside(zz))

    @pl.loop(0, 8)
    def _(s):
        @pl.when(w <= 1)
        def _():
            sent(across(s))

        @pl.when((w == 0) | (w == 2))
        def _():
            sent(near(w, s))

        @pl.when(w >= 2)
        def _():
            sent(near(w - 2, s))

    @pl.when((w == 1) | (w == 3))
    def _():
        for copy in side_near(w - 1):
            copy.wait_recv()

    @pl.when(w == 3)
    def _():
        for copy in side_near(0):
            copy.wait_recv()

    @pl.when(w == 2)
    def _():
        for copy in side_near(1):
            copy.wait_recv()

    @pl.when(w <= 1)
    def _():
        sent(side_across())

    @pl.when((w == 0) | (w == 2))
    def _():
        sent(side_near(w))

    @pl.when(w >= 2)
    def _():
        sent(side_near(w - 2))


def shard_fast(own, line):
    hbm = pl.BlockSpec(memory_space=pl.ANY)
    dma = pltpu.SemaphoreType.DMA
    sds = jax.ShapeDtypeStruct
    return pl.pallas_call(
        shard_kernel,
        name="shard_fast",
        out_shape=(sds((own.shape[0], 8) + own.shape[1:], BF), sds((8,) + line.shape, BF)),
        in_specs=[hbm] * 2,
        out_specs=(hbm,) * 2,
        scratch_shapes=[dma((2,)), dma((2, 8)), dma((3, 2)), dma((4, 2))],
        compiler_params=pltpu.CompilerParams(collective_id=2, has_side_effects=True),
        cost_estimate=pl.CostEstimate(flops=int(10e9), bytes_accessed=int(10e6), transcendentals=0),
    )(own, line)


def gather_fast(own, line, ctx, lse):
    hbm = pl.BlockSpec(memory_space=pl.ANY)
    dma = pltpu.SemaphoreType.DMA
    sds = jax.ShapeDtypeStruct
    return pl.pallas_call(
        gather_kernel,
        name="gather_fast",
        out_shape=(sds((4, 8) + own.shape, BF), sds((4, 8) + line.shape, BF),
                   sds((4,) + ctx.shape[1:], BF), sds((4,) + lse.shape[1:], F32)),
        in_specs=[hbm] * 4,
        out_specs=(hbm,) * 4,
        scratch_shapes=[dma((4,)), dma((2, 4, 8)), dma((3, 2)), dma((4, 2)), dma((4, 8, 2)), dma((8, 2)),
                        dma((2, 4)), dma((4, 2)), dma((2,))],
        compiler_params=pltpu.CompilerParams(collective_id=3, has_side_effects=True),
        cost_estimate=pl.CostEstimate(flops=int(30e9), bytes_accessed=int(30e6), transcendentals=0),
    )(own, line, ctx, lse)


def columns(array):
    return jnp.broadcast_to(array[:, :, None], array.shape + (128,)).astype(BF)


def gather_all(pack):
    return lax.all_gather(pack, ("width", "tok"), axis=0, tiled=False)


def scatter_all(terms):
    flat = terms.reshape((-1,) + terms.shape[2:])
    return lax.psum_scatter(flat, ("width", "tok"), scatter_dimension=0, tiled=True)[0]


def local(tokens_in, seq_lengths, *rest):
    weights, biases, out_grad = rest[:6], rest[6:15], rest[15]
    groups = lax.axis_size("width")
    shards = lax.axis_size("tok")
    level = lax.axis_index("width")
    tokens, width = tokens_in.shape
    owned = weights[0].shape[0]
    owned_ff = weights[4].shape[0]
    feat = owned * shards
    units = owned_ff * shards

    def flat(*vectors):
        line = jnp.concatenate(vectors)
        return jnp.pad(line, (0, width - line.shape[0]))[None, :]

    fast = groups == 4 and shards == 8 and owned % 8 == 0
    late = gather_all(jnp.concatenate([weights[4], flat(*biases[2:])], axis=0))
    late = late.reshape((groups, shards) + late.shape[1:])
    soon = jnp.stack(weights[:3])
    line = jnp.concatenate(biases[:2])
    if fast:
        line = jnp.pad(line[None, :], ((0, 7), (0, 128 - line.shape[0])))
        own, line = shard_fast(soon, line)
        line = line[:, 0, : 2 * owned]
    else:
        own = lax.all_gather(soon, "tok", axis=1)
        line = lax.all_gather(line, "tok", axis=0)
    own = own.reshape(3, feat, width)
    qv = jnp.stack([line[:, :owned].reshape(feat), line[:, owned:].reshape(feat)])

    ends = jnp.cumsum(seq_lengths[0])
    positions = jnp.arange(tokens, dtype=jnp.int32)
    segment = jnp.sum((positions[:, None] >= ends[None, :]).astype(jnp.int32), axis=1)
    lows = jnp.sum((segment[None, :] < segment[::BR, None]).astype(jnp.int32), axis=1)
    highs = jnp.sum((segment[None, :] <= segment[BR - 1 :: BR, None]).astype(jnp.int32), axis=1)
    bounds = jnp.stack([lows // BC, (highs + BC - 1) // BC])
    segc = jnp.broadcast_to(segment[:, None], (tokens, 128))
    segr = jnp.broadcast_to(segment[None, :], (8, tokens))
    scal = level[None].astype(jnp.int32)

    def as_bias(pair):
        return jnp.pad(pair.astype(F32), ((0, 0), (0, 6), (0, 0)))

    ctx, lse = run_fwd(bounds, tokens_in, own, as_bias(qv[None]), segc, segr)
    if fast:
        ws, wo, ctx, lse = gather_fast(weights[5], weights[3], ctx, lse)
    else:
        both = gather_all(jnp.concatenate([weights[5], weights[3]], axis=0))
        both = both.reshape((groups, shards) + both.shape[1:])
        ws, wo = both[:, :, :owned_ff], both[:, :, owned_ff:]
        ctx, lse = (lax.all_gather(part[0], "width", axis=0) for part in (ctx, lse))
    wo = wo.reshape(groups, feat, width)
    we, chunks = late, shards
    if not fast:
        we, ws, chunks = late[:, :, :owned_ff].reshape(groups, 1, units, width), ws.reshape(groups, 1, units, width), 1
    row = late[:, :, owned_ff]
    sizes = [b.shape[0] for b in biases[2:]]
    starts = [sum(sizes[:n]) for n in range(7)]
    vecs = [row[:, :, a : a + n].reshape(groups, n * shards) for a, n in zip(starts, sizes)]
    eb = jnp.pad(vecs[1][:, None, :].astype(F32), ((0, 0), (0, 7), (0, 0)))
    vec = jnp.stack([v.reshape(-1) for v in [vecs[0], vecs[2]] + vecs[3:]]).astype(F32)
    vec = jnp.pad(vec, ((2, 0), (0, 0)))

    qv = jnp.pad(qv, ((0, 6), (0, width - feat)))
    own, wo = lax.optimization_barrier((own, wo))
    wqkv = lax.all_gather(jnp.concatenate([own.reshape(3 * feat, width), qv], axis=0), "width", axis=0)
    qv = wqkv[:, 3 * feat : 3 * feat + 2, :feat]
    bias = as_bias(qv)
    bcol = jnp.pad(jnp.swapaxes(qv, 1, 2), ((0, 0), (0, 0), (0, 126)))

    result, s1g, do, dot, vg, ebg, first, rest = run_middle(
        scal, tokens_in, ctx, wo, we, ws, vec, eb, out_grad[0])
    mine = jnp.arange(groups) <= level

    def split(line):
        return line.reshape(groups, shards, -1)

    def only(term):
        return jnp.where(mine.reshape((groups,) + (1,) * (term.ndim - 1)), term, jnp.zeros_like(term))

    def parted(term, sizes):
        if fast:
            return term
        out, at = [], 0
        for size in sizes:
            out.append(term[:, 0, at : at + size * shards].reshape(groups, shards, size, width))
            at = at + size * shards
        return jnp.concatenate(out + [jnp.zeros((groups, shards, 8, width), BF)], axis=2)

    def lined(*lines):
        line = jnp.concatenate(lines, axis=2).astype(BF)
        line = jnp.pad(line, ((0, 0), (0, 0), (0, width - line.shape[2])))
        return jnp.pad(line[:, :, None, :], ((0, 0), (0, 0), (0, 7), (0, 0)))

    line = lined(only(split(ebg[:, 0])), *(split(vg[n]) for n in range(2, 8)))
    if not fast:
        first = jnp.concatenate([first[:, :, :-8], rest], axis=2)
        first = parted(first, (owned, owned_ff, owned_ff))
    first = lax.dynamic_update_slice(first, line, (0, 0, first.shape[2] - 8, 0))
    first, s1g = lax.optimization_barrier((first, s1g))
    early = scatter_all(first)
    input_grad, second = run_bwd(
        chunks, scal, bounds, tokens_in, wqkv, bias, bcol, segc, segr, ctx, lse, do, dot, s1g, rest)

    if fast:
        final = reduce_fast(second)
        shrunk, final = final[: rest.shape[2]], final[rest.shape[2] :]
        late = [final[3 * owned, :owned], final[3 * owned, 256 : 256 + owned]]
    else:
        second = second[:, :, rest.shape[2] :]
        line = only(jnp.concatenate([split(second[:, 0, 3 * feat, n : n + feat]) for n in (0, 256)], axis=2))
        second = only(parted(second, (owned,) * 3))
        line = jnp.pad(line, ((0, 0), (0, 0), (0, width - line.shape[2])))[:, :, None, :]
        second = lax.dynamic_update_slice(second, line, (0, 0, 3 * owned, 0))
        final = scatter_all(second).astype(F32)
        late = [final[3 * owned, :owned], final[3 * owned, owned : 2 * owned]]
    early = early.astype(F32)
    outs = [final[n * owned : (n + 1) * owned] for n in range(3)]
    last = early[owned + owned_ff : early.shape[0] - 8]
    if fast:
        last = jnp.concatenate([last, shrunk], axis=0)
    outs += [early[:owned], early[owned : owned + owned_ff], last]
    soon = early[-8]
    vecs = [soon[owned_ff + n * owned : owned_ff + (n + 1) * owned] for n in range(6)]
    outs += late + [vecs[0], soon[:owned_ff]] + vecs[1:]
    return (result[None], input_grad[None]) + tuple(outs)


def solution(mesh):
    both = ("width", "tok")
    placed = (P("tok", None), P("tok", None)) + (P(both, None),) * 6 + (P(both),) * 9
    return jax.shard_map(
        local,
        mesh=mesh,
        in_specs=placed + (P("width", "tok", None),),
        out_specs=(P("width", "tok", None), P("width", "tok", None))
        + (P(both, None),) * 6 + (P(both),) * 9,
        check_vma=False,
    )
```
